128 devices in a mesh: ctx: 16 (over y, x), tp: 8 (over z, core).
Axes of the slice: x: 4, y: 4, z: 4, core: 2. Of those that a mesh axis runs over, the one named last changes fastest.
Arguments:
- hidden: bfloat16 [8, 8192], P(None, 'ctx'), may hold values from -4.8 to 4.8, as said below
- norm_gains: bfloat16 [4, 8192], P(None, 'ctx'), may hold values from 0.5 to 1.5
- w_query: bfloat16 [4, 8192, 8192], P(None, 'ctx', 'tp'), may hold values from -0.0625 to 0.0625
- w_key: bfloat16 [4, 8192, 1024], P(None, 'ctx', 'tp'), may hold values from -0.125 to 0.125
- w_value: bfloat16 [4, 8192, 1024], P(None, 'ctx', 'tp'), may hold values from -0.125 to 0.125
- w_out: bfloat16 [4, 8192, 8192], P(None, 'tp', 'ctx'), may hold values from -0.0625 to 0.0625
- key_cache: bfloat16 [4, 8, 8, 2048, 128], P(None, None, 'tp', 'ctx'), may hold values from -9 to 9
- value_cache: bfloat16 [4, 8, 8, 2048, 128], P(None, None, 'tp', 'ctx'), may hold values from -6 to 6
- lengths: int32 [8], replicated, may hold values from 1 to 2048, 8200 in all
Outputs:
- updated: float32 [8, 8192], P(None, 'ctx')
The draws below stay inside these ranges and needn't reach their ends.
Inputs may be any that keep to these rules, and one draw needn't show every extreme that they name: Each sequence has lengths[b] valid cache positions 0 .. lengths[b] - 1, between 1 and 2048; the longest sequence has exactly 2048; the new token sits at position lengths[b]. `hidden`: activations of order 0.2; in each block of 512 consecutive features one sequence, chosen at random, has entries four times larger.
All inputs are finite; a program needn't handle non-finite values.
Results may differ from the reference program's by a relative error of at most 0.02.
Values sent between devices are 32-bit elements.
A program may use at most 64 MiB of HBM per device.

```python
import math
import jax
import jax.numpy as jnp
import numpy as np
from jax import lax

D = 8192
HQ = 64
KVH = 8
HD = 128
LAYERS = 4
BATCH = 8
CAP = 2048
D_DEV = 512


def draw_hidden(key, part):
    base_key, owner_key = jax.random.split(jax.random.fold_in(key, 7))
    block_count = D // D_DEV
    owners = jax.random.randint(owner_key, (block_count,), 0, BATCH)
    column_owner = owners[jnp.arange(D) // D_DEV]
    factor = jnp.where(column_owner[None, :] == jnp.arange(BATCH)[:, None], 4.0, 1.0)
    base_draw = jnp.clip(jax.random.normal(base_key, (BATCH, D), jnp.float32), -6.0, 6.0)
    return (0.2 * factor * base_draw).astype(jnp.bfloat16)


def block_scale(rng, extent, pieces, smallest, high):
    gain = 1.0
    for axis_at, parts in pieces:
        draws = jax.random.uniform(jax.random.fold_in(jax.random.fold_in(rng, 6), axis_at), (parts,), jnp.float32, smallest / len(pieces), high / len(pieces))
        gain = gain * jnp.repeat(jnp.exp(draws), extent[axis_at] // parts).reshape((-1,) + (1,) * (len(extent) - 1 - axis_at))
    return gain


def profile(count, total, reach, slope):
    portions = [(1 << 20) // math.isqrt(grade ** slope) + 1 for grade in range(2, count + 1)]
    surplus, given = total - reach - (count - 1), [1] * (count - 1)
    while surplus > 0:
        movable = [i for i in range(count - 1) if given[i] < reach]
        mass, remaining = sum([portions[i] for i in movable]), surplus
        for i in movable:
            extra = min(reach - given[i], max(1, remaining * portions[i] // mass), surplus)
            given[i] = given[i] + extra
            surplus = surplus - extra
    return np.array([reach] + given)


def ragged(rng, amount, total, most, lean):
    if amount == 2:
        one = jax.random.randint(rng, (), max(1, total - most), min(most, total - 1) + 1)
        return jnp.stack([one, total - one])
    sizes = jnp.asarray(profile(amount, total, most, lean), jnp.int32)
    couples = (amount - 1) // 2
    source_of, taker = sizes[1:1 + 2 * couples:2], sizes[2:2 + 2 * couples:2]
    slack = jnp.minimum(source_of - 1, most - taker)
    shifted = jax.random.randint(jax.random.fold_in(rng, 1), (couples,), 0, 1 << 20) % (slack + 1)
    sizes = sizes.at[1:1 + 2 * couples:2].set(source_of - shifted).at[2:2 + 2 * couples:2].set(taker + shifted)
    return sizes[jax.random.permutation(jax.random.fold_in(rng, 2), amount)]


def scatter_about(stream_key, dims, scale, limit, pieces=(), kind=jnp.bfloat16):
    array = scale * jax.random.normal(stream_key, dims, jnp.float32)
    if pieces:
        array = array * block_scale(stream_key, dims, pieces, -0.22, 0.18)
    return jnp.clip(array, -limit, limit).astype(kind)


def setup_inputs(seed: int = 0) -> dict:
    key_list = jax.random.split(jax.random.key(seed), 10)
    hidden = draw_hidden(jax.random.fold_in(key_list[9], 71), 0)
    norm_gains = jnp.clip(1.0 + 0.1 * jax.random.normal(key_list[1], (LAYERS, D), jnp.float32), 0.5, 1.5).astype(jnp.bfloat16)
    w_query = scatter_about(key_list[2], (LAYERS, D, HQ * HD), D ** -0.5, 0.0625, ((1, 16), (2, 8)))
    w_key = scatter_about(key_list[3], (LAYERS, D, KVH * HD), (D // 4) ** -0.5, 0.125, ((1, 16), (2, 8)))
    w_value = scatter_about(key_list[4], (LAYERS, D, KVH * HD), (D // 4) ** -0.5, 0.125, ((1, 16), (2, 8)))
    w_out = scatter_about(key_list[5], (LAYERS, HQ * HD, D), (HQ * HD) ** -0.5, 0.0625, ((1, 8), (2, 16)))
    key_cache = scatter_about(key_list[6], (LAYERS, BATCH, KVH, CAP, HD), 1.5, 9.0, ((2, 8), (3, 16)))
    value_cache = scatter_about(key_list[7], (LAYERS, BATCH, KVH, CAP, HD), 1.0, 6.0, ((2, 8), (3, 16)))
    lengths = ragged(key_list[8], BATCH, BATCH * CAP // 2 + BATCH, CAP, 2).astype(jnp.int32)
    return dict(hidden=hidden, norm_gains=norm_gains, w_query=w_query, w_key=w_key, w_value=w_value, w_out=w_out, key_cache=key_cache, value_cache=value_cache, lengths=lengths)


mask_fill = -1e+30
norm_eps = 1e-05
rope_base = 500000.0

def rotate(vectors, positions):
    width = vectors.shape[-1]
    half_width = width // 2
    exponents = jnp.arange(half_width, dtype=jnp.float32) * (2.0 / width)
    frequency = jnp.exp(-exponents * math.log(rope_base))
    angles = positions.astype(jnp.float32)[:, None] * frequency[None, :]
    cosine = jnp.cos(angles)[:, None, :]
    sine_part = jnp.sin(angles)[:, None, :]
    first_half = vectors[..., :half_width]
    second_half = vectors[..., half_width:]
    return jnp.concatenate([first_half * cosine - second_half * sine_part, second_half * cosine + first_half * sine_part], axis=-1)

def reference(hidden, norm_gains, w_query, w_key, w_value, w_out, key_cache, value_cache, lengths):
    stream = hidden.astype(jnp.float32)
    group_size = HQ // KVH
    logit_multiplier = 1.0 / math.sqrt(HD)
    positions = jnp.arange(CAP, dtype=jnp.int32)
    usable = (positions[None, :] < lengths[:, None])[:, None, None, :]
    for layer_idx in range(LAYERS):
        reciprocal_value = lax.rsqrt(lax.optimization_barrier(jnp.sum(stream * stream, axis=1)) / D + norm_eps)
        scaled = (stream * norm_gains[layer_idx].astype(jnp.float32)).astype(jnp.bfloat16)
        raw_query = jnp.dot(scaled, w_query[layer_idx], preferred_element_type=jnp.float32)
        raw_key = jnp.dot(scaled, w_key[layer_idx], preferred_element_type=jnp.float32)
        raw_value = jnp.dot(scaled, w_value[layer_idx], preferred_element_type=jnp.float32)
        query = rotate((raw_query * reciprocal_value[:, None]).reshape(BATCH, HQ, HD), lengths).astype(jnp.bfloat16)
        fresh_lookup_vector = rotate((raw_key * reciprocal_value[:, None]).reshape(BATCH, KVH, HD), lengths).astype(jnp.bfloat16)
        new_value = (raw_value * reciprocal_value[:, None]).reshape(BATCH, KVH, HD).astype(jnp.bfloat16)
        shared_head_sets = query.reshape(BATCH, KVH, group_size, HD).astype(jnp.float32)
        scores = jnp.einsum('bkgd,bksd->bkgs', shared_head_sets, key_cache[layer_idx].astype(jnp.float32), precision=lax.Precision.HIGHEST) * logit_multiplier
        self_match_logit = jnp.einsum('uryj,urj->ury', shared_head_sets, fresh_lookup_vector.astype(jnp.float32), precision=lax.Precision.HIGHEST) * logit_multiplier
        masked = jnp.where(usable, scores, mask_fill)
        largest = jnp.maximum(lax.optimization_barrier(jnp.max(masked, axis=-1)), self_match_logit)
        attention_probabilities = jnp.where(usable, jnp.exp(masked - largest[..., None]), 0.0)
        fresh = jnp.exp(self_match_logit - largest)
        nearest_whole = lax.optimization_barrier(attention_probabilities.astype(jnp.bfloat16)).astype(jnp.float32)
        fresh_rounded = lax.optimization_barrier(fresh.astype(jnp.bfloat16)).astype(jnp.float32)
        numerator = jnp.einsum('bkgs,bksd->bkgd', nearest_whole, value_cache[layer_idx].astype(jnp.float32), precision=lax.Precision.HIGHEST)
        numerator = numerator + fresh_rounded[..., None] * new_value.astype(jnp.float32)[:, :, None, :]
        denominator = lax.optimization_barrier(jnp.sum(attention_probabilities, axis=-1)) + fresh
        context = (numerator / denominator[..., None]).reshape(BATCH, HQ * HD).astype(jnp.bfloat16)
        stream = stream + jnp.dot(context, w_out[layer_idx], preferred_element_type=jnp.float32)
    return stream
```

```python
import functools
import math

import jax
import jax.numpy as jnp
from jax import lax
from jax.experimental import pallas as pl
from jax.experimental.pallas import tpu as pltpu
from jax.sharding import PartitionSpec as P

mask_fill = -1e30
norm_eps = 1e-05
rope_base = 500000.0
MESH = pl.DeviceIdType.MESH
QROWS = 11


def kernel(dims, hidden_ref, gains_ref, lengths_ref, wq_h, wk_h, wv_h, wo_h, kc_h, vc_h, out_ref,
           wq, wk, wv, wo, kc, vc, gain, bias, cosine, sine, qs, qr, kst, vst, krv, vrv, kb, vb,
           orr, cm, tps, tpr, w_sem, qs_sem, qr_sem, os_sem, or_sem, ts_sem, tr_sem, hs_sem, hr_sem):
    n, tn, side, layers, batch, feat, total, heads, hd, span = dims
    f32, bf16 = jnp.float32, jnp.bfloat16
    pieces = tps.shape[0]
    piece = feat // pieces
    scale = 1.0 / math.sqrt(hd)
    me = lax.axis_index("ctx")
    mt = lax.axis_index("tp")
    y, x = me // side, lax.rem(me, side)
    z, core = mt // 2, lax.rem(mt, 2)
    zn = tn // 2
    weights = ((kc_h, kc), (vc_h, vc), (wq_h, wq), (wk_h, wk), (wv_h, wv), (wo_h, wo))
    KC, VC, WQ, WK, WV, WO = range(6)

    def load(index, layer):
        source, target = weights[index]
        return pltpu.make_async_copy(source.at[layer], target.at[layer], w_sem.at[index, layer])

    for index in range(len(weights)):
        load(index, 0).start()

    def hops(step, size):
        return min(step, size - step)

    offsets = [(dy, dx) for dy in range(side) for dx in range(side) if (dy, dx) != (0, 0)]
    offsets.sort(key=lambda o: -(hops(o[0], side) + hops(o[1], side)))
    peers = []
    for dy, dx in offsets:
        py, px = lax.rem(y + dy, side), lax.rem(x + dx, side)
        peers.append((py * side + px, py, px))
    toffsets = [(dz, dc) for dz in range(zn) for dc in range(2) if (dz, dc) != (0, 0)]
    toffsets.sort(key=lambda o: -(2 * hops(o[0], zn) + o[1]))
    tpeers = [lax.rem(z + dz, zn) * 2 + lax.rem(core + dc, 2) for dz, dc in toffsets]

    barrier = pltpu.get_barrier_semaphore()
    for p, _, _ in peers:
        pl.semaphore_signal(barrier, inc=1, device_id={"ctx": p}, device_id_type=MESH)
    for p in tpeers:
        pl.semaphore_signal(barrier, inc=1, device_id={"tp": p}, device_id_type=MESH)

    half = hd // 2
    lane = lax.broadcasted_iota(jnp.int32, (heads, hd), 1)
    low = lane < half
    mine = (x, side + y)
    slot = lax.broadcasted_iota(jnp.int32, (heads, side * span), 1)
    block = slot // span
    positions = (y * side * span + slot, (block * side + x) * span + lax.rem(slot, span))
    exponent = jnp.where(low, lane, lane - half).astype(f32) * (2.0 / hd)
    frequency = jnp.exp(-exponent * math.log(rope_base))
    for g in range(2):
        size = lengths_ref[mine[g]]
        bias[g] = jnp.where(positions[g] < size, 0.0, mask_fill)
        angle = jnp.full((heads, hd), size, jnp.int32).astype(f32) * frequency
        cosine[g] = jnp.cos(angle)
        sine[g] = jnp.where(low, -jnp.sin(angle), jnp.sin(angle))
    for l in range(layers):
        gain[l] = jnp.broadcast_to(gains_ref[l:l + 1, :].astype(f32), (batch, feat))
    out_ref[...] = hidden_ref[...].astype(f32)
    own_mask = jnp.where(jnp.full((heads, 1), y, jnp.int32) == jnp.full((heads, 1), x, jnp.int32), 0.0, mask_fill)

    def ship(l):
        copies = []
        for r in range(1, side):
            px, py = lax.rem(x + r, side), lax.rem(y + r, side)
            for i, (source, target) in enumerate(((kst, krv), (vst, vrv))):
                copies.append(pltpu.make_async_remote_copy(
                    src_ref=source.at[l, px], dst_ref=target.at[l, 0, x],
                    send_sem=hs_sem.at[l, i, 0, r - 1], recv_sem=hr_sem.at[l, i, 0, r - 1],
                    device_id={"ctx": y * side + px}, device_id_type=MESH))
                copies.append(pltpu.make_async_remote_copy(
                    src_ref=source.at[l, side + py], dst_ref=target.at[l, 1, y],
                    send_sem=hs_sem.at[l, i, 1, r - 1], recv_sem=hr_sem.at[l, i, 1, r - 1],
                    device_id={"ctx": py * side + x}, device_id_type=MESH))
        return copies

    def stage(l):
        load(KC, l).wait()
        load(VC, l).wait()
        for source, staged, held in ((kc, kst, krv), (vc, vst, vrv)):
            for b in range(batch):
                staged[l, b] = source[l, b, 0].astype(f32)
            held[l, 0, x] = source[l, mine[0], 0].astype(f32)
            held[l, 1, y] = source[l, mine[1], 0].astype(f32)

    stage(0)
    pl.semaphore_wait(barrier, n - 1 + tn - 1)
    for c in ship(0):
        c.start()

    def rotate(u, g):
        return u * cosine[g] + pltpu.roll(u, half, 1) * sine[g]

    def rounded(u):
        return u.astype(bf16).astype(f32)

    def layer_step(l, carry):
        stream = out_ref[...]
        scaled = (stream * gain[l]).astype(bf16)
        squares = jnp.sum(stream * stream, axis=1, keepdims=True)
        load(WQ, l).wait()
        load(WK, l).wait()
        load(WV, l).wait()

        @pl.when(l + 1 < layers)
        def _():
            for index in range(len(weights)):
                load(index, l + 1).start()

        def put(row, tile):
            qs[pl.ds(row, batch, stride=16), :] = tile

        put(heads, jnp.dot(scaled, wk[l], preferred_element_type=f32))
        put(heads + 1, jnp.dot(scaled, wv[l], preferred_element_type=f32))
        put(heads + 2, jnp.broadcast_to(squares, (batch, hd)))
        q = jnp.dot(scaled, wq[l], preferred_element_type=f32)
        for h in range(heads):
            put(h, q[:, h * hd:(h + 1) * hd])
        qc = []
        for k, (p, py, px) in enumerate(peers):
            for g, b in ((0, px), (1, side + py)):
                c = pltpu.make_async_remote_copy(
                    src_ref=qs.at[pl.ds(pl.multiple_of(b * 16, 16), QROWS)], dst_ref=qr.at[k, g, pl.ds(0, QROWS)],
                    send_sem=qs_sem.at[k, g], recv_sem=qr_sem.at[k, g],
                    device_id={"ctx": p}, device_id_type=MESH)
                c.start()
                qc.append(c)

        for c in ship(l):
            c.wait()
        for g in range(2):
            kb[g] = krv[l, g].reshape(side * span, hd).astype(bf16)
            vb[g] = vrv[l, g].reshape(side * span, hd).astype(bf16)

        for c in qc:
            c.wait_recv()
        stats = []
        for g in range(2):
            at = pl.multiple_of(mine[g] * 16, 16)
            whole = qs[pl.ds(at, heads), :]
            rest = qs[pl.ds(pl.multiple_of(at + 8, 8), QROWS - heads), :]
            for k in range(n - 1):
                whole = whole + qr[k, g, 0:heads]
                rest = rest + qr[k, g, heads:QROWS]
            inverse = lax.rsqrt(rest[2:3] / total + norm_eps)
            query = rounded(rotate(whole * inverse, g))
            new_key = rounded(rotate(jnp.broadcast_to(rest[0:1] * inverse, (heads, hd)), g))
            new_value = rounded(rest[1:2] * inverse)
            score = lax.dot_general(query.astype(bf16), kb[g], (((1,), (1,)), ((), ())), preferred_element_type=f32)
            own = jnp.sum(query * new_key, axis=1, keepdims=True) * scale + own_mask
            masked = score * scale + bias[g]
            top = jnp.maximum(jnp.max(masked, axis=1, keepdims=True), own)
            weight = jnp.exp(masked - top)
            fresh = jnp.exp(own - top)
            denominator = jnp.sum(weight, axis=1, keepdims=True) + fresh
            numerator = jnp.dot(weight.astype(bf16), vb[g], preferred_element_type=f32) + rounded(fresh) * new_value
            orr[me, g * heads:(g + 1) * heads, :] = numerator / denominator
            stats.append(top + jnp.log(denominator))
        orr[me, 2 * heads:3 * heads, :] = jnp.where(low, stats[0], stats[1])
        oc = []
        for k, (p, _, _) in enumerate(peers):
            c = pltpu.make_async_remote_copy(
                src_ref=orr.at[me], dst_ref=orr.at[me], send_sem=os_sem.at[k], recv_sem=or_sem.at[k],
                device_id={"ctx": p}, device_id_type=MESH)
            c.start()
            oc.append(c)

        @pl.when(l + 1 < layers)
        def _():
            stage(l + 1)

        load(WO, l).wait()
        for c in qc:
            c.wait_send()
        for c in oc:
            c.wait_recv()

        @pl.when(l + 1 < layers)
        def _():
            for c in ship(l + 1):
                c.start()

        logs = [orr[c, 2 * heads:3 * heads, :] for c in range(n)]
        groups = [[[r * side + b for r in range(side)] for b in range(side)],
                  [[b * side + r for r in range(side)] for b in range(side)]]

        def over(values, op):
            return [[functools.reduce(op, [values[c] for c in group]) for group in part] for part in groups]

        def split(pair, c):
            return jnp.where(low, pair[0][c % side], pair[1][c // side])

        largest = over(logs, jnp.maximum)
        factors = [jnp.exp(logs[c] - split(largest, c)) for c in range(n)]
        sums = over(factors, jnp.add)
        inverses = [[1.0 / s for s in part] for part in sums]
        factors = [factors[c] * split(inverses, c) for c in range(n)]
        swapped = [pltpu.roll(f, half, 1) for f in factors]
        for g in range(2):
            for b, group in enumerate(groups[g]):
                merged = None
                for c in group:
                    factor = jnp.where(low, factors[c], swapped[c]) if g == 0 else jnp.where(low, swapped[c], factors[c])
                    term = orr[c, g * heads:(g + 1) * heads, :] * factor
                    merged = term if merged is None else merged + term
                at = (g * side + b) * heads
                cm[at:at + heads, :] = merged
        context = jnp.concatenate([cm[pl.ds(h, batch, stride=heads), :] for h in range(heads)], axis=1).astype(bf16)
        odd = lax.rem(l, 2)
        ts = []
        for i in range(pieces):
            cut = slice(i * piece, (i + 1) * piece)
            tps[i] = jnp.dot(context, wo[l, :, cut], preferred_element_type=f32)
            for k, p in enumerate(tpeers):
                c = pltpu.make_async_remote_copy(
                    src_ref=tps.at[i], dst_ref=tpr.at[odd, i, k], send_sem=ts_sem.at[i, k],
                    recv_sem=tr_sem.at[odd, i, k], device_id={"tp": p}, device_id_type=MESH)
                c.start()
                ts.append(c)
        for c in oc:
            c.wait_send()
        for i in range(pieces):
            cut = slice(i * piece, (i + 1) * piece)
            moved = out_ref[:, cut] + tps[i]
            for k in range(tn - 1):
                ts[i * (tn - 1) + k].wait_recv()
                moved = moved + tpr[odd, i, k]
            out_ref[:, cut] = moved
        for c in ts:
            c.wait_send()
        return carry

    lax.fori_loop(0, layers, layer_step, 0)


def shards(sizes, hidden, norm_gains, w_query, w_key, w_value, w_out, key_cache, value_cache, lengths):
    n, tn = sizes
    layers, feat, columns = w_query.shape
    batch = hidden.shape[0]
    _, _, _, span, hd = key_cache.shape
    heads = columns // hd
    side = math.isqrt(n)
    dims = (n, tn, side, layers, batch, feat, feat * n, heads, hd, span)
    pieces = 2
    f32, bf16 = jnp.float32, jnp.bfloat16
    vmem = pl.BlockSpec(memory_space=pltpu.VMEM)
    far = pl.BlockSpec(memory_space=pl.ANY)

    def like(array):
        return pltpu.VMEM(array.shape, array.dtype)

    dma = pltpu.SemaphoreType.DMA
    return pl.pallas_call(
        functools.partial(kernel, dims),
        out_shape=jax.ShapeDtypeStruct((batch, feat), f32),
        in_specs=[vmem, vmem, pl.BlockSpec(memory_space=pltpu.SMEM)] + [far] * 6,
        out_specs=vmem,
        scratch_shapes=[
            like(w_query), like(w_key), like(w_value), like(w_out), like(key_cache), like(value_cache),
            pltpu.VMEM((layers, batch, feat), f32),
            pltpu.VMEM((2, heads, side * span), f32),
            pltpu.VMEM((2, heads, hd), f32),
            pltpu.VMEM((2, heads, hd), f32),
            pltpu.VMEM((batch * 16, hd), f32),
            pltpu.VMEM((n - 1, 2, 16, hd), f32),
            pltpu.VMEM((layers, batch, span, hd), f32),
            pltpu.VMEM((layers, batch, span, hd), f32),
            pltpu.VMEM((layers, 2, side, span, hd), f32),
            pltpu.VMEM((layers, 2, side, span, hd), f32),
            pltpu.VMEM((2, side * span, hd), bf16),
            pltpu.VMEM((2, side * span, hd), bf16),
            pltpu.VMEM((n, 3 * heads, hd), f32),
            pltpu.VMEM((batch * heads, hd), f32),
            pltpu.VMEM((pieces, batch, feat // pieces), f32),
            pltpu.VMEM((2, pieces, tn - 1, batch, feat // pieces), f32),
            dma((6, layers)),
            dma((n - 1, 2)), dma((n - 1, 2)),
            dma((n - 1,)), dma((n - 1,)),
            dma((pieces, tn - 1)), dma((2, pieces, tn - 1)),
            dma((layers, 2, 2, side - 1)), dma((layers, 2, 2, side - 1)),
        ],
        compiler_params=pltpu.CompilerParams(
            collective_id=0, has_side_effects=True, vmem_limit_bytes=60 * 1024 * 1024),
    )(hidden, norm_gains, lengths, w_query, w_key, w_value, w_out, key_cache, value_cache)


def solution(mesh):
    sizes = (mesh.shape["ctx"], mesh.shape["tp"])
    return jax.shard_map(
        functools.partial(shards, sizes),
        mesh=mesh,
        in_specs=(
            P(None, "ctx"),
            P(None, "ctx"),
            P(None, "ctx", "tp"),
            P(None, "ctx", "tp"),
            P(None, "ctx", "tp"),
            P(None, "tp", "ctx"),
            P(None, None, "tp", "ctx", None),
            P(None, None, "tp", "ctx", None),
            P(),
        ),
        out_specs=P(None, "ctx"),
        check_vma=False,
    )
```

```python
import functools
import math

import jax
import jax.numpy as jnp
from jax import lax
from jax.experimental import pallas as pl
from jax.experimental.pallas import tpu as pltpu
from jax.sharding import PartitionSpec as P

mask_fill = -1e30
norm_eps = 1e-05
rope_base = 500000.0
MESH = pl.DeviceIdType.MESH
QROWS = 11


def kernel(dims, hidden_h, gains_h, lengths_h, wq_h, wk_h, wv_h, wo_h, kc_h, vc_h, out_ref,
           hidden_ref, gains_ref, lengths_ref, wq, wk, wv, wo, kc, vc, gain, bias, cosine, sine, qs, qr, kst, vst, krv, vrv, kb, vb,
           orr, cm, tps, tpr, w_sem, qs_sem, qr_sem, os_sem, or_sem, ts_sem, tr_sem, hs_sem, hr_sem, small_sem, ready):
    n, tn, side, layers, batch, feat, total, heads, hd, span = dims
    f32, bf16 = jnp.float32, jnp.bfloat16
    pieces = tps.shape[0]
    piece = feat // pieces
    scale = 1.0 / math.sqrt(hd)
    me = lax.axis_index("ctx")
    mt = lax.axis_index("tp")
    y, x = me // side, lax.rem(me, side)
    z, core = mt // 2, lax.rem(mt, 2)
    zn = tn // 2
    weights = ((kc_h, kc), (vc_h, vc), (wq_h, wq), (wk_h, wk), (wv_h, wv), (wo_h, wo))
    KC, VC, WQ, WK, WV, WO = range(6)

    def load(index, layer):
        source, target = weights[index]
        return pltpu.make_async_copy(source.at[layer], target.at[layer], w_sem.at[index, layer])

    def hops(step, size):
        return min(step, size - step)

    offsets = [(dy, dx) for dy in range(side) for dx in range(side) if (dy, dx) != (0, 0)]
    offsets.sort(key=lambda o: -(hops(o[0], side) + hops(o[1], side)))
    peers = []
    for dy, dx in offsets:
        py, px = lax.rem(y + dy, side), lax.rem(x + dx, side)
        peers.append((py * side + px, py, px))
    toffsets = [(dz, dc) for dz in range(zn) for dc in range(2) if (dz, dc) != (0, 0)]
    toffsets.sort(key=lambda o: -(2 * hops(o[0], zn) + o[1]))
    tpeers = [lax.rem(z + dz, zn) * 2 + lax.rem(core + dc, 2) for dz, dc in toffsets]

    column = [lax.rem(y + r, side) * side + x for r in range(1, side)]
    row = [y * side + lax.rem(x + r, side) for r in range(1, side)]
    barrier = pltpu.get_barrier_semaphore()
    for p in row + column:
        pl.semaphore_signal(barrier, inc=1, device_id={"ctx": p}, device_id_type=MESH)
    for p in tpeers:
        pl.semaphore_signal(barrier, inc=1, device_id={"tp": p}, device_id_type=MESH)

    smalls = [pltpu.make_async_copy(source, target, small_sem.at[i]) for i, (source, target) in enumerate(
        ((hidden_h, hidden_ref), (gains_h, gains_ref), (lengths_h, lengths_ref)))]
    for index in (KC, VC):
        load(index, 0).start()
    for c in smalls:
        c.start()
    for index in (WQ, WK, WV, WO):
        load(index, 0).start()
    for c in smalls:
        c.wait()

    half = hd // 2
    lane = lax.broadcasted_iota(jnp.int32, (heads, hd), 1)
    low = lane < half
    mine = (x, side + y)
    slot = lax.broadcasted_iota(jnp.int32, (heads, side * span), 1)
    block = slot // span
    positions = (y * side * span + slot, (block * side + x) * span + lax.rem(slot, span))
    exponent = jnp.where(low, lane, lane - half).astype(f32) * (2.0 / hd)
    frequency = jnp.exp(-exponent * math.log(rope_base))
    for g in range(2):
        size = lengths_ref[mine[g]]
        bias[g] = jnp.where(positions[g] < size, 0.0, mask_fill)
        angle = jnp.full((heads, hd), size, jnp.int32).astype(f32) * frequency
        cosine[g] = jnp.cos(angle)
        sine[g] = jnp.where(low, -jnp.sin(angle), jnp.sin(angle))
    for l in range(layers):
        gain[l] = jnp.broadcast_to(gains_ref[l:l + 1, :].astype(f32), (batch, feat))
    out_ref[...] = hidden_ref[...].astype(f32)
    own_mask = jnp.where(jnp.full((heads, 1), y, jnp.int32) == jnp.full((heads, 1), x, jnp.int32), 0.0, mask_fill)

    def ship(l):
        copies = []
        for r in range(1, side):
            px, py = lax.rem(x + r, side), lax.rem(y + r, side)
            for i, (source, target) in enumerate(((kst, krv), (vst, vrv))):
                copies.append(pltpu.make_async_remote_copy(
                    src_ref=source.at[l, px], dst_ref=target.at[l, 0, x],
                    send_sem=hs_sem.at[l, i, 0, r - 1], recv_sem=hr_sem.at[l, i, 0, r - 1],
                    device_id={"ctx": y * side + px}, device_id_type=MESH))
                copies.append(pltpu.make_async_remote_copy(
                    src_ref=source.at[l, side + py], dst_ref=target.at[l, 1, y],
                    send_sem=hs_sem.at[l, i, 1, r - 1], recv_sem=hr_sem.at[l, i, 1, r - 1],
                    device_id={"ctx": py * side + x}, device_id_type=MESH))
        return copies

    def stage(l):
        load(KC, l).wait()
        load(VC, l).wait()
        for source, staged, held in ((kc, kst, krv), (vc, vst, vrv)):
            for b in range(batch):
                staged[l, b] = source[l, b, 0].astype(f32)
            held[l, 0, x] = source[l, mine[0], 0].astype(f32)
            held[l, 1, y] = source[l, mine[1], 0].astype(f32)

    stage(0)
    pl.semaphore_wait(barrier, len(row) + len(column) + len(tpeers))
    for p in column:
        pl.semaphore_signal(ready, inc=1, device_id={"ctx": p}, device_id_type=MESH)
    for c in ship(0):
        c.start()
    pl.semaphore_wait(ready, len(column))

    def rotate(u, g):
        return u * cosine[g] + pltpu.roll(u, half, 1) * sine[g]

    def rounded(u):
        return u.astype(bf16).astype(f32)

    def layer_step(l, carry):
        stream = out_ref[...]
        scaled = (stream * gain[l]).astype(bf16)
        squares = jnp.sum(stream * stream, axis=1, keepdims=True)
        load(WQ, l).wait()
        load(WK, l).wait()
        load(WV, l).wait()

        @pl.when(l + 1 < layers)
        def _():
            for index in range(len(weights)):
                load(index, l + 1).start()

        def put(row, tile):
            qs[pl.ds(row, batch, stride=16), :] = tile

        put(heads, jnp.dot(scaled, wk[l], preferred_element_type=f32))
        put(heads + 1, jnp.dot(scaled, wv[l], preferred_element_type=f32))
        put(heads + 2, jnp.broadcast_to(squares, (batch, hd)))
        q = jnp.dot(scaled, wq[l], preferred_element_type=f32)
        for h in range(heads):
            put(h, q[:, h * hd:(h + 1) * hd])
        qc = []
        for k, (p, py, px) in enumerate(peers):
            for g, b in ((0, px), (1, side + py)):
                c = pltpu.make_async_remote_copy(
                    src_ref=qs.at[pl.ds(pl.multiple_of(b * 16, 16), QROWS)], dst_ref=qr.at[k, g, pl.ds(0, QROWS)],
                    send_sem=qs_sem.at[k, g], recv_sem=qr_sem.at[k, g],
                    device_id={"ctx": p}, device_id_type=MESH)
                c.start()
                qc.append(c)

        for c in ship(l):
            c.wait()
        for g in range(2):
            kb[g] = krv[l, g].reshape(side * span, hd).astype(bf16)
            vb[g] = vrv[l, g].reshape(side * span, hd).astype(bf16)

        for c in qc:
            c.wait_recv()
        stats = []
        for g in range(2):
            at = pl.multiple_of(mine[g] * 16, 16)
            whole = qs[pl.ds(at, heads), :]
            rest = qs[pl.ds(pl.multiple_of(at + 8, 8), QROWS - heads), :]
            for k in range(n - 1):
                whole = whole + qr[k, g, 0:heads]
                rest = rest + qr[k, g, heads:QROWS]
            inverse = lax.rsqrt(rest[2:3] / total + norm_eps)
            query = rounded(rotate(whole * inverse, g))
            new_key = rounded(rotate(jnp.broadcast_to(rest[0:1] * inverse, (heads, hd)), g))
            new_value = rounded(rest[1:2] * inverse)
            score = lax.dot_general(query.astype(bf16), kb[g], (((1,), (1,)), ((), ())), preferred_element_type=f32)
            own = jnp.sum(query * new_key, axis=1, keepdims=True) * scale + own_mask
            masked = score * scale + bias[g]
            top = jnp.maximum(jnp.max(masked, axis=1, keepdims=True), own)
            weight = jnp.exp(masked - top)
            fresh = jnp.exp(own - top)
            denominator = jnp.sum(weight, axis=1, keepdims=True) + fresh
            numerator = jnp.dot(weight.astype(bf16), vb[g], preferred_element_type=f32) + rounded(fresh) * new_value
            orr[me, g * heads:(g + 1) * heads, :] = numerator / denominator
            stats.append(top + jnp.log(denominator))
        orr[me, 2 * heads:3 * heads, :] = jnp.where(low, stats[0], stats[1])
        oc = []
        for k, (p, _, _) in enumerate(peers):
            c = pltpu.make_async_remote_copy(
                src_ref=orr.at[me], dst_ref=orr.at[me], send_sem=os_sem.at[k], recv_sem=or_sem.at[k],
                device_id={"ctx": p}, device_id_type=MESH)
            c.start()
            oc.append(c)

        @pl.when(l + 1 < layers)
        def _():
            stage(l + 1)

        load(WO, l).wait()
        for c in qc:
            c.wait_send()
        for c in oc:
            c.wait_recv()

        logs = [orr[c, 2 * heads:3 * heads, :] for c in range(n)]
        groups = [[[r * side + b for r in range(side)] for b in range(side)],
                  [[b * side + r for r in range(side)] for b in range(side)]]

        def over(values, op):
            return [[functools.reduce(op, [values[c] for c in group]) for group in part] for part in groups]

        def split(pair, c):
            return jnp.where(low, pair[0][c % side], pair[1][c // side])

        largest = over(logs, jnp.maximum)
        factors = [jnp.exp(logs[c] - split(largest, c)) for c in range(n)]
        sums = over(factors, jnp.add)
        inverses = [[1.0 / s for s in part] for part in sums]
        factors = [factors[c] * split(inverses, c) for c in range(n)]
        swapped = [pltpu.roll(f, half, 1) for f in factors]
        for g in range(2):
            for b, group in enumerate(groups[g]):
                merged = None
                for c in group:
                    factor = jnp.where(low, factors[c], swapped[c]) if g == 0 else jnp.where(low, swapped[c], factors[c])
                    term = orr[c, g * heads:(g + 1) * heads, :] * factor
                    merged = term if merged is None else merged + term
                at = (g * side + b) * heads
                cm[at:at + heads, :] = merged
        context = jnp.concatenate([cm[pl.ds(h, batch, stride=heads), :] for h in range(heads)], axis=1).astype(bf16)
        odd = lax.rem(l, 2)
        ts = []
        for i in range(pieces):
            cut = slice(i * piece, (i + 1) * piece)
            tps[i] = jnp.dot(context, wo[l, :, cut], preferred_element_type=f32)
            for k, p in enumerate(tpeers):
                c = pltpu.make_async_remote_copy(
                    src_ref=tps.at[i], dst_ref=tpr.at[odd, i, k], send_sem=ts_sem.at[i, k],
                    recv_sem=tr_sem.at[odd, i, k], device_id={"tp": p}, device_id_type=MESH)
                c.start()
                ts.append(c)
        @pl.when(l + 1 < layers)
        def _():
            for c in ship(l + 1):
                c.start()

        for c in oc:
            c.wait_send()
        for i in range(pieces):
            cut = slice(i * piece, (i + 1) * piece)
            moved = out_ref[:, cut] + tps[i]
            for k in range(tn - 1):
                ts[i * (tn - 1) + k].wait_recv()
                moved = moved + tpr[odd, i, k]
            out_ref[:, cut] = moved
        for c in ts:
            c.wait_send()
        return carry

    lax.fori_loop(0, layers, layer_step, 0)


def shards(sizes, hidden, norm_gains, w_query, w_key, w_value, w_out, key_cache, value_cache, lengths):
    n, tn = sizes
    layers, feat, columns = w_query.shape
    batch = hidden.shape[0]
    _, _, _, span, hd = key_cache.shape
    heads = columns // hd
    side = math.isqrt(n)
    dims = (n, tn, side, layers, batch, feat, feat * n, heads, hd, span)
    pieces = 2
    f32, bf16 = jnp.float32, jnp.bfloat16
    vmem = pl.BlockSpec(memory_space=pltpu.VMEM)
    far = pl.BlockSpec(memory_space=pl.ANY)

    def like(array):
        return pltpu.VMEM(array.shape, array.dtype)

    dma = pltpu.SemaphoreType.DMA
    return pl.pallas_call(
        functools.partial(kernel, dims),
        out_shape=pltpu.VMEM((batch, feat), f32),
        in_specs=[far] * 9,
        out_specs=vmem,
        scratch_shapes=[
            like(hidden), like(norm_gains), pltpu.SMEM(lengths.shape, lengths.dtype),
            like(w_query), like(w_key), like(w_value), like(w_out), like(key_cache), like(value_cache),
            pltpu.VMEM((layers, batch, feat), f32),
            pltpu.VMEM((2, heads, side * span), f32),
            pltpu.VMEM((2, heads, hd), f32),
            pltpu.VMEM((2, heads, hd), f32),
            pltpu.VMEM((batch * 16, hd), f32),
            pltpu.VMEM((n - 1, 2, 16, hd), f32),
            pltpu.VMEM((layers, batch, span, hd), f32),
            pltpu.VMEM((layers, batch, span, hd), f32),
            pltpu.VMEM((layers, 2, side, span, hd), f32),
            pltpu.VMEM((layers, 2, side, span, hd), f32),
            pltpu.VMEM((2, side * span, hd), bf16),
            pltpu.VMEM((2, side * span, hd), bf16),
            pltpu.VMEM((n, 3 * heads, hd), f32),
            pltpu.VMEM((batch * heads, hd), f32),
            pltpu.VMEM((pieces, batch, feat // pieces), f32),
            pltpu.VMEM((2, pieces, tn - 1, batch, feat // pieces), f32),
            dma((6, layers)),
            dma((n - 1, 2)), dma((n - 1, 2)),
            dma((n - 1,)), dma((n - 1,)),
            dma((pieces, tn - 1)), dma((2, pieces, tn - 1)),
            dma((layers, 2, 2, side - 1)), dma((layers, 2, 2, side - 1)),
            dma((3,)), pltpu.SemaphoreType.REGULAR,
        ],
        compiler_params=pltpu.CompilerParams(
            collective_id=0, has_side_effects=True, vmem_limit_bytes=60 * 1024 * 1024),
    )(hidden, norm_gains, lengths, w_query, w_key, w_value, w_out, key_cache, value_cache)


def solution(mesh):
    sizes = (mesh.shape["ctx"], mesh.shape["tp"])
    return jax.shard_map(
        functools.partial(shards, sizes),
        mesh=mesh,
        in_specs=(
            P(None, "ctx"),
            P(None, "ctx"),
            P(None, "ctx", "tp"),
            P(None, "ctx", "tp"),
            P(None, "ctx", "tp"),
            P(None, "tp", "ctx"),
            P(None, None, "tp", "ctx", None),
            P(None, None, "tp", "ctx", None),
            P(),
        ),
        out_specs=P(None, "ctx"),
        check_vma=False,
    )
```

```python
import functools
import math

import jax
import jax.numpy as jnp
from jax import lax
from jax.experimental import pallas as pl
from jax.experimental.pallas import tpu as pltpu
from jax.sharding import PartitionSpec as P

mask_fill = -1e30
norm_eps = 1e-05
rope_base = 500000.0
MESH = pl.DeviceIdType.MESH
QROWS = 11


def kernel(dims, hidden_h, gains_h, lengths_h, wq_h, wk_h, wv_h, wo_h, kc_h, vc_h, out_ref,
           hidden_ref, gains_ref, lengths_ref, wq, wk, wv, wo, kc, vc, gain, bias, cosine, sine, qs, qr, kst, vst, krv, vrv, kb, vb,
           orr, cm, tps, tpr, w_sem, qs_sem, qr_sem, os_sem, or_sem, ts_sem, tr_sem, hs_sem, hr_sem, small_sem, ready):
    n, tn, side, layers, batch, feat, total, heads, hd, span = dims
    f32, bf16 = jnp.float32, jnp.bfloat16
    pieces = tps.shape[0]
    piece = feat // pieces
    scale = 1.0 / math.sqrt(hd)
    me = lax.axis_index("ctx")
    mt = lax.axis_index("tp")
    y, x = me // side, lax.rem(me, side)
    z, core = mt // 2, lax.rem(mt, 2)
    zn = tn // 2
    weights = ((kc_h, kc), (vc_h, vc), (wq_h, wq), (wk_h, wk), (wv_h, wv), (wo_h, wo))
    KC, VC, WQ, WK, WV, WO = range(6)

    def load(index, layer):
        source, target = weights[index]
        return pltpu.make_async_copy(source.at[layer], target.at[layer], w_sem.at[index, layer])

    def hops(step, size):
        return min(step, size - step)

    offsets = [(dy, dx) for dy in range(side) for dx in range(side) if (dy, dx) != (0, 0)]
    offsets.sort(key=lambda o: -(hops(o[0], side) + hops(o[1], side)))
    peers = []
    for dy, dx in offsets:
        py, px = lax.rem(y + dy, side), lax.rem(x + dx, side)
        peers.append((py * side + px, py, px))
    toffsets = [(dz, dc) for dz in range(zn) for dc in range(2) if (dz, dc) != (0, 0)]
    toffsets.sort(key=lambda o: -(2 * hops(o[0], zn) + o[1]))
    tpeers = [lax.rem(z + dz, zn) * 2 + lax.rem(core + dc, 2) for dz, dc in toffsets]

    column = [lax.rem(y + r, side) * side + x for r in range(1, side)]
    row = [y * side + lax.rem(x + r, side) for r in range(1, side)]
    barrier = pltpu.get_barrier_semaphore()
    for p in row + column:
        pl.semaphore_signal(barrier, inc=1, device_id={"ctx": p}, device_id_type=MESH)
    for p in tpeers:
        pl.semaphore_signal(barrier, inc=1, device_id={"tp": p}, device_id_type=MESH)

    smalls = [pltpu.make_async_copy(source, target, small_sem.at[i]) for i, (source, target) in enumerate(
        ((hidden_h, hidden_ref), (gains_h, gains_ref), (lengths_h, lengths_ref)))]
    for index in (KC, VC):
        load(index, 0).start()
    for c in smalls:
        c.start()
    for index in (WQ, WK, WV, WO):
        load(index, 0).start()
    for c in smalls:
        c.wait()

    half = hd // 2
    lane = lax.broadcasted_iota(jnp.int32, (heads, hd), 1)
    low = lane < half
    mine = (x, side + y)
    slot = lax.broadcasted_iota(jnp.int32, (heads, side * span), 1)
    block = slot // span
    positions = (y * side * span + slot, (block * side + x) * span + lax.rem(slot, span))
    exponent = jnp.where(low, lane, lane - half).astype(f32) * (2.0 / hd)
    frequency = jnp.exp(-exponent * math.log(rope_base))
    for g in range(2):
        size = lengths_ref[mine[g]]
        bias[g] = jnp.where(positions[g] < size, 0.0, mask_fill)
        angle = jnp.full((heads, hd), size, jnp.int32).astype(f32) * frequency
        cosine[g] = jnp.cos(angle)
        sine[g] = jnp.where(low, -jnp.sin(angle), jnp.sin(angle))
    for l in range(layers):
        gain[l] = jnp.broadcast_to(gains_ref[l:l + 1, :].astype(f32), (batch, feat))
    out_ref[...] = hidden_ref[...].astype(f32)
    own_mask = jnp.where(jnp.full((heads, 1), y, jnp.int32) == jnp.full((heads, 1), x, jnp.int32), 0.0, mask_fill)

    def ship(l):
        copies = []
        for r in (2, 1, 3):
            px, py = lax.rem(x + r, side), lax.rem(y + r, side)
            for i, (source, target) in enumerate(((kst, krv), (vst, vrv))):
                copies.append(pltpu.make_async_remote_copy(
                    src_ref=source.at[l, px], dst_ref=target.at[l, 0, x],
                    send_sem=hs_sem.at[l, i, 0, r - 1], recv_sem=hr_sem.at[l, i, 0, r - 1],
                    device_id={"ctx": y * side + px}, device_id_type=MESH))
                copies.append(pltpu.make_async_remote_copy(
                    src_ref=source.at[l, side + py], dst_ref=target.at[l, 1, y],
                    send_sem=hs_sem.at[l, i, 1, r - 1], recv_sem=hr_sem.at[l, i, 1, r - 1],
                    device_id={"ctx": py * side + x}, device_id_type=MESH))
        return copies

    def stage(l):
        load(KC, l).wait()
        load(VC, l).wait()
        for source, staged, held in ((kc, kst, krv), (vc, vst, vrv)):
            for b in range(batch):
                staged[l, b] = source[l, b, 0].astype(f32)
            held[l, 0, x] = source[l, mine[0], 0].astype(f32)
            held[l, 1, y] = source[l, mine[1], 0].astype(f32)

    stage(0)
    pl.semaphore_wait(barrier, len(row) + len(column) + len(tpeers))
    for p in column:
        pl.semaphore_signal(ready, inc=1, device_id={"ctx": p}, device_id_type=MESH)
    for c in ship(0):
        c.start()
    pl.semaphore_wait(ready, len(column))

    def rotate(u, g):
        return u * cosine[g] + pltpu.roll(u, half, 1) * sine[g]

    def rounded(u):
        return u.astype(bf16).astype(f32)

    def layer_step(l, carry):
        stream = out_ref[...]
        scaled = (stream * gain[l]).astype(bf16)
        squares = jnp.sum(stream * stream, axis=1, keepdims=True)
        load(WQ, l).wait()
        load(WK, l).wait()
        load(WV, l).wait()

        @pl.when(l + 1 < layers)
        def _():
            for index in range(len(weights)):
                load(index, l + 1).start()

        def put(row, tile):
            qs[pl.ds(row, batch, stride=16), :] = tile

        put(heads, jnp.dot(scaled, wk[l], preferred_element_type=f32))
        put(heads + 1, jnp.dot(scaled, wv[l], preferred_element_type=f32))
        put(heads + 2, jnp.broadcast_to(squares, (batch, hd)))
        q = jnp.dot(scaled, wq[l], preferred_element_type=f32)
        for h in range(heads):
            put(h, q[:, h * hd:(h + 1) * hd])
        qc = []
        for k, (p, py, px) in enumerate(peers):
            for g, b in ((0, px), (1, side + py)):
                c = pltpu.make_async_remote_copy(
                    src_ref=qs.at[pl.ds(pl.multiple_of(b * 16, 16), QROWS)], dst_ref=qr.at[k, g, pl.ds(0, QROWS)],
                    send_sem=qs_sem.at[k, g], recv_sem=qr_sem.at[k, g],
                    device_id={"ctx": p}, device_id_type=MESH)
                c.start()
                qc.append(c)

        for c in ship(l):
            c.wait()
        for g in range(2):
            kb[g] = krv[l, g].reshape(side * span, hd).astype(bf16)
            vb[g] = vrv[l, g].reshape(side * span, hd).astype(bf16)

        for c in qc:
            c.wait_recv()
        stats = []
        for g in range(2):
            at = pl.multiple_of(mine[g] * 16, 16)
            whole = qs[pl.ds(at, heads), :]
            rest = qs[pl.ds(pl.multiple_of(at + 8, 8), QROWS - heads), :]
            for k in range(n - 1):
                whole = whole + qr[k, g, 0:heads]
                rest = rest + qr[k, g, heads:QROWS]
            inverse = lax.rsqrt(rest[2:3] / total + norm_eps)
            query = rounded(rotate(whole * inverse, g))
            new_key = rounded(rotate(jnp.broadcast_to(rest[0:1] * inverse, (heads, hd)), g))
            new_value = rounded(rest[1:2] * inverse)
            score = lax.dot_general(query.astype(bf16), kb[g], (((1,), (1,)), ((), ())), preferred_element_type=f32)
            own = jnp.sum(query * new_key, axis=1, keepdims=True) * scale + own_mask
            masked = score * scale + bias[g]
            top = jnp.maximum(jnp.max(masked, axis=1, keepdims=True), own)
            weight = jnp.exp(masked - top)
            fresh = jnp.exp(own - top)
            denominator = jnp.sum(weight, axis=1, keepdims=True) + fresh
            numerator = jnp.dot(weight.astype(bf16), vb[g], preferred_element_type=f32) + rounded(fresh) * new_value
            orr[me, g * heads:(g + 1) * heads, :] = numerator / denominator
            stats.append(top + jnp.log(denominator))
        orr[me, 2 * heads:3 * heads, :] = jnp.where(low, stats[0], stats[1])
        oc = []
        for k, (p, _, _) in enumerate(peers):
            c = pltpu.make_async_remote_copy(
                src_ref=orr.at[me], dst_ref=orr.at[me], send_sem=os_sem.at[k], recv_sem=or_sem.at[k],
                device_id={"ctx": p}, device_id_type=MESH)
            c.start()
            oc.append(c)

        @pl.when(l + 1 < layers)
        def _():
            stage(l + 1)

        load(WO, l).wait()
        for c in qc:
            c.wait_send()
        for c in oc:
            c.wait_recv()

        @pl.when(l + 1 < layers)
        def _():
            for c in ship(l + 1):
                c.start()

        logs = [orr[c, 2 * heads:3 * heads, :] for c in range(n)]
        groups = [[[r * side + b for r in range(side)] for b in range(side)],
                  [[b * side + r for r in range(side)] for b in range(side)]]

        def over(values, op):
            return [[functools.reduce(op, [values[c] for c in group]) for group in part] for part in groups]

        def split(pair, c):
            return jnp.where(low, pair[0][c % side], pair[1][c // side])

        largest = over(logs, jnp.maximum)
        factors = [jnp.exp(logs[c] - split(largest, c)) for c in range(n)]
        sums = over(factors, jnp.add)
        inverses = [[1.0 / s for s in part] for part in sums]
        factors = [factors[c] * split(inverses, c) for c in range(n)]
        swapped = [pltpu.roll(f, half, 1) for f in factors]
        for g in range(2):
            for b, group in enumerate(groups[g]):
                merged = None
                for c in group:
                    factor = jnp.where(low, factors[c], swapped[c]) if g == 0 else jnp.where(low, swapped[c], factors[c])
                    term = orr[c, g * heads:(g + 1) * heads, :] * factor
                    merged = term if merged is None else merged + term
                at = (g * side + b) * heads
                cm[at:at + heads, :] = merged
        context = jnp.concatenate([cm[pl.ds(h, batch, stride=heads), :] for h in range(heads)], axis=1).astype(bf16)
        odd = lax.rem(l, 2)
        ts = []
        for i in range(pieces):
            cut = slice(i * piece, (i + 1) * piece)
            tps[i] = jnp.dot(context, wo[l, :, cut], preferred_element_type=f32)
            for k, p in enumerate(tpeers):
                c = pltpu.make_async_remote_copy(
                    src_ref=tps.at[i], dst_ref=tpr.at[odd, i, k], send_sem=ts_sem.at[i, k],
                    recv_sem=tr_sem.at[odd, i, k], device_id={"tp": p}, device_id_type=MESH)
                c.start()
                ts.append(c)
        for c in oc:
            c.wait_send()
        for i in range(pieces):
            cut = slice(i * piece, (i + 1) * piece)
            moved = out_ref[:, cut] + tps[i]
            for k in range(tn - 1):
                ts[i * (tn - 1) + k].wait_recv()
                moved = moved + tpr[odd, i, k]
            out_ref[:, cut] = moved
        for c in ts:
            c.wait_send()
        return carry

    lax.fori_loop(0, layers, layer_step, 0)


def shards(sizes, hidden, norm_gains, w_query, w_key, w_value, w_out, key_cache, value_cache, lengths):
    n, tn = sizes
    layers, feat, columns = w_query.shape
    batch = hidden.shape[0]
    _, _, _, span, hd = key_cache.shape
    heads = columns // hd
    side = math.isqrt(n)
    dims = (n, tn, side, layers, batch, feat, feat * n, heads, hd, span)
    pieces = 2
    f32, bf16 = jnp.float32, jnp.bfloat16
    vmem = pl.BlockSpec(memory_space=pltpu.VMEM)
    far = pl.BlockSpec(memory_space=pl.ANY)

    def like(array):
        return pltpu.VMEM(array.shape, array.dtype)

    dma = pltpu.SemaphoreType.DMA
    return pl.pallas_call(
        functools.partial(kernel, dims),
        out_shape=pltpu.VMEM((batch, feat), f32),
        in_specs=[far] * 9,
        out_specs=vmem,
        scratch_shapes=[
            like(hidden), like(norm_gains), pltpu.SMEM(lengths.shape, lengths.dtype),
            like(w_query), like(w_key), like(w_value), like(w_out), like(key_cache), like(value_cache),
            pltpu.VMEM((layers, batch, feat), f32),
            pltpu.VMEM((2, heads, side * span), f32),
            pltpu.VMEM((2, heads, hd), f32),
            pltpu.VMEM((2, heads, hd), f32),
            pltpu.VMEM((batch * 16, hd), f32),
            pltpu.VMEM((n - 1, 2, 16, hd), f32),
            pltpu.VMEM((layers, batch, span, hd), f32),
            pltpu.VMEM((layers, batch, span, hd), f32),
            pltpu.VMEM((layers, 2, side, span, hd), f32),
            pltpu.VMEM((layers, 2, side, span, hd), f32),
            pltpu.VMEM((2, side * span, hd), bf16),
            pltpu.VMEM((2, side * span, hd), bf16),
            pltpu.VMEM((n, 3 * heads, hd), f32),
            pltpu.VMEM((batch * heads, hd), f32),
            pltpu.VMEM((pieces, batch, feat // pieces), f32),
            pltpu.VMEM((2, pieces, tn - 1, batch, feat // pieces), f32),
            dma((6, layers)),
            dma((n - 1, 2)), dma((n - 1, 2)),
            dma((n - 1,)), dma((n - 1,)),
            dma((pieces, tn - 1)), dma((2, pieces, tn - 1)),
            dma((layers, 2, 2, side - 1)), dma((layers, 2, 2, side - 1)),
            dma((3,)), pltpu.SemaphoreType.REGULAR,
        ],
        compiler_params=pltpu.CompilerParams(
            collective_id=0, has_side_effects=True, vmem_limit_bytes=60 * 1024 * 1024),
    )(hidden, norm_gains, lengths, w_query, w_key, w_value, w_out, key_cache, value_cache)


def solution(mesh):
    sizes = (mesh.shape["ctx"], mesh.shape["tp"])
    return jax.shard_map(
        functools.partial(shards, sizes),
        mesh=mesh,
        in_specs=(
            P(None, "ctx"),
            P(None, "ctx"),
            P(None, "ctx", "tp"),
            P(None, "ctx", "tp"),
            P(None, "ctx", "tp"),
            P(None, "tp", "ctx"),
            P(None, None, "tp", "ctx", None),
            P(None, None, "tp", "ctx", None),
            P(),
        ),
        out_specs=P(None, "ctx"),
        check_vma=False,
    )
```

```python
import functools
import math

import jax
import jax.numpy as jnp
from jax import lax
from jax.experimental import pallas as pl
from jax.experimental.pallas import tpu as pltpu
from jax.sharding import PartitionSpec as P

mask_fill = -1e30
norm_eps = 1e-05
rope_base = 500000.0
MESH = pl.DeviceIdType.MESH
QROWS = 9


def kernel(dims, hidden_h, gains_h, lengths_h, wq_h, wk_h, wv_h, wo_h, kc_h, vc_h, out_ref,
           hidden_ref, gains_ref, lengths_ref, wq, wk, wv, wo, kc, vc, gain, bias, cosine, sine, qs, qr, ks, kr, fresh_sum, kst, vst, krv, vrv, kb, vb,
           orr, cm, tps, tpr, w_sem, qs_sem, qr_sem, ks_sem, kr_sem, os_sem, or_sem, ts_sem, tr_sem, hs_sem, hr_sem, small_sem, ready):
    n, tn, side, layers, batch, feat, total, heads, hd, span = dims
    f32, bf16 = jnp.float32, jnp.bfloat16
    pieces = tps.shape[0]
    piece = feat // pieces
    scale = 1.0 / math.sqrt(hd)
    me = lax.axis_index("ctx")
    mt = lax.axis_index("tp")
    y, x = me // side, lax.rem(me, side)
    z, core = mt // 2, lax.rem(mt, 2)
    zn = tn // 2
    weights = ((kc_h, kc), (vc_h, vc), (wq_h, wq), (wk_h, wk), (wv_h, wv), (wo_h, wo))
    KC, VC, WQ, WK, WV, WO = range(6)

    def load(index, layer):
        source, target = weights[index]
        return pltpu.make_async_copy(source.at[layer], target.at[layer], w_sem.at[index, layer])

    def hops(step, size):
        return min(step, size - step)

    offsets = [(dy, dx) for dy in range(side) for dx in range(side) if (dy, dx) != (0, 0)]
    offsets.sort(key=lambda o: -(hops(o[0], side) + hops(o[1], side)))
    peers = []
    for dy, dx in offsets:
        py, px = lax.rem(y + dy, side), lax.rem(x + dx, side)
        peers.append((py * side + px, py, px))
    toffsets = [(dz, dc) for dz in range(zn) for dc in range(2) if (dz, dc) != (0, 0)]
    toffsets.sort(key=lambda o: -(2 * hops(o[0], zn) + o[1]))
    tpeers = [lax.rem(z + dz, zn) * 2 + lax.rem(core + dc, 2) for dz, dc in toffsets]

    column = [lax.rem(y + r, side) * side + x for r in range(1, side)]
    row = [y * side + lax.rem(x + r, side) for r in range(1, side)]
    barrier = pltpu.get_barrier_semaphore()
    for p in row + column:
        pl.semaphore_signal(barrier, inc=1, device_id={"ctx": p}, device_id_type=MESH)
    for p in tpeers:
        pl.semaphore_signal(barrier, inc=1, device_id={"tp": p}, device_id_type=MESH)

    smalls = [pltpu.make_async_copy(source, target, small_sem.at[i]) for i, (source, target) in enumerate(
        ((hidden_h, hidden_ref), (gains_h, gains_ref), (lengths_h, lengths_ref)))]
    for index in (KC, VC):
        load(index, 0).start()
    for c in smalls:
        c.start()
    for index in (WQ, WK, WV, WO):
        load(index, 0).start()
    for c in smalls:
        c.wait()

    half = hd // 2
    lane = lax.broadcasted_iota(jnp.int32, (heads, hd), 1)
    low = lane < half
    mine = (x, side + y)
    slot = lax.broadcasted_iota(jnp.int32, (heads, side * span), 1)
    block = slot // span
    positions = (y * side * span + slot, (block * side + x) * span + lax.rem(slot, span))
    exponent = jnp.where(low, lane, lane - half).astype(f32) * (2.0 / hd)
    frequency = jnp.exp(-exponent * math.log(rope_base))
    for g in range(2):
        size = lengths_ref[mine[g]]
        bias[g] = jnp.where(positions[g] < size, 0.0, mask_fill)
        angle = jnp.full((heads, hd), size, jnp.int32).astype(f32) * frequency
        cosine[g] = jnp.cos(angle)
        sine[g] = jnp.where(low, -jnp.sin(angle), jnp.sin(angle))
    for l in range(layers):
        gain[l] = jnp.broadcast_to(gains_ref[l:l + 1, :].astype(f32), (batch, feat))
    out_ref[...] = hidden_ref[...].astype(f32)
    own_mask = jnp.where(jnp.full((heads, 1), y, jnp.int32) == jnp.full((heads, 1), x, jnp.int32), 0.0, mask_fill)

    def ship(l):
        copies = []
        for r in (2, 1, 3):
            px, py = lax.rem(x + r, side), lax.rem(y + r, side)
            for i, (source, target) in enumerate(((kst, krv), (vst, vrv))):
                copies.append(pltpu.make_async_remote_copy(
                    src_ref=source.at[l, px], dst_ref=target.at[l, 0, x],
                    send_sem=hs_sem.at[l, i, 0, r - 1], recv_sem=hr_sem.at[l, i, 0, r - 1],
                    device_id={"ctx": y * side + px}, device_id_type=MESH))
                copies.append(pltpu.make_async_remote_copy(
                    src_ref=source.at[l, side + py], dst_ref=target.at[l, 1, y],
                    send_sem=hs_sem.at[l, i, 1, r - 1], recv_sem=hr_sem.at[l, i, 1, r - 1],
                    device_id={"ctx": py * side + x}, device_id_type=MESH))
        return copies

    def stage(l):
        load(KC, l).wait()
        load(VC, l).wait()
        for source, staged, held in ((kc, kst, krv), (vc, vst, vrv)):
            for b in range(batch):
                staged[l, b] = source[l, b, 0].astype(f32)
            held[l, 0, x] = source[l, mine[0], 0].astype(f32)
            held[l, 1, y] = source[l, mine[1], 0].astype(f32)

    def fresh_copy(d):
        return pltpu.make_async_remote_copy(
            src_ref=ks.at[pl.ds(8 * d, 4)], dst_ref=kr.at[me], send_sem=ks_sem.at[d], recv_sem=kr_sem,
            device_id={"ctx": d * side + d}, device_id_type=MESH)

    fresh_sum[...] = jnp.zeros_like(fresh_sum)
    stage(0)
    pl.semaphore_wait(barrier, len(row) + len(column) + len(tpeers))
    for p in column:
        pl.semaphore_signal(ready, inc=1, device_id={"ctx": p}, device_id_type=MESH)
    for c in ship(0):
        c.start()
    pl.semaphore_wait(ready, len(column))

    def rotate(u, g):
        return u * cosine[g] + pltpu.roll(u, half, 1) * sine[g]

    def rounded(u):
        return u.astype(bf16).astype(f32)

    def layer_step(l, carry):
        stream = out_ref[...]
        scaled = (stream * gain[l]).astype(bf16)
        squares = jnp.sum(stream * stream, axis=1, keepdims=True)
        load(WQ, l).wait()
        load(WK, l).wait()
        load(WV, l).wait()

        @pl.when(l + 1 < layers)
        def _():
            for index in range(len(weights)):
                load(index, l + 1).start()

        def put(row, tile):
            qs[pl.ds(row, batch, stride=16), :] = tile

        for i, w in enumerate((wk, wv)):
            kv = jnp.dot(scaled, w[l], preferred_element_type=f32)
            for g in range(2):
                ks[pl.ds(2 * g + i, side, stride=8), :] = kv[g * side:(g + 1) * side]
        for d in range(side):
            @pl.when(me != d * side + d)
            def _():
                fresh_copy(d).start()

        put(heads, jnp.broadcast_to(squares, (batch, hd)))
        q = jnp.dot(scaled, wq[l], preferred_element_type=f32)
        for h in range(heads):
            put(h, q[:, h * hd:(h + 1) * hd])
        qc = []
        for k, (p, py, px) in enumerate(peers):
            for g, b in ((0, px), (1, side + py)):
                c = pltpu.make_async_remote_copy(
                    src_ref=qs.at[pl.ds(pl.multiple_of(b * 16, 16), QROWS)], dst_ref=qr.at[k, g, pl.ds(0, QROWS)],
                    send_sem=qs_sem.at[k, g], recv_sem=qr_sem.at[k, g],
                    device_id={"ctx": p}, device_id_type=MESH)
                c.start()
                qc.append(c)
        for c in ship(l):
            c.wait()
        for g in range(2):
            kb[g] = krv[l, g].reshape(side * span, hd).astype(bf16)
            vb[g] = vrv[l, g].reshape(side * span, hd).astype(bf16)

        @pl.when(y == x)
        def _():
            kr[me] = ks[pl.ds(pl.multiple_of(8 * x, 8), 4), :]
            pltpu.make_async_copy(kr.at[pl.ds(0, n - 1)], kr.at[pl.ds(0, n - 1)], kr_sem).wait()
            fresh_sum[...] = functools.reduce(jnp.add, [kr[c] for c in range(n)])

        for c in qc:
            c.wait_recv()
        stats = []
        for g in range(2):
            at = pl.multiple_of(mine[g] * 16, 16)
            whole = qs[pl.ds(at, heads), :]
            square = qs[pl.ds(pl.multiple_of(at + 8, 8), 1), :]
            for k in range(n - 1):
                whole = whole + qr[k, g, 0:heads]
                square = square + qr[k, g, heads:QROWS]
            inverse = lax.rsqrt(square / total + norm_eps)
            query = rounded(rotate(whole * inverse, g))
            score = lax.dot_general(query.astype(bf16), kb[g], (((1,), (1,)), ((), ())), preferred_element_type=f32)
            new_key = rounded(rotate(jnp.broadcast_to(fresh_sum[2 * g:2 * g + 1] * inverse, (heads, hd)), g))
            new_value = rounded(fresh_sum[2 * g + 1:2 * g + 2] * inverse)
            own = jnp.sum(query * new_key, axis=1, keepdims=True) * scale + own_mask
            masked = score * scale + bias[g]
            top = jnp.maximum(jnp.max(masked, axis=1, keepdims=True), own)
            weight = jnp.exp(masked - top)
            fresh = jnp.exp(own - top)
            denominator = jnp.sum(weight, axis=1, keepdims=True) + fresh
            numerator = jnp.dot(weight.astype(bf16), vb[g], preferred_element_type=f32) + rounded(fresh) * new_value
            orr[me, g * heads:(g + 1) * heads, :] = numerator / denominator
            stats.append(top + jnp.log(denominator))
        orr[me, 2 * heads:3 * heads, :] = jnp.where(low, stats[0], stats[1])
        oc = []
        for k, (p, _, _) in enumerate(peers):
            c = pltpu.make_async_remote_copy(
                src_ref=orr.at[me], dst_ref=orr.at[me], send_sem=os_sem.at[k], recv_sem=or_sem.at[k],
                device_id={"ctx": p}, device_id_type=MESH)
            c.start()
            oc.append(c)

        @pl.when(l + 1 < layers)
        def _():
            stage(l + 1)

        load(WO, l).wait()
        for c in qc:
            c.wait_send()
        for d in range(side):
            @pl.when(me != d * side + d)
            def _():
                fresh_copy(d).wait_send()
        for c in oc:
            c.wait_recv()

        @pl.when(l + 1 < layers)
        def _():
            for c in ship(l + 1):
                c.start()

        logs = [orr[c, 2 * heads:3 * heads, :] for c in range(n)]
        groups = [[[r * side + b for r in range(side)] for b in range(side)],
                  [[b * side + r for r in range(side)] for b in range(side)]]

        def over(values, op):
            return [[functools.reduce(op, [values[c] for c in group]) for group in part] for part in groups]

        def split(pair, c):
            return jnp.where(low, pair[0][c % side], pair[1][c // side])

        largest = over(logs, jnp.maximum)
        factors = [jnp.exp(logs[c] - split(largest, c)) for c in range(n)]
        sums = over(factors, jnp.add)
        inverses = [[1.0 / s for s in part] for part in sums]
        factors = [factors[c] * split(inverses, c) for c in range(n)]
        swapped = [pltpu.roll(f, half, 1) for f in factors]
        for g in range(2):
            for b, group in enumerate(groups[g]):
                merged = None
                for c in group:
                    factor = jnp.where(low, factors[c], swapped[c]) if g == 0 else jnp.where(low, swapped[c], factors[c])
                    term = orr[c, g * heads:(g + 1) * heads, :] * factor
                    merged = term if merged is None else merged + term
                at = (g * side + b) * heads
                cm[at:at + heads, :] = merged
        context = jnp.concatenate([cm[pl.ds(h, batch, stride=heads), :] for h in range(heads)], axis=1).astype(bf16)
        odd = lax.rem(l, 2)
        ts = []
        for i in range(pieces):
            cut = slice(i * piece, (i + 1) * piece)
            tps[i] = jnp.dot(context, wo[l, :, cut], preferred_element_type=f32)
            for k, p in enumerate(tpeers):
                c = pltpu.make_async_remote_copy(
                    src_ref=tps.at[i], dst_ref=tpr.at[odd, i, k], send_sem=ts_sem.at[i, k],
                    recv_sem=tr_sem.at[odd, i, k], device_id={"tp": p}, device_id_type=MESH)
                c.start()
                ts.append(c)
        for c in oc:
            c.wait_send()
        for i in range(pieces):
            cut = slice(i * piece, (i + 1) * piece)
            moved = out_ref[:, cut] + tps[i]
            for k in range(tn - 1):
                ts[i * (tn - 1) + k].wait_recv()
                moved = moved + tpr[odd, i, k]
            out_ref[:, cut] = moved
        for c in ts:
            c.wait_send()
        return carry

    lax.fori_loop(0, layers, layer_step, 0)


def shards(sizes, hidden, norm_gains, w_query, w_key, w_value, w_out, key_cache, value_cache, lengths):
    n, tn = sizes
    layers, feat, columns = w_query.shape
    batch = hidden.shape[0]
    _, _, _, span, hd = key_cache.shape
    heads = columns // hd
    side = math.isqrt(n)
    dims = (n, tn, side, layers, batch, feat, feat * n, heads, hd, span)
    pieces = 1
    f32, bf16 = jnp.float32, jnp.bfloat16
    vmem = pl.BlockSpec(memory_space=pltpu.VMEM)
    far = pl.BlockSpec(memory_space=pl.ANY)

    def like(array):
        return pltpu.VMEM(array.shape, array.dtype)

    dma = pltpu.SemaphoreType.DMA
    return pl.pallas_call(
        functools.partial(kernel, dims),
        out_shape=pltpu.VMEM((batch, feat), f32),
        in_specs=[far] * 9,
        out_specs=vmem,
        scratch_shapes=[
            like(hidden), like(norm_gains), pltpu.SMEM(lengths.shape, lengths.dtype),
            like(w_query), like(w_key), like(w_value), like(w_out), like(key_cache), like(value_cache),
            pltpu.VMEM((layers, batch, feat), f32),
            pltpu.VMEM((2, heads, side * span), f32),
            pltpu.VMEM((2, heads, hd), f32),
            pltpu.VMEM((2, heads, hd), f32),
            pltpu.VMEM((batch * 16, hd), f32),
            pltpu.VMEM((n - 1, 2, 16, hd), f32),
            pltpu.VMEM((side * 8, hd), f32),
            pltpu.VMEM((n, 4, hd), f32),
            pltpu.VMEM((4, hd), f32),
            pltpu.VMEM((layers, batch, span, hd), f32),
            pltpu.VMEM((layers, batch, span, hd), f32),
            pltpu.VMEM((layers, 2, side, span, hd), f32),
            pltpu.VMEM((layers, 2, side, span, hd), f32),
            pltpu.VMEM((2, side * span, hd), bf16),
            pltpu.VMEM((2, side * span, hd), bf16),
            pltpu.VMEM((n, 3 * heads, hd), f32),
            pltpu.VMEM((batch * heads, hd), f32),
            pltpu.VMEM((pieces, batch, feat // pieces), f32),
            pltpu.VMEM((2, pieces, tn - 1, batch, feat // pieces), f32),
            dma((6, layers)),
            dma((n - 1, 2)), dma((n - 1, 2)),
            dma((side,)), dma(()),
            dma((n - 1,)), dma((n - 1,)),
            dma((pieces, tn - 1)), dma((2, pieces, tn - 1)),
            dma((layers, 2, 2, side - 1)), dma((layers, 2, 2, side - 1)),
            dma((3,)), pltpu.SemaphoreType.REGULAR,
        ],
        compiler_params=pltpu.CompilerParams(
            collective_id=0, has_side_effects=True, vmem_limit_bytes=60 * 1024 * 1024),
    )(hidden, norm_gains, lengths, w_query, w_key, w_value, w_out, key_cache, value_cache)


def solution(mesh):
    sizes = (mesh.shape["ctx"], mesh.shape["tp"])
    return jax.shard_map(
        functools.partial(shards, sizes),
        mesh=mesh,
        in_specs=(
            P(None, "ctx"),
            P(None, "ctx"),
            P(None, "ctx", "tp"),
            P(None, "ctx", "tp"),
            P(None, "ctx", "tp"),
            P(None, "tp", "ctx"),
            P(None, None, "tp", "ctx", None),
            P(None, None, "tp", "ctx", None),
            P(),
        ),
        out_specs=P(None, "ctx"),
        check_vma=False,
    )
```

```python
import functools
import math

import jax
import jax.numpy as jnp
from jax import lax
from jax.experimental import pallas as pl
from jax.experimental.pallas import tpu as pltpu
from jax.sharding import PartitionSpec as P

mask_fill = -1e30
norm_eps = 1e-05
rope_base = 500000.0
MESH = pl.DeviceIdType.MESH
QROWS = 9


def kernel(dims, hidden_h, gains_h, lengths_h, wq_h, wk_h, wv_h, wo_h, kc_h, vc_h, out_ref,
           hidden_ref, gains_ref, lengths_ref, wq, wk, wv, wo, kc, vc, gain, bias, cosine, sine, qs, qr, ks, kr, fresh_sum, kst, vst, krv, vrv, kb, vb,
           orr, od, cm, tps, tpr, w_sem, qs_sem, qr_sem, ks_sem, kr_sem, os_sem, or_sem, ts_sem, tr_sem, hs_sem, hr_sem, small_sem, ready):
    n, tn, side, layers, batch, feat, total, heads, hd, span = dims
    f32, bf16 = jnp.float32, jnp.bfloat16
    pieces = tps.shape[0]
    piece = feat // pieces
    scale = 1.0 / math.sqrt(hd)
    me = lax.axis_index("ctx")
    mt = lax.axis_index("tp")
    y, x = me // side, lax.rem(me, side)
    z, core = mt // 2, lax.rem(mt, 2)
    zn = tn // 2
    weights = ((kc_h, kc), (vc_h, vc), (wq_h, wq), (wk_h, wk), (wv_h, wv), (wo_h, wo))
    KC, VC, WQ, WK, WV, WO = range(6)

    def load(index, layer):
        source, target = weights[index]
        return pltpu.make_async_copy(source.at[layer], target.at[layer], w_sem.at[index, layer])

    def hops(step, size):
        return min(step, size - step)

    offsets = [(dy, dx) for dy in range(side) for dx in range(side) if (dy, dx) != (0, 0)]
    offsets.sort(key=lambda o: -(hops(o[0], side) + hops(o[1], side)))
    peers = []
    for dy, dx in offsets:
        py, px = lax.rem(y + dy, side), lax.rem(x + dx, side)
        peers.append((py * side + px, py, px))
    toffsets = [(dz, dc) for dz in range(zn) for dc in range(2) if (dz, dc) != (0, 0)]
    toffsets.sort(key=lambda o: -(2 * hops(o[0], zn) + o[1]))
    tpeers = [lax.rem(z + dz, zn) * 2 + lax.rem(core + dc, 2) for dz, dc in toffsets]

    column = [lax.rem(y + r, side) * side + x for r in range(1, side)]
    row = [y * side + lax.rem(x + r, side) for r in range(1, side)]
    barrier = pltpu.get_barrier_semaphore()
    cores = (2 * z, 2 * z + 1)
    for p in row + column:
        for t in cores:
            pl.semaphore_signal(barrier, inc=1, device_id={"ctx": p, "tp": t}, device_id_type=MESH)
    for p in tpeers:
        pl.semaphore_signal(barrier, inc=1, device_id={"tp": p}, device_id_type=MESH)

    smalls = [pltpu.make_async_copy(source, target, small_sem.at[i]) for i, (source, target) in enumerate(
        ((hidden_h, hidden_ref), (gains_h, gains_ref), (lengths_h, lengths_ref)))]
    for index in (KC, VC):
        load(index, 0).start()
    for c in smalls:
        c.start()
    for index in (WQ, WK, WV, WO):
        load(index, 0).start()
    for c in smalls:
        c.wait()

    half = hd // 2
    lane = lax.broadcasted_iota(jnp.int32, (heads, hd), 1)
    low = lane < half
    mine = (x, side + y)
    slot = lax.broadcasted_iota(jnp.int32, (heads, side * span), 1)
    block = slot // span
    positions = (y * side * span + slot, (block * side + x) * span + lax.rem(slot, span))
    exponent = jnp.where(low, lane, lane - half).astype(f32) * (2.0 / hd)
    frequency = jnp.exp(-exponent * math.log(rope_base))
    for g in range(2):
        size = lengths_ref[mine[g]]
        bias[g] = jnp.where(positions[g] < size, 0.0, mask_fill)
        angle = jnp.full((heads, hd), size, jnp.int32).astype(f32) * frequency
        cosine[g] = jnp.cos(angle)
        sine[g] = jnp.where(low, -jnp.sin(angle), jnp.sin(angle))
    for l in range(layers):
        gain[l] = jnp.broadcast_to(gains_ref[l:l + 1, :].astype(f32), (batch, feat))
    out_ref[...] = hidden_ref[...].astype(f32)
    own_mask = jnp.where(jnp.full((heads, 1), y, jnp.int32) == jnp.full((heads, 1), x, jnp.int32), 0.0, mask_fill)

    def ship(l, rounds):
        copies = []
        for r in rounds:
            px, py = lax.rem(x + r, side), lax.rem(y + r, side)
            for i, (source, target) in enumerate(((kst, krv), (vst, vrv))):
                copies.append(pltpu.make_async_remote_copy(
                    src_ref=source.at[l, px], dst_ref=target.at[l, core, x],
                    send_sem=hs_sem.at[l, i], recv_sem=hr_sem.at[l, core, i],
                    device_id={"ctx": y * side + px, "tp": cores[1]}, device_id_type=MESH))
                copies.append(pltpu.make_async_remote_copy(
                    src_ref=source.at[l, side + py], dst_ref=target.at[l, core, side + y],
                    send_sem=hs_sem.at[l, i], recv_sem=hr_sem.at[l, core, i],
                    device_id={"ctx": py * side + x, "tp": cores[1]}, device_id_type=MESH))
        return copies

    def ship_start(l):
        for c in ship(l, (2, 1, 3)):
            c.start()

        @pl.when(core == 0)
        def _():
            for c in ship(l, (0,)):
                c.start()

    def taken(ref, sem):
        pltpu.make_async_copy(ref, ref, sem).wait()

    def stage(l):
        load(KC, l).wait()
        load(VC, l).wait()
        for source, staged, held in ((kc, kst, krv), (vc, vst, vrv)):
            for b in range(batch):
                staged[l, b] = source[l, b, 0].astype(f32)

            @pl.when(core == 1)
            def _():
                held[l, 1, x] = source[l, mine[0], 0].astype(f32)
                held[l, 1, side + y] = source[l, mine[1], 0].astype(f32)

    def fresh_copy(d):
        return pltpu.make_async_remote_copy(
            src_ref=ks.at[pl.ds(8 * d, 4)], dst_ref=kr.at[core, me], send_sem=ks_sem.at[d], recv_sem=kr_sem.at[core],
            device_id={"ctx": d * side + d, "tp": cores[1]}, device_id_type=MESH)

    def fresh_sends(act):
        for d in range(side):
            @pl.when(jnp.logical_or(core == 0, me != d * side + d))
            def _():
                act(fresh_copy(d))

    places = peers + [(me, y, x)]
    far_chips = range(n - 1)

    def q_copies(k):
        p, py, px = places[k]
        return [pltpu.make_async_remote_copy(
            src_ref=qs.at[pl.ds(pl.multiple_of(b * 16, 16), QROWS)], dst_ref=qr.at[core, k, g, pl.ds(0, QROWS)],
            send_sem=qs_sem.at[k, g], recv_sem=qr_sem.at[core, k, g],
            device_id={"ctx": p, "tp": cores[1]}, device_id_type=MESH) for g, b in ((0, px), (1, side + py))]

    def q_arrivals(h):
        for k in range(n - h):
            for g in range(2):
                taken(qr.at[h, k, g, pl.ds(0, QROWS)], qr_sem.at[h, k, g])

    def o_copy(h, k):
        return pltpu.make_async_remote_copy(
            src_ref=orr.at[me] if h else od, dst_ref=orr.at[me], send_sem=os_sem.at[h, k], recv_sem=or_sem.at[k],
            device_id={"ctx": places[k][0], "tp": cores[h]}, device_id_type=MESH)

    fresh_sum[...] = jnp.zeros_like(fresh_sum)
    stage(0)
    pl.semaphore_wait(barrier, 2 * len(row) + 2 * len(column) + len(tpeers))
    for p in column:
        for t in cores:
            pl.semaphore_signal(ready, inc=1, device_id={"ctx": p, "tp": t}, device_id_type=MESH)
    ship_start(0)
    pl.semaphore_wait(ready, 2 * len(column))

    def rotate(u, g):
        return u * cosine[g] + pltpu.roll(u, half, 1) * sine[g]

    def rounded(u):
        return u.astype(bf16).astype(f32)

    def attend(h):
        stats = []
        for g in range(2):
            whole, square = qr[h, 0, g, 0:heads], qr[h, 0, g, heads:QROWS]
            for k in range(1, n - h):
                whole = whole + qr[h, k, g, 0:heads]
                square = square + qr[h, k, g, heads:QROWS]
            if h:
                at = pl.multiple_of(mine[g] * 16, 16)
                whole = whole + qs[pl.ds(at, heads), :]
                square = square + qs[pl.ds(pl.multiple_of(at + 8, 8), 1), :]
            inverse = lax.rsqrt(square / total + norm_eps)
            query = rounded(rotate(whole * inverse, g))
            score = lax.dot_general(
                query.astype(bf16), kb[h, g], (((1,), (1,)), ((), ())), preferred_element_type=f32)
            new_key = fresh_sum[h, 2 * g:2 * g + 1] * inverse
            new_key = rounded(rotate(jnp.broadcast_to(new_key, (heads, hd)), g))
            new_value = rounded(fresh_sum[h, 2 * g + 1:2 * g + 2] * inverse)
            own = jnp.sum(query * new_key, axis=1, keepdims=True) * scale + own_mask
            masked = score * scale + bias[g]
            top = jnp.maximum(jnp.max(masked, axis=1, keepdims=True), own)
            weight = jnp.exp(masked - top)
            fresh = jnp.exp(own - top)
            denominator = jnp.sum(weight, axis=1, keepdims=True) + fresh
            numerator = jnp.dot(weight.astype(bf16), vb[h, g], preferred_element_type=f32) + rounded(fresh) * new_value
            if h:
                orr[me, g * heads:(g + 1) * heads, :] = numerator / denominator
            else:
                od[g * heads:(g + 1) * heads, :] = numerator / denominator
            stats.append(top + jnp.log(denominator))
        if h:
            orr[me, 2 * heads:3 * heads, :] = jnp.where(low, stats[0], stats[1])
        else:
            od[2 * heads:3 * heads, :] = jnp.where(low, stats[0], stats[1])

    def layer_step(l, carry):
        stream = out_ref[...]
        scaled = (stream * gain[l]).astype(bf16)
        squares = jnp.sum(stream * stream, axis=1, keepdims=True)
        load(WQ, l).wait()
        load(WK, l).wait()
        load(WV, l).wait()

        @pl.when(l + 1 < layers)
        def _():
            for index in range(len(weights)):
                load(index, l + 1).start()

        def put(row, tile):
            qs[pl.ds(row, batch, stride=16), :] = tile

        for i, w in enumerate((wk, wv)):
            kv = jnp.dot(scaled, w[l], preferred_element_type=f32)
            for g in range(2):
                ks[pl.ds(2 * g + i, side, stride=8), :] = kv[g * side:(g + 1) * side]
        fresh_sends(lambda c: c.start())
        put(heads, jnp.broadcast_to(squares, (batch, hd)))
        q = jnp.dot(scaled, wq[l], preferred_element_type=f32)
        for h in range(heads):
            put(h, q[:, h * hd:(h + 1) * hd])
        for k in far_chips:
            for c in q_copies(k):
                c.start()

        @pl.when(core == 0)
        def _():
            for c in q_copies(n - 1):
                c.start()
            taken(kst.at[l], hs_sem.at[l, 0])
            taken(vst.at[l], hs_sem.at[l, 1])

        @pl.when(core == 1)
        def _():
            blocks = 2 * side
            taken(kst.at[l, pl.ds(0, blocks - 2)], hs_sem.at[l, 0])
            taken(vst.at[l, pl.ds(0, blocks - 2)], hs_sem.at[l, 1])
            for h in (1, 0):
                taken(krv.at[l, h, pl.ds(0, blocks - 2 * h)], hr_sem.at[l, h, 0])
                taken(vrv.at[l, h, pl.ds(0, blocks - 2 * h)], hr_sem.at[l, h, 1])
                for g in range(2):
                    part = slice(g * side, (g + 1) * side)
                    kb[h, g] = krv[l, h, part].reshape(side * span, hd).astype(bf16)
                    vb[h, g] = vrv[l, h, part].reshape(side * span, hd).astype(bf16)

            @pl.when(y == x)
            def _():
                kr[1, me] = ks[pl.ds(pl.multiple_of(8 * x, 8), 4), :]
                for h in (1, 0):
                    taken(kr.at[h, pl.ds(0, n - h)], kr_sem.at[h])
                    fresh_sum[h] = functools.reduce(jnp.add, [kr[h, c] for c in range(n)])

            for h in (1, 0):
                q_arrivals(h)
                attend(h)
                for k in range(n - h):
                    o_copy(h, k).start()

        @pl.when(l + 1 < layers)
        def _():
            stage(l + 1)

        load(WO, l).wait()
        for k in far_chips:
            for c in q_copies(k):
                c.wait_send()
        fresh_sends(lambda c: c.wait_send())

        @pl.when(core == 0)
        def _():
            for c in q_copies(n - 1):
                c.wait_send()
            taken(orr.at[me], or_sem.at[n - 1])

        for k in far_chips:
            taken(orr.at[places[k][0]], or_sem.at[k])

        @pl.when(l + 1 < layers)
        def _():
            ship_start(l + 1)

        logs = [orr[c, 2 * heads:3 * heads, :] for c in range(n)]
        groups = [[[r * side + b for r in range(side)] for b in range(side)],
                  [[b * side + r for r in range(side)] for b in range(side)]]

        def over(values, op):
            return [[functools.reduce(op, [values[c] for c in group]) for group in part] for part in groups]

        def split(pair, c):
            return jnp.where(low, pair[0][c % side], pair[1][c // side])

        largest = over(logs, jnp.maximum)
        factors = [jnp.exp(logs[c] - split(largest, c)) for c in range(n)]
        sums = over(factors, jnp.add)
        inverses = [[1.0 / s for s in part] for part in sums]
        factors = [factors[c] * split(inverses, c) for c in range(n)]
        swapped = [pltpu.roll(f, half, 1) for f in factors]
        for g in range(2):
            for b, group in enumerate(groups[g]):
                merged = None
                for c in group:
                    factor = jnp.where(low, factors[c], swapped[c]) if g == 0 else jnp.where(low, swapped[c], factors[c])
                    term = orr[c, g * heads:(g + 1) * heads, :] * factor
                    merged = term if merged is None else merged + term
                at = (g * side + b) * heads
                cm[at:at + heads, :] = merged
        context = jnp.concatenate([cm[pl.ds(h, batch, stride=heads), :] for h in range(heads)], axis=1).astype(bf16)
        odd = lax.rem(l, 2)
        ts = []
        for i in range(pieces):
            cut = slice(i * piece, (i + 1) * piece)
            tps[i] = jnp.dot(context, wo[l, :, cut], preferred_element_type=f32)
            for k, p in enumerate(tpeers):
                c = pltpu.make_async_remote_copy(
                    src_ref=tps.at[i], dst_ref=tpr.at[odd, i, k], send_sem=ts_sem.at[i, k],
                    recv_sem=tr_sem.at[odd, i, k], device_id={"tp": p}, device_id_type=MESH)
                c.start()
                ts.append(c)
        @pl.when(core == 1)
        def _():
            for h in (1, 0):
                for k in range(n - h):
                    o_copy(h, k).wait_send()

        for i in range(pieces):
            cut = slice(i * piece, (i + 1) * piece)
            moved = out_ref[:, cut] + tps[i]
            for k in range(tn - 1):
                ts[i * (tn - 1) + k].wait_recv()
                moved = moved + tpr[odd, i, k]
            out_ref[:, cut] = moved
        for c in ts:
            c.wait_send()
        return carry

    lax.fori_loop(0, layers, layer_step, 0)


def shards(sizes, hidden, norm_gains, w_query, w_key, w_value, w_out, key_cache, value_cache, lengths):
    n, tn = sizes
    layers, feat, columns = w_query.shape
    batch = hidden.shape[0]
    _, _, _, span, hd = key_cache.shape
    heads = columns // hd
    side = math.isqrt(n)
    dims = (n, tn, side, layers, batch, feat, feat * n, heads, hd, span)
    pieces = 1
    f32, bf16 = jnp.float32, jnp.bfloat16
    vmem = pl.BlockSpec(memory_space=pltpu.VMEM)
    far = pl.BlockSpec(memory_space=pl.ANY)

    def like(array):
        return pltpu.VMEM(array.shape, array.dtype)

    dma = pltpu.SemaphoreType.DMA
    return pl.pallas_call(
        functools.partial(kernel, dims),
        out_shape=pltpu.VMEM((batch, feat), f32),
        in_specs=[far] * 9,
        out_specs=vmem,
        scratch_shapes=[
            like(hidden), like(norm_gains), pltpu.SMEM(lengths.shape, lengths.dtype),
            like(w_query), like(w_key), like(w_value), like(w_out), like(key_cache), like(value_cache),
            pltpu.VMEM((layers, batch, feat), f32),
            pltpu.VMEM((2, heads, side * span), f32),
            pltpu.VMEM((2, heads, hd), f32),
            pltpu.VMEM((2, heads, hd), f32),
            pltpu.VMEM((batch * 16, hd), f32),
            pltpu.VMEM((2, n, 2, 16, hd), f32),
            pltpu.VMEM((side * 8, hd), f32),
            pltpu.VMEM((2, n, 4, hd), f32),
            pltpu.VMEM((2, 4, hd), f32),
            pltpu.VMEM((layers, batch, span, hd), f32),
            pltpu.VMEM((layers, batch, span, hd), f32),
            pltpu.VMEM((layers, 2, 2 * side, span, hd), f32),
            pltpu.VMEM((layers, 2, 2 * side, span, hd), f32),
            pltpu.VMEM((2, 2, side * span, hd), bf16),
            pltpu.VMEM((2, 2, side * span, hd), bf16),
            pltpu.VMEM((n, 3 * heads, hd), f32),
            pltpu.VMEM((3 * heads, hd), f32),
            pltpu.VMEM((batch * heads, hd), f32),
            pltpu.VMEM((pieces, batch, feat // pieces), f32),
            pltpu.VMEM((2, pieces, tn - 1, batch, feat // pieces), f32),
            dma((6, layers)),
            dma((n, 2)), dma((2, n, 2)),
            dma((side,)), dma((2,)),
            dma((2, n)), dma((n,)),
            dma((pieces, tn - 1)), dma((2, pieces, tn - 1)),
            dma((layers, 2)), dma((layers, 2, 2)),
            dma((3,)), pltpu.SemaphoreType.REGULAR,
        ],
        compiler_params=pltpu.CompilerParams(
            collective_id=0, has_side_effects=True, vmem_limit_bytes=60 * 1024 * 1024),
    )(hidden, norm_gains, lengths, w_query, w_key, w_value, w_out, key_cache, value_cache)


def solution(mesh):
    sizes = (mesh.shape["ctx"], mesh.shape["tp"])
    return jax.shard_map(
        functools.partial(shards, sizes),
        mesh=mesh,
        in_specs=(
            P(None, "ctx"),
            P(None, "ctx"),
            P(None, "ctx", "tp"),
            P(None, "ctx", "tp"),
            P(None, "ctx", "tp"),
            P(None, "tp", "ctx"),
            P(None, None, "tp", "ctx", None),
            P(None, None, "tp", "ctx", None),
            P(),
        ),
        out_specs=P(None, "ctx"),
        check_vma=False,
    )
```

```python
import functools
import math

import jax
import jax.numpy as jnp
from jax import lax
from jax.experimental import pallas as pl
from jax.experimental.pallas import tpu as pltpu
from jax.sharding import PartitionSpec as P

mask_fill = -1e30
norm_eps = 1e-05
rope_base = 500000.0
MESH = pl.DeviceIdType.MESH
QROWS = 9


def kernel(dims, hidden_h, gains_h, lengths_h, wq_h, wk_h, wv_h, wo_h, kc_h, vc_h, out_ref,
           hidden_ref, gains_ref, lengths_ref, wq, wk, wv, wo, kc, vc, gain, bias, cosine, sine, qs, qr, ks, kr, fresh_sum, kst, vst, krv, vrv, kb, vb,
           orr, od, cm, tps, tpr, w_sem, qs_sem, qr_sem, ks_sem, kr_sem, os_sem, or_sem, ts_sem, tr_sem, hs_sem, hr_sem, small_sem, ready):
    n, tn, side, layers, batch, feat, total, heads, hd, span = dims
    f32, bf16 = jnp.float32, jnp.bfloat16
    pieces = tps.shape[0]
    piece = feat // pieces
    scale = 1.0 / math.sqrt(hd)
    me = lax.axis_index("ctx")
    mt = lax.axis_index("tp")
    y, x = me // side, lax.rem(me, side)
    z, core = mt // 2, lax.rem(mt, 2)
    zn = tn // 2
    weights = ((kc_h, kc), (vc_h, vc), (wq_h, wq), (wk_h, wk), (wv_h, wv), (wo_h, wo))
    KC, VC, WQ, WK, WV, WO = range(6)

    def load(index, layer):
        source, target = weights[index]
        return pltpu.make_async_copy(source.at[layer], target.at[layer], w_sem.at[index, layer])

    def hops(step, size):
        return min(step, size - step)

    offsets = [(dy, dx) for dy in range(side) for dx in range(side) if (dy, dx) != (0, 0)]
    offsets.sort(key=lambda o: -(hops(o[0], side) + hops(o[1], side)))
    peers = []
    for dy, dx in offsets:
        py, px = lax.rem(y + dy, side), lax.rem(x + dx, side)
        peers.append((py * side + px, py, px))
    toffsets = [(dz, dc) for dz in range(zn) for dc in range(2) if (dz, dc) != (0, 0)]
    toffsets.sort(key=lambda o: -(2 * hops(o[0], zn) + o[1]))
    tpeers = [lax.rem(z + dz, zn) * 2 + lax.rem(core + dc, 2) for dz, dc in toffsets]

    column = [lax.rem(y + r, side) * side + x for r in range(1, side)]
    row = [y * side + lax.rem(x + r, side) for r in range(1, side)]
    barrier = pltpu.get_barrier_semaphore()
    cores = (2 * z, 2 * z + 1)
    for p in row + column:
        for t in cores:
            pl.semaphore_signal(barrier, inc=1, device_id={"ctx": p, "tp": t}, device_id_type=MESH)
    for p in tpeers:
        pl.semaphore_signal(barrier, inc=1, device_id={"tp": p}, device_id_type=MESH)

    smalls = [pltpu.make_async_copy(source, target, small_sem.at[i]) for i, (source, target) in enumerate(
        ((hidden_h, hidden_ref), (gains_h, gains_ref), (lengths_h, lengths_ref)))]
    for index in (KC, VC):
        load(index, 0).start()
    for c in smalls:
        c.start()
    for index in (WQ, WK, WV, WO):
        load(index, 0).start()
    for c in smalls:
        c.wait()

    half = hd // 2
    lane = lax.broadcasted_iota(jnp.int32, (heads, hd), 1)
    low = lane < half
    mine = (x, side + y)
    slot = lax.broadcasted_iota(jnp.int32, (heads, side * span), 1)
    block = slot // span
    positions = (y * side * span + slot, (block * side + x) * span + lax.rem(slot, span))
    exponent = jnp.where(low, lane, lane - half).astype(f32) * (2.0 / hd)
    frequency = jnp.exp(-exponent * math.log(rope_base))
    for g in range(2):
        size = lengths_ref[mine[g]]
        bias[g] = jnp.where(positions[g] < size, 0.0, mask_fill)
        angle = jnp.full((heads, hd), size, jnp.int32).astype(f32) * frequency
        cosine[g] = jnp.cos(angle)
        sine[g] = jnp.where(low, -jnp.sin(angle), jnp.sin(angle))
    for l in range(layers):
        gain[l] = jnp.broadcast_to(gains_ref[l:l + 1, :].astype(f32), (batch, feat))
    out_ref[...] = hidden_ref[...].astype(f32)
    own_mask = jnp.where(jnp.full((heads, 1), y, jnp.int32) == jnp.full((heads, 1), x, jnp.int32), 0.0, mask_fill)

    def ship(l, rounds):
        copies = []
        for r in rounds:
            px, py = lax.rem(x + r, side), lax.rem(y + r, side)
            for i, (source, target) in enumerate(((kst, krv), (vst, vrv))):
                copies.append(pltpu.make_async_remote_copy(
                    src_ref=source.at[l, px], dst_ref=target.at[l, core, x],
                    send_sem=hs_sem.at[l, i], recv_sem=hr_sem.at[l, core, i],
                    device_id={"ctx": y * side + px, "tp": cores[1]}, device_id_type=MESH))
                copies.append(pltpu.make_async_remote_copy(
                    src_ref=source.at[l, side + py], dst_ref=target.at[l, core, side + y],
                    send_sem=hs_sem.at[l, i], recv_sem=hr_sem.at[l, core, i],
                    device_id={"ctx": py * side + x, "tp": cores[1]}, device_id_type=MESH))
        return copies

    def ship_start(l):
        for c in ship(l, (2, 1, 3)):
            c.start()

        @pl.when(core == 0)
        def _():
            for c in ship(l, (0,)):
                c.start()

    def taken(ref, sem):
        pltpu.make_async_copy(ref, ref, sem).wait()

    def stage(l):
        load(KC, l).wait()
        load(VC, l).wait()
        for source, staged, held in ((kc, kst, krv), (vc, vst, vrv)):
            for b in range(batch):
                staged[l, b] = source[l, b, 0].astype(f32)

            @pl.when(core == 1)
            def _():
                held[l, 1, x] = source[l, mine[0], 0].astype(f32)
                held[l, 1, side + y] = source[l, mine[1], 0].astype(f32)

    def fresh_copy(d):
        return pltpu.make_async_remote_copy(
            src_ref=ks.at[pl.ds(8 * d, 4)], dst_ref=kr.at[core, me], send_sem=ks_sem.at[d], recv_sem=kr_sem.at[core],
            device_id={"ctx": d * side + d, "tp": cores[1]}, device_id_type=MESH)

    def fresh_sends(act):
        for d in range(side):
            @pl.when(jnp.logical_or(core == 0, me != d * side + d))
            def _():
                act(fresh_copy(d))

    places = peers + [(me, y, x)]
    far_chips = range(n - 1)

    def q_copies(k):
        p, py, px = places[k]
        return [pltpu.make_async_remote_copy(
            src_ref=qs.at[pl.ds(pl.multiple_of(b * 16, 16), QROWS)], dst_ref=qr.at[core, k, g, pl.ds(0, QROWS)],
            send_sem=qs_sem.at[k, g], recv_sem=qr_sem.at[core, k, g],
            device_id={"ctx": p, "tp": cores[1]}, device_id_type=MESH) for g, b in ((0, px), (1, side + py))]

    def q_arrivals(h):
        for k in range(n - h):
            for g in range(2):
                taken(qr.at[h, k, g, pl.ds(0, QROWS)], qr_sem.at[h, k, g])

    def o_copy(h, k):
        return pltpu.make_async_remote_copy(
            src_ref=orr.at[me] if h else od, dst_ref=orr.at[me], send_sem=os_sem.at[h, k], recv_sem=or_sem.at[k],
            device_id={"ctx": places[k][0], "tp": cores[h]}, device_id_type=MESH)

    fresh_sum[...] = jnp.zeros_like(fresh_sum)
    stage(0)
    pl.semaphore_wait(barrier, 2 * len(row) + 2 * len(column) + len(tpeers))
    for p in column:
        for t in cores:
            pl.semaphore_signal(ready, inc=1, device_id={"ctx": p, "tp": t}, device_id_type=MESH)
    ship_start(0)
    pl.semaphore_wait(ready, 2 * len(column))

    def rotate(u, g):
        return u * cosine[g] + pltpu.roll(u, half, 1) * sine[g]

    def rounded(u):
        return u.astype(bf16).astype(f32)

    def attend(h):
        both = range(2)
        inverse, query = [], []
        for g in both:
            whole, square = qr[h, 0, g, 0:heads], qr[h, 0, g, heads:QROWS]
            for k in range(1, n - h):
                whole = whole + qr[h, k, g, 0:heads]
                square = square + qr[h, k, g, heads:QROWS]
            if h:
                at = pl.multiple_of(mine[g] * 16, 16)
                whole = whole + qs[pl.ds(at, heads), :]
                square = square + qs[pl.ds(pl.multiple_of(at + 8, 8), 1), :]
            inverse.append(lax.rsqrt(square / total + norm_eps))
            query.append(rounded(rotate(whole * inverse[g], g)))
        score = [lax.dot_general(
            query[g].astype(bf16), kb[h, g], (((1,), (1,)), ((), ())), preferred_element_type=f32) for g in both]
        new_key = [rounded(rotate(jnp.broadcast_to(fresh_sum[h, 2 * g:2 * g + 1] * inverse[g], (heads, hd)), g)) for g in both]
        new_value = [rounded(fresh_sum[h, 2 * g + 1:2 * g + 2] * inverse[g]) for g in both]
        own = [jnp.sum(query[g] * new_key[g], axis=1, keepdims=True) * scale + own_mask for g in both]
        masked = [score[g] * scale + bias[g] for g in both]
        top = [jnp.maximum(jnp.max(masked[g], axis=1, keepdims=True), own[g]) for g in both]
        weight = [jnp.exp(masked[g] - top[g]) for g in both]
        numerator = [jnp.dot(weight[g].astype(bf16), vb[h, g], preferred_element_type=f32) for g in both]
        fresh = [jnp.exp(own[g] - top[g]) for g in both]
        denominator = [jnp.sum(weight[g], axis=1, keepdims=True) + fresh[g] for g in both]
        logs = [top[g] + jnp.log(denominator[g]) for g in both]
        share = [1.0 / denominator[g] for g in both]
        parts = [(numerator[g] + rounded(fresh[g]) * new_value[g]) * share[g] for g in both]
        parts.append(jnp.where(low, logs[0], logs[1]))
        for i, part in enumerate(parts):
            if h:
                orr[me, i * heads:(i + 1) * heads, :] = part
            else:
                od[i * heads:(i + 1) * heads, :] = part

    def layer_step(l, carry):
        stream = out_ref[...]
        scaled = (stream * gain[l]).astype(bf16)
        squares = jnp.sum(stream * stream, axis=1, keepdims=True)
        load(WQ, l).wait()
        load(WK, l).wait()
        load(WV, l).wait()

        @pl.when(l + 1 < layers)
        def _():
            for index in range(len(weights)):
                load(index, l + 1).start()

        def put(row, tile):
            qs[pl.ds(row, batch, stride=16), :] = tile

        for i, w in enumerate((wk, wv)):
            kv = jnp.dot(scaled, w[l], preferred_element_type=f32)
            for g in range(2):
                ks[pl.ds(2 * g + i, side, stride=8), :] = kv[g * side:(g + 1) * side]
        put(heads, jnp.broadcast_to(squares, (batch, hd)))
        q = jnp.dot(scaled, wq[l], preferred_element_type=f32)
        for h in range(heads):
            put(h, q[:, h * hd:(h + 1) * hd])
        fresh_sends(lambda c: c.start())
        for k in far_chips:
            for c in q_copies(k):
                c.start()

        @pl.when(core == 0)
        def _():
            for c in q_copies(n - 1):
                c.start()
            taken(kst.at[l], hs_sem.at[l, 0])
            taken(vst.at[l], hs_sem.at[l, 1])

        @pl.when(core == 1)
        def _():
            blocks = 2 * side
            taken(kst.at[l, pl.ds(0, blocks - 2)], hs_sem.at[l, 0])
            taken(vst.at[l, pl.ds(0, blocks - 2)], hs_sem.at[l, 1])
            for h in (1, 0):
                taken(krv.at[l, h, pl.ds(0, blocks - 2 * h)], hr_sem.at[l, h, 0])
                taken(vrv.at[l, h, pl.ds(0, blocks - 2 * h)], hr_sem.at[l, h, 1])
                for g in range(2):
                    part = slice(g * side, (g + 1) * side)
                    kb[h, g] = krv[l, h, part].reshape(side * span, hd).astype(bf16)
                    vb[h, g] = vrv[l, h, part].reshape(side * span, hd).astype(bf16)

            @pl.when(y == x)
            def _():
                kr[1, me] = ks[pl.ds(pl.multiple_of(8 * x, 8), 4), :]
                for h in (1, 0):
                    taken(kr.at[h, pl.ds(0, n - h)], kr_sem.at[h])
                    fresh_sum[h] = functools.reduce(jnp.add, [kr[h, c] for c in range(n)])

            for h in (1, 0):
                q_arrivals(h)
                attend(h)
                for k in range(n - h):
                    o_copy(h, k).start()

        @pl.when(l + 1 < layers)
        def _():
            stage(l + 1)

        load(WO, l).wait()
        for k in far_chips:
            for c in q_copies(k):
                c.wait_send()
        fresh_sends(lambda c: c.wait_send())

        @pl.when(core == 0)
        def _():
            for c in q_copies(n - 1):
                c.wait_send()
            taken(orr.at[me], or_sem.at[n - 1])

        for k in far_chips:
            taken(orr.at[places[k][0]], or_sem.at[k])

        @pl.when(l + 1 < layers)
        def _():
            ship_start(l + 1)

        logs = [orr[c, 2 * heads:3 * heads, :] for c in range(n)]
        groups = [[[r * side + b for r in range(side)] for b in range(side)],
                  [[b * side + r for r in range(side)] for b in range(side)]]

        def over(values, op):
            return [[functools.reduce(op, [values[c] for c in group]) for group in part] for part in groups]

        def split(pair, c):
            return jnp.where(low, pair[0][c % side], pair[1][c // side])

        largest = over(logs, jnp.maximum)
        factors = [jnp.exp(logs[c] - split(largest, c)) for c in range(n)]
        sums = over(factors, jnp.add)
        inverses = [[1.0 / s for s in part] for part in sums]
        factors = [factors[c] * split(inverses, c) for c in range(n)]
        swapped = [pltpu.roll(f, half, 1) for f in factors]
        for g in range(2):
            for b, group in enumerate(groups[g]):
                merged = None
                for c in group:
                    factor = jnp.where(low, factors[c], swapped[c]) if g == 0 else jnp.where(low, swapped[c], factors[c])
                    term = orr[c, g * heads:(g + 1) * heads, :] * factor
                    merged = term if merged is None else merged + term
                at = (g * side + b) * heads
                cm[at:at + heads, :] = merged
        context = jnp.concatenate([cm[pl.ds(h, batch, stride=heads), :] for h in range(heads)], axis=1).astype(bf16)
        odd = lax.rem(l, 2)
        ts = []
        for i in range(pieces):
            cut = slice(i * piece, (i + 1) * piece)
            tps[i] = jnp.dot(context, wo[l, :, cut], preferred_element_type=f32)
            for k, p in enumerate(tpeers):
                c = pltpu.make_async_remote_copy(
                    src_ref=tps.at[i], dst_ref=tpr.at[odd, i, k], send_sem=ts_sem.at[i, k],
                    recv_sem=tr_sem.at[odd, i, k], device_id={"tp": p}, device_id_type=MESH)
                c.start()
                ts.append(c)
        @pl.when(core == 1)
        def _():
            for h in (1, 0):
                for k in range(n - h):
                    o_copy(h, k).wait_send()

        for i in range(pieces):
            cut = slice(i * piece, (i + 1) * piece)
            moved = out_ref[:, cut] + tps[i]
            for k in range(tn - 1):
                ts[i * (tn - 1) + k].wait_recv()
                moved = moved + tpr[odd, i, k]
            out_ref[:, cut] = moved
        for c in ts:
            c.wait_send()
        return carry

    lax.fori_loop(0, layers, layer_step, 0)


def shards(sizes, hidden, norm_gains, w_query, w_key, w_value, w_out, key_cache, value_cache, lengths):
    n, tn = sizes
    layers, feat, columns = w_query.shape
    batch = hidden.shape[0]
    _, _, _, span, hd = key_cache.shape
    heads = columns // hd
    side = math.isqrt(n)
    dims = (n, tn, side, layers, batch, feat, feat * n, heads, hd, span)
    pieces = 1
    f32, bf16 = jnp.float32, jnp.bfloat16
    vmem = pl.BlockSpec(memory_space=pltpu.VMEM)
    far = pl.BlockSpec(memory_space=pl.ANY)

    def like(array):
        return pltpu.VMEM(array.shape, array.dtype)

    dma = pltpu.SemaphoreType.DMA
    return pl.pallas_call(
        functools.partial(kernel, dims),
        out_shape=pltpu.VMEM((batch, feat), f32),
        in_specs=[far] * 9,
        out_specs=vmem,
        scratch_shapes=[
            like(hidden), like(norm_gains), pltpu.SMEM(lengths.shape, lengths.dtype),
            like(w_query), like(w_key), like(w_value), like(w_out), like(key_cache), like(value_cache),
            pltpu.VMEM((layers, batch, feat), f32),
            pltpu.VMEM((2, heads, side * span), f32),
            pltpu.VMEM((2, heads, hd), f32),
            pltpu.VMEM((2, heads, hd), f32),
            pltpu.VMEM((batch * 16, hd), f32),
            pltpu.VMEM((2, n, 2, 16, hd), f32),
            pltpu.VMEM((side * 8, hd), f32),
            pltpu.VMEM((2, n, 4, hd), f32),
            pltpu.VMEM((2, 4, hd), f32),
            pltpu.VMEM((layers, batch, span, hd), f32),
            pltpu.VMEM((layers, batch, span, hd), f32),
            pltpu.VMEM((layers, 2, 2 * side, span, hd), f32),
            pltpu.VMEM((layers, 2, 2 * side, span, hd), f32),
            pltpu.VMEM((2, 2, side * span, hd), bf16),
            pltpu.VMEM((2, 2, side * span, hd), bf16),
            pltpu.VMEM((n, 3 * heads, hd), f32),
            pltpu.VMEM((3 * heads, hd), f32),
            pltpu.VMEM((batch * heads, hd), f32),
            pltpu.VMEM((pieces, batch, feat // pieces), f32),
            pltpu.VMEM((2, pieces, tn - 1, batch, feat // pieces), f32),
            dma((6, layers)),
            dma((n, 2)), dma((2, n, 2)),
            dma((side,)), dma((2,)),
            dma((2, n)), dma((n,)),
            dma((pieces, tn - 1)), dma((2, pieces, tn - 1)),
            dma((layers, 2)), dma((layers, 2, 2)),
            dma((3,)), pltpu.SemaphoreType.REGULAR,
        ],
        compiler_params=pltpu.CompilerParams(
            collective_id=0, has_side_effects=True, vmem_limit_bytes=60 * 1024 * 1024),
    )(hidden, norm_gains, lengths, w_query, w_key, w_value, w_out, key_cache, value_cache)


def solution(mesh):
    sizes = (mesh.shape["ctx"], mesh.shape["tp"])
    return jax.shard_map(
        functools.partial(shards, sizes),
        mesh=mesh,
        in_specs=(
            P(None, "ctx"),
            P(None, "ctx"),
            P(None, "ctx", "tp"),
            P(None, "ctx", "tp"),
            P(None, "ctx", "tp"),
            P(None, "tp", "ctx"),
            P(None, None, "tp", "ctx", None),
            P(None, None, "tp", "ctx", None),
            P(),
        ),
        out_specs=P(None, "ctx"),
        check_vma=False,
    )
```

```python
import functools
import math

import jax
import jax.numpy as jnp
from jax import lax
from jax.experimental import pallas as pl
from jax.experimental.pallas import tpu as pltpu
from jax.sharding import PartitionSpec as P

mask_fill = -1e30
norm_eps = 1e-05
rope_base = 500000.0
MESH = pl.DeviceIdType.MESH
QROWS = 9


def kernel(dims, hidden_h, gains_h, lengths_h, wq_h, wk_h, wv_h, wo_h, kc_h, vc_h, out_ref,
           hidden_ref, gains_ref, lengths_ref, wq, wk, wv, wo, kc, vc, gain, bias, cosine, sine, qs, qr, ks, kr, fresh_sum, kst, vst, krv, vrv, kb, vb,
           orr, cm, wst, wo2, wob, tps, tpr, w_sem, qs_sem, qr_sem, ks_sem, kr_sem, os_sem, or_sem, ts_sem, tr_sem, hs_sem, hr_sem, xs_sem, xr_sem, small_sem, ready, go):
    n, tn, side, layers, batch, feat, total, heads, hd, span = dims
    f32, bf16 = jnp.float32, jnp.bfloat16
    scale = 1.0 / math.sqrt(hd)
    me = lax.axis_index("ctx")
    mt = lax.axis_index("tp")
    y, x = me // side, lax.rem(me, side)
    z, core = mt // 2, lax.rem(mt, 2)
    zn = tn // 2
    weights = ((kc_h, kc), (vc_h, vc), (wq_h, wq), (wk_h, wk), (wv_h, wv), (wo_h, wo))
    KC, VC, WQ, WK, WV, WO = range(6)

    def load(index, layer):
        source, target = weights[index]
        return pltpu.make_async_copy(source.at[layer], target.at[layer], w_sem.at[index, layer])

    def hops(step, size):
        return min(step, size - step)

    offsets = [(dy, dx) for dy in range(side) for dx in range(side) if (dy, dx) != (0, 0)]
    offsets.sort(key=lambda o: -(hops(o[0], side) + hops(o[1], side)))
    peers = []
    for dy, dx in offsets:
        py, px = lax.rem(y + dy, side), lax.rem(x + dx, side)
        peers.append((py * side + px, py, px))
    toffsets = [(dz, dc) for dz in range(zn) for dc in range(2) if (dz, dc) != (0, 0)]
    toffsets.sort(key=lambda o: -(2 * hops(o[0], zn) + o[1]))
    tpeers = [lax.rem(z + dz, zn) * 2 + lax.rem(core + dc, 2) for dz, dc in toffsets]

    column = [lax.rem(y + r, side) * side + x for r in range(1, side)]
    row = [y * side + lax.rem(x + r, side) for r in range(1, side)]
    barrier = pltpu.get_barrier_semaphore()
    cores = (2 * z, 2 * z + 1)
    for p in row + column:
        for t in cores:
            pl.semaphore_signal(barrier, inc=1, device_id={"ctx": p, "tp": t}, device_id_type=MESH)
    for p in tpeers:
        pl.semaphore_signal(barrier, inc=1, device_id={"tp": p}, device_id_type=MESH)

    smalls = [pltpu.make_async_copy(source, target, small_sem.at[i]) for i, (source, target) in enumerate(
        ((hidden_h, hidden_ref), (gains_h, gains_ref), (lengths_h, lengths_ref)))]
    for index in (KC, VC):
        load(index, 0).start()
    for c in smalls:
        c.start()
    for index in (WQ, WK, WV, WO):
        load(index, 0).start()
    for c in smalls:
        c.wait()

    half = hd // 2
    lane = lax.broadcasted_iota(jnp.int32, (heads, hd), 1)
    low = lane < half
    mine = (x, side + y)
    slot = lax.broadcasted_iota(jnp.int32, (heads, side * span), 1)
    block = slot // span
    positions = (y * side * span + slot, (block * side + x) * span + lax.rem(slot, span))
    exponent = jnp.where(low, lane, lane - half).astype(f32) * (2.0 / hd)
    frequency = jnp.exp(-exponent * math.log(rope_base))
    for g in range(2):
        size = lengths_ref[mine[g]]
        bias[g] = jnp.where(positions[g] < size, 0.0, mask_fill)
        angle = jnp.full((heads, hd), size, jnp.int32).astype(f32) * frequency
        cosine[g] = jnp.cos(angle)
        sine[g] = jnp.where(low, -jnp.sin(angle), jnp.sin(angle))
    for l in range(layers):
        gain[l] = jnp.broadcast_to(gains_ref[l:l + 1, :].astype(f32), (batch, feat))
    out_ref[...] = hidden_ref[...].astype(f32)
    own_mask = jnp.where(jnp.full((heads, 1), y, jnp.int32) == jnp.full((heads, 1), x, jnp.int32), 0.0, mask_fill)

    def ship(l, rounds):
        copies = []
        for r in rounds:
            px, py = lax.rem(x + r, side), lax.rem(y + r, side)
            for i, (source, target) in enumerate(((kst, krv), (vst, vrv))):
                copies.append(pltpu.make_async_remote_copy(
                    src_ref=source.at[l, px], dst_ref=target.at[l, core, x],
                    send_sem=hs_sem.at[l, i], recv_sem=hr_sem.at[l, core, i],
                    device_id={"ctx": y * side + px, "tp": cores[1]}, device_id_type=MESH))
                copies.append(pltpu.make_async_remote_copy(
                    src_ref=source.at[l, side + py], dst_ref=target.at[l, core, side + y],
                    send_sem=hs_sem.at[l, i], recv_sem=hr_sem.at[l, core, i],
                    device_id={"ctx": py * side + x, "tp": cores[1]}, device_id_type=MESH))
        return copies

    def ship_start(l):
        for c in ship(l, (2, 1, 3)):
            c.start()

        @pl.when(core == 0)
        def _():
            for c in ship(l, (0,)):
                c.start()

    def taken(ref, sem):
        pltpu.make_async_copy(ref, ref, sem).wait()

    def stage(l):
        load(KC, l).wait()
        load(VC, l).wait()
        for source, staged, held in ((kc, kst, krv), (vc, vst, vrv)):
            for b in range(batch):
                staged[l, b] = source[l, b, 0].astype(f32)

            @pl.when(core == 1)
            def _():
                held[l, 1, x] = source[l, mine[0], 0].astype(f32)
                held[l, 1, side + y] = source[l, mine[1], 0].astype(f32)

    def fresh_copy(d):
        return pltpu.make_async_remote_copy(
            src_ref=ks.at[pl.ds(8 * d, 4)], dst_ref=kr.at[core, me], send_sem=ks_sem.at[d], recv_sem=kr_sem.at[core],
            device_id={"ctx": d * side + d, "tp": cores[1]}, device_id_type=MESH)

    def fresh_sends(act):
        for d in range(side):
            @pl.when(jnp.logical_or(core == 0, me != d * side + d))
            def _():
                act(fresh_copy(d))

    places = peers + [(me, y, x)]
    far_chips = range(n - 1)

    def q_copies(k):
        p, py, px = places[k]
        return [pltpu.make_async_remote_copy(
            src_ref=qs.at[pl.ds(pl.multiple_of(b * 16, 16), QROWS)], dst_ref=qr.at[core, k, g, pl.ds(0, QROWS)],
            send_sem=qs_sem.at[k, g], recv_sem=qr_sem.at[core, k, g],
            device_id={"ctx": p, "tp": cores[1]}, device_id_type=MESH) for g, b in ((0, px), (1, side + py))]

    def q_arrivals(h):
        for k in range(n - h):
            for g in range(2):
                taken(qr.at[h, k, g, pl.ds(0, QROWS)], qr_sem.at[h, k, g])

    def o_copy(h, k):
        return pltpu.make_async_remote_copy(
            src_ref=orr.at[h, me], dst_ref=orr.at[h, me], send_sem=os_sem.at[h, k], recv_sem=or_sem.at[h, k],
            device_id={"ctx": places[k][0]}, device_id_type=MESH)

    def w_out_copy(l):
        return pltpu.make_async_remote_copy(
            src_ref=wst.at[l], dst_ref=wo2.at[l], send_sem=xs_sem.at[l], recv_sem=xr_sem.at[l],
            device_id={"tp": cores[1]}, device_id_type=MESH)

    def w_out_start(l):
        load(WO, l).wait()
        wst[l] = wo[l].astype(f32)
        w_out_copy(l).start()

    def t_copy(odd, k):
        return pltpu.make_async_remote_copy(
            src_ref=tps, dst_ref=tpr.at[odd, k], send_sem=ts_sem.at[k], recv_sem=tr_sem.at[odd, k],
            device_id={"tp": tpeers[k]}, device_id_type=MESH)

    def t_arrivals(odd, cross):
        moved = None
        for k, (dz, dc) in enumerate(toffsets):
            if dc == cross:
                taken(tpr.at[odd, k], tr_sem.at[odd, k])
                moved = tpr[odd, k] if moved is None else moved + tpr[odd, k]
        return moved

    fresh_sum[...] = jnp.zeros_like(fresh_sum)
    stage(0)
    pl.semaphore_wait(barrier, 2 * len(row) + 2 * len(column) + len(tpeers))
    for p in column:
        for t in cores:
            pl.semaphore_signal(ready, inc=1, device_id={"ctx": p, "tp": t}, device_id_type=MESH)
    ship_start(0)
    pl.semaphore_wait(ready, 2 * len(column))

    def rotate(u, g):
        return u * cosine[g] + pltpu.roll(u, half, 1) * sine[g]

    def rounded(u):
        return u.astype(bf16).astype(f32)

    def attend(h):
        both = range(2)
        inverse, query = [], []
        for g in both:
            whole, square = qr[h, 0, g, 0:heads], qr[h, 0, g, heads:QROWS]
            for k in range(1, n - h):
                whole = whole + qr[h, k, g, 0:heads]
                square = square + qr[h, k, g, heads:QROWS]
            if h:
                at = pl.multiple_of(mine[g] * 16, 16)
                whole = whole + qs[pl.ds(at, heads), :]
                square = square + qs[pl.ds(pl.multiple_of(at + 8, 8), 1), :]
            inverse.append(lax.rsqrt(square / total + norm_eps))
            query.append(rounded(rotate(whole * inverse[g], g)))
        score = [lax.dot_general(
            query[g].astype(bf16), kb[h, g], (((1,), (1,)), ((), ())), preferred_element_type=f32) for g in both]
        new_key = [rounded(rotate(jnp.broadcast_to(fresh_sum[h, 2 * g:2 * g + 1] * inverse[g], (heads, hd)), g)) for g in both]
        new_value = [rounded(fresh_sum[h, 2 * g + 1:2 * g + 2] * inverse[g]) for g in both]
        own = [jnp.sum(query[g] * new_key[g], axis=1, keepdims=True) * scale + own_mask for g in both]
        masked = [score[g] * scale + bias[g] for g in both]
        top = [jnp.maximum(jnp.max(masked[g], axis=1, keepdims=True), own[g]) for g in both]
        weight = [jnp.exp(masked[g] - top[g]) for g in both]
        numerator = [jnp.dot(weight[g].astype(bf16), vb[h, g], preferred_element_type=f32) for g in both]
        fresh = [jnp.exp(own[g] - top[g]) for g in both]
        denominator = [jnp.sum(weight[g], axis=1, keepdims=True) + fresh[g] for g in both]
        logs = [top[g] + jnp.log(denominator[g]) for g in both]
        share = [1.0 / denominator[g] for g in both]
        parts = [(numerator[g] + rounded(fresh[g]) * new_value[g]) * share[g] for g in both]
        parts.append(jnp.where(low, logs[0], logs[1]))
        for i, part in enumerate(parts):
            orr[h, me, i * heads:(i + 1) * heads, :] = part

    def merge(h):
        logs = [orr[h, c, 2 * heads:3 * heads, :] for c in range(n)]
        groups = [[[r * side + b for r in range(side)] for b in range(side)],
                  [[b * side + r for r in range(side)] for b in range(side)]]

        def over(values, op):
            return [[functools.reduce(op, [values[c] for c in group]) for group in part] for part in groups]

        def split(pair, c):
            return jnp.where(low, pair[0][c % side], pair[1][c // side])

        largest = over(logs, jnp.maximum)
        factors = [jnp.exp(logs[c] - split(largest, c)) for c in range(n)]
        sums = over(factors, jnp.add)
        inverses = [[1.0 / s for s in part] for part in sums]
        factors = [factors[c] * split(inverses, c) for c in range(n)]
        swapped = [pltpu.roll(f, half, 1) for f in factors]
        for g in range(2):
            for b, group in enumerate(groups[g]):
                merged = None
                for c in group:
                    factor = jnp.where(low, factors[c], swapped[c]) if g == 0 else jnp.where(low, swapped[c], factors[c])
                    term = orr[h, c, g * heads:(g + 1) * heads, :] * factor
                    merged = term if merged is None else merged + term
                at = (g * side + b) * heads
                cm[h, at:at + heads, :] = merged
        return jnp.concatenate([cm[h, pl.ds(t, batch, stride=heads), :] for t in range(heads)], axis=1).astype(bf16)

    def layer_step(l, carry):
        stream = out_ref[...]
        scaled = (stream * gain[l]).astype(bf16)
        squares = jnp.sum(stream * stream, axis=1, keepdims=True)
        load(WQ, l).wait()
        load(WK, l).wait()
        load(WV, l).wait()

        @pl.when(l + 1 < layers)
        def _():
            for index in range(len(weights)):
                load(index, l + 1).start()

        def put(row, tile):
            qs[pl.ds(row, batch, stride=16), :] = tile

        for i, w in enumerate((wk, wv)):
            kv = jnp.dot(scaled, w[l], preferred_element_type=f32)
            for g in range(2):
                ks[pl.ds(2 * g + i, side, stride=8), :] = kv[g * side:(g + 1) * side]
        put(heads, jnp.broadcast_to(squares, (batch, hd)))
        q = jnp.dot(scaled, wq[l], preferred_element_type=f32)
        for h in range(heads):
            put(h, q[:, h * hd:(h + 1) * hd])
        fresh_sends(lambda c: c.start())
        for k in far_chips:
            for c in q_copies(k):
                c.start()

        odd = lax.rem(l, 2)
        more = l + 1 < layers

        @pl.when(core == 0)
        def _():
            for c in q_copies(n - 1):
                c.start()

            @pl.when(l == 0)
            def _():
                w_out_start(0)

            @pl.when(more)
            def _():
                stage(l + 1)
                w_out_start(l + 1)

            taken(kst.at[l], hs_sem.at[l, 0])
            taken(vst.at[l], hs_sem.at[l, 1])
            for k in range(n):
                for c in q_copies(k):
                    c.wait_send()
            fresh_sends(lambda c: c.wait_send())

            @pl.when(more)
            def _():
                pl.semaphore_wait(go, 1)
                ship_start(l + 1)

            out_ref[...] = out_ref[...] + t_arrivals(odd, 1)

            @pl.when(l == 0)
            def _():
                w_out_copy(0).wait_send()

            @pl.when(more)
            def _():
                w_out_copy(l + 1).wait_send()

        @pl.when(core == 1)
        def _():
            blocks = 2 * side
            taken(kst.at[l, pl.ds(0, blocks - 2)], hs_sem.at[l, 0])
            taken(vst.at[l, pl.ds(0, blocks - 2)], hs_sem.at[l, 1])
            for h in (1, 0):
                taken(krv.at[l, h, pl.ds(0, blocks - 2 * h)], hr_sem.at[l, h, 0])
                taken(vrv.at[l, h, pl.ds(0, blocks - 2 * h)], hr_sem.at[l, h, 1])
                for g in range(2):
                    part = slice(g * side, (g + 1) * side)
                    kb[h, g] = krv[l, h, part].reshape(side * span, hd).astype(bf16)
                    vb[h, g] = vrv[l, h, part].reshape(side * span, hd).astype(bf16)

            @pl.when(y == x)
            def _():
                kr[1, me] = ks[pl.ds(pl.multiple_of(8 * x, 8), 4), :]
                for h in (1, 0):
                    taken(kr.at[h, pl.ds(0, n - h)], kr_sem.at[h])
                    fresh_sum[h] = functools.reduce(jnp.add, [kr[h, c] for c in range(n)])

            for h in (1, 0):
                q_arrivals(h)
                attend(h)
                for k in far_chips:
                    o_copy(h, k).start()

            @pl.when(more)
            def _():
                stage(l + 1)

            load(WO, l).wait()
            taken(wo2.at[l], xr_sem.at[l])
            wob[...] = wo2[l].astype(bf16)
            for k in far_chips:
                for c in q_copies(k):
                    c.wait_send()
            fresh_sends(lambda c: c.wait_send())
            for k in far_chips[11:]:
                taken(orr.at[1, places[k][0]], or_sem.at[1, k])
            @pl.when(more)
            def _():
                pl.semaphore_signal(go, inc=1, device_id={"tp": cores[0]}, device_id_type=MESH)

            @pl.when(more)
            def _():
                ship_start(l + 1)

            for k in far_chips[:11]:
                taken(orr.at[1, places[k][0]], or_sem.at[1, k])
            tps[...] = jnp.dot(merge(1), wo[l], preferred_element_type=f32)
            for k in far_chips:
                taken(orr.at[0, places[k][0]], or_sem.at[0, k])

            tps[...] = tps[...] + jnp.dot(merge(0), wob[...], preferred_element_type=f32)
            for k in range(tn - 1):
                t_copy(odd, k).start()
            for h in (1, 0):
                for k in far_chips:
                    o_copy(h, k).wait_send()
            out_ref[...] = out_ref[...] + tps[...] + t_arrivals(odd, 0)
            for k in range(tn - 1):
                t_copy(odd, k).wait_send()

        return carry

    lax.fori_loop(0, layers, layer_step, 0)


def shards(sizes, hidden, norm_gains, w_query, w_key, w_value, w_out, key_cache, value_cache, lengths):
    n, tn = sizes
    layers, feat, columns = w_query.shape
    batch = hidden.shape[0]
    _, _, _, span, hd = key_cache.shape
    heads = columns // hd
    side = math.isqrt(n)
    dims = (n, tn, side, layers, batch, feat, feat * n, heads, hd, span)
    f32, bf16 = jnp.float32, jnp.bfloat16
    vmem = pl.BlockSpec(memory_space=pltpu.VMEM)
    far = pl.BlockSpec(memory_space=pl.ANY)

    def like(array):
        return pltpu.VMEM(array.shape, array.dtype)

    dma = pltpu.SemaphoreType.DMA
    return pl.pallas_call(
        functools.partial(kernel, dims),
        out_shape=pltpu.VMEM((batch, feat), f32),
        in_specs=[far] * 9,
        out_specs=vmem,
        scratch_shapes=[
            like(hidden), like(norm_gains), pltpu.SMEM(lengths.shape, lengths.dtype),
            like(w_query), like(w_key), like(w_value), like(w_out), like(key_cache), like(value_cache),
            pltpu.VMEM((layers, batch, feat), f32),
            pltpu.VMEM((2, heads, side * span), f32),
            pltpu.VMEM((2, heads, hd), f32),
            pltpu.VMEM((2, heads, hd), f32),
            pltpu.VMEM((batch * 16, hd), f32),
            pltpu.VMEM((2, n, 2, 16, hd), f32),
            pltpu.VMEM((side * 8, hd), f32),
            pltpu.VMEM((2, n, 4, hd), f32),
            pltpu.VMEM((2, 4, hd), f32),
            pltpu.VMEM((layers, batch, span, hd), f32),
            pltpu.VMEM((layers, batch, span, hd), f32),
            pltpu.VMEM((layers, 2, 2 * side, span, hd), f32),
            pltpu.VMEM((layers, 2, 2 * side, span, hd), f32),
            pltpu.VMEM((2, 2, side * span, hd), bf16),
            pltpu.VMEM((2, 2, side * span, hd), bf16),
            pltpu.VMEM((2, n, 3 * heads, hd), f32),
            pltpu.VMEM((2, batch * heads, hd), f32),
            pltpu.VMEM(w_out.shape, f32),
            pltpu.VMEM(w_out.shape, f32),
            pltpu.VMEM(w_out.shape[1:], bf16),
            pltpu.VMEM((batch, feat), f32),
            pltpu.VMEM((2, tn - 1, batch, feat), f32),
            dma((6, layers)),
            dma((n, 2)), dma((2, n, 2)),
            dma((side,)), dma((2,)),
            dma((2, n)), dma((2, n)),
            dma((tn - 1,)), dma((2, tn - 1)),
            dma((layers, 2)), dma((layers, 2, 2)),
            dma((layers,)), dma((layers,)),
            dma((3,)), pltpu.SemaphoreType.REGULAR, pltpu.SemaphoreType.REGULAR,
        ],
        compiler_params=pltpu.CompilerParams(
            collective_id=0, has_side_effects=True, vmem_limit_bytes=60 * 1024 * 1024),
    )(hidden, norm_gains, lengths, w_query, w_key, w_value, w_out, key_cache, value_cache)


def solution(mesh):
    sizes = (mesh.shape["ctx"], mesh.shape["tp"])
    return jax.shard_map(
        functools.partial(shards, sizes),
        mesh=mesh,
        in_specs=(
            P(None, "ctx"),
            P(None, "ctx"),
            P(None, "ctx", "tp"),
            P(None, "ctx", "tp"),
            P(None, "ctx", "tp"),
            P(None, "tp", "ctx"),
            P(None, None, "tp", "ctx", None),
            P(None, None, "tp", "ctx", None),
            P(),
        ),
        out_specs=P(None, "ctx"),
        check_vma=False,
    )
```

```python
import functools
import math

import jax
import jax.numpy as jnp
from jax import lax
from jax.experimental import pallas as pl
from jax.experimental.pallas import tpu as pltpu
from jax.sharding import PartitionSpec as P

mask_fill = -1e30
norm_eps = 1e-05
rope_base = 500000.0
MESH = pl.DeviceIdType.MESH
QROWS = 9
ROWS = 17


def kernel(dims, hidden_h, gains_h, lengths_h, wq_h, wk_h, wv_h, wo_h, kc_h, vc_h, out_ref,
           hidden_ref, gains_ref, lengths_ref, wq, wk, wv, wo, kc, vc, gain, bias, cosine, sine, qs, qr, ks, kr, fresh_sum, kst, vst, krv, vrv, kb, vb,
           orr, cm, wst, wo2, wob, tps, tpr, w_sem, qs_sem, qr_sem, ks_sem, kr_sem, os_sem, or_sem, ts_sem, tr_sem, hs_sem, hr_sem, xs_sem, xr_sem, small_sem, ready, go):
    n, tn, side, layers, batch, feat, total, heads, hd, span = dims
    f32, bf16 = jnp.float32, jnp.bfloat16
    scale = 1.0 / math.sqrt(hd)
    me = lax.axis_index("ctx")
    mt = lax.axis_index("tp")
    y, x = me // side, lax.rem(me, side)
    z, core = mt // 2, lax.rem(mt, 2)
    zn = tn // 2
    weights = ((kc_h, kc), (vc_h, vc), (wq_h, wq), (wk_h, wk), (wv_h, wv), (wo_h, wo))
    KC, VC, WQ, WK, WV, WO = range(6)

    def load(index, layer):
        source, target = weights[index]
        return pltpu.make_async_copy(source.at[layer], target.at[layer], w_sem.at[index, layer])

    def hops(step, size):
        return min(step, size - step)

    offsets = [(dy, dx) for dy in range(side) for dx in range(side) if (dy, dx) != (0, 0)]
    offsets.sort(key=lambda o: -(hops(o[0], side) + hops(o[1], side)))
    peers = []
    for dy, dx in offsets:
        py, px = lax.rem(y + dy, side), lax.rem(x + dx, side)
        peers.append((py * side + px, py, px))
    toffsets = [(dz, dc) for dz in range(zn) for dc in range(2) if (dz, dc) != (0, 0)]
    toffsets.sort(key=lambda o: -(2 * hops(o[0], zn) + o[1]))
    tpeers = [lax.rem(z + dz, zn) * 2 + lax.rem(core + dc, 2) for dz, dc in toffsets]

    column = [lax.rem(y + r, side) * side + x for r in range(1, side)]
    row = [y * side + lax.rem(x + r, side) for r in range(1, side)]
    barrier = pltpu.get_barrier_semaphore()
    cores = (2 * z, 2 * z + 1)
    for p in row + column:
        for t in cores:
            pl.semaphore_signal(barrier, inc=1, device_id={"ctx": p, "tp": t}, device_id_type=MESH)
    for p in tpeers:
        pl.semaphore_signal(barrier, inc=1, device_id={"tp": p}, device_id_type=MESH)

    smalls = [pltpu.make_async_copy(source, target, small_sem.at[i]) for i, (source, target) in enumerate(
        ((hidden_h, hidden_ref), (gains_h, gains_ref), (lengths_h, lengths_ref)))]
    for index in (KC, VC):
        load(index, 0).start()
    for c in smalls:
        c.start()
    for index in (WQ, WK, WV, WO):
        load(index, 0).start()
    for c in smalls:
        c.wait()

    half = hd // 2
    lane = lax.broadcasted_iota(jnp.int32, (heads, hd), 1)
    low = lane < half
    head = lax.broadcasted_iota(jnp.int32, (heads, hd), 0)
    picks = (lane == head, lane == head + half)
    mine = (x, side + y)
    slot = lax.broadcasted_iota(jnp.int32, (heads, side * span), 1)
    block = slot // span
    positions = (y * side * span + slot, (block * side + x) * span + lax.rem(slot, span))
    exponent = jnp.where(low, lane, lane - half).astype(f32) * (2.0 / hd)
    frequency = jnp.exp(-exponent * math.log(rope_base))
    for g in range(2):
        size = lengths_ref[mine[g]]
        bias[g] = jnp.where(positions[g] < size, 0.0, mask_fill)
        angle = jnp.full((heads, hd), size, jnp.int32).astype(f32) * frequency
        cosine[g] = jnp.cos(angle)
        sine[g] = jnp.where(low, -jnp.sin(angle), jnp.sin(angle))
    for l in range(layers):
        gain[l] = jnp.broadcast_to(gains_ref[l:l + 1, :].astype(f32), (batch, feat))
    out_ref[...] = hidden_ref[...].astype(f32)
    own_mask = jnp.where(jnp.full((heads, 1), y, jnp.int32) == jnp.full((heads, 1), x, jnp.int32), 0.0, mask_fill)

    def ship(l, rounds):
        copies = []
        for r in rounds:
            px, py = lax.rem(x + r, side), lax.rem(y + r, side)
            for i, (source, target) in enumerate(((kst, krv), (vst, vrv))):
                copies.append(pltpu.make_async_remote_copy(
                    src_ref=source.at[l, px], dst_ref=target.at[l, core, x],
                    send_sem=hs_sem.at[l, i], recv_sem=hr_sem.at[l, core, i],
                    device_id={"ctx": y * side + px, "tp": cores[1]}, device_id_type=MESH))
                copies.append(pltpu.make_async_remote_copy(
                    src_ref=source.at[l, side + py], dst_ref=target.at[l, core, side + y],
                    send_sem=hs_sem.at[l, i], recv_sem=hr_sem.at[l, core, i],
                    device_id={"ctx": py * side + x, "tp": cores[1]}, device_id_type=MESH))
        return copies

    def ship_start(l):
        for c in ship(l, (2, 1, 3)):
            c.start()

        @pl.when(core == 0)
        def _():
            for c in ship(l, (0,)):
                c.start()

    def taken(ref, sem):
        pltpu.make_async_copy(ref, ref, sem).wait()

    def stage(l):
        load(KC, l).wait()
        load(VC, l).wait()
        for source, staged, held in ((kc, kst, krv), (vc, vst, vrv)):
            for b in range(batch):
                staged[l, b] = source[l, b, 0].astype(f32)

            @pl.when(core == 1)
            def _():
                held[l, 1, x] = source[l, mine[0], 0].astype(f32)
                held[l, 1, side + y] = source[l, mine[1], 0].astype(f32)

    def fresh_copy(d):
        return pltpu.make_async_remote_copy(
            src_ref=ks.at[pl.ds(8 * d, 4)], dst_ref=kr.at[core, me], send_sem=ks_sem.at[d], recv_sem=kr_sem.at[core],
            device_id={"ctx": d * side + d, "tp": cores[1]}, device_id_type=MESH)

    def fresh_sends(act):
        for d in range(side):
            @pl.when(jnp.logical_or(core == 0, me != d * side + d))
            def _():
                act(fresh_copy(d))

    places = peers + [(me, y, x)]
    far_chips = range(n - 1)

    def q_copies(k):
        p, py, px = places[k]
        return [pltpu.make_async_remote_copy(
            src_ref=qs.at[pl.ds(pl.multiple_of(b * 16, 16), QROWS)], dst_ref=qr.at[core, k, g, pl.ds(0, QROWS)],
            send_sem=qs_sem.at[k, g], recv_sem=qr_sem.at[core, k, g],
            device_id={"ctx": p, "tp": cores[1]}, device_id_type=MESH) for g, b in ((0, px), (1, side + py))]

    def q_arrivals(h):
        for k in range(n - h):
            for g in range(2):
                taken(qr.at[h, k, g, pl.ds(0, QROWS)], qr_sem.at[h, k, g])

    def o_copy(h, k):
        return pltpu.make_async_remote_copy(
            src_ref=orr.at[h, me, pl.ds(0, ROWS)], dst_ref=orr.at[h, me, pl.ds(0, ROWS)], send_sem=os_sem.at[h, k], recv_sem=or_sem.at[h, k],
            device_id={"ctx": places[k][0]}, device_id_type=MESH)

    def w_out_copy(l):
        return pltpu.make_async_remote_copy(
            src_ref=wst.at[l], dst_ref=wo2.at[l], send_sem=xs_sem.at[l], recv_sem=xr_sem.at[l],
            device_id={"tp": cores[1]}, device_id_type=MESH)

    def w_out_start(l):
        load(WO, l).wait()
        wst[l] = wo[l].astype(f32)
        w_out_copy(l).start()

    def t_copy(odd, k):
        return pltpu.make_async_remote_copy(
            src_ref=tps, dst_ref=tpr.at[odd, k], send_sem=ts_sem.at[k], recv_sem=tr_sem.at[odd, k],
            device_id={"tp": tpeers[k]}, device_id_type=MESH)

    def t_arrivals(odd, cross):
        moved = None
        for k, (dz, dc) in enumerate(toffsets):
            if dc == cross:
                taken(tpr.at[odd, k], tr_sem.at[odd, k])
                moved = tpr[odd, k] if moved is None else moved + tpr[odd, k]
        return moved

    fresh_sum[...] = jnp.zeros_like(fresh_sum)
    stage(0)
    pl.semaphore_wait(barrier, 2 * len(row) + 2 * len(column) + len(tpeers))
    for p in column:
        for t in cores:
            pl.semaphore_signal(ready, inc=1, device_id={"ctx": p, "tp": t}, device_id_type=MESH)
    ship_start(0)
    pl.semaphore_wait(ready, 2 * len(column))

    def rotate(u, g):
        return u * cosine[g] + pltpu.roll(u, half, 1) * sine[g]

    def rounded(u):
        return u.astype(bf16).astype(f32)

    def attend(h):
        both = range(2)
        inverse, query = [], []
        for g in both:
            whole, square = qr[h, 0, g, 0:heads], qr[h, 0, g, heads:QROWS]
            for k in range(1, n - h):
                whole = whole + qr[h, k, g, 0:heads]
                square = square + qr[h, k, g, heads:QROWS]
            if h:
                at = pl.multiple_of(mine[g] * 16, 16)
                whole = whole + qs[pl.ds(at, heads), :]
                square = square + qs[pl.ds(pl.multiple_of(at + 8, 8), 1), :]
            inverse.append(lax.rsqrt(square / total + norm_eps))
            query.append(rounded(rotate(whole * inverse[g], g)))
        score = [lax.dot_general(
            query[g].astype(bf16), kb[h, g], (((1,), (1,)), ((), ())), preferred_element_type=f32) for g in both]
        new_key = [rounded(rotate(jnp.broadcast_to(fresh_sum[h, 2 * g:2 * g + 1] * inverse[g], (heads, hd)), g)) for g in both]
        new_value = [rounded(fresh_sum[h, 2 * g + 1:2 * g + 2] * inverse[g]) for g in both]
        own = [jnp.sum(query[g] * new_key[g], axis=1, keepdims=True) * scale + own_mask for g in both]
        masked = [score[g] * scale + bias[g] for g in both]
        top = [jnp.maximum(jnp.max(masked[g], axis=1, keepdims=True), own[g]) for g in both]
        weight = [jnp.exp(masked[g] - top[g]) for g in both]
        numerator = [jnp.dot(weight[g].astype(bf16), vb[h, g], preferred_element_type=f32) for g in both]
        fresh = [jnp.exp(own[g] - top[g]) for g in both]
        denominator = [jnp.sum(weight[g], axis=1, keepdims=True) + fresh[g] for g in both]
        logs = [top[g] + jnp.log(denominator[g]) for g in both]
        share = [1.0 / denominator[g] for g in both]
        parts = [(numerator[g] + rounded(fresh[g]) * new_value[g]) * share[g] for g in both]
        for g in both:
            orr[h, me, g * heads:(g + 1) * heads, :] = parts[g]
        spread = jnp.where(picks[0], logs[0], jnp.where(picks[1], logs[1], 0.0))
        orr[h, me, 2 * heads:ROWS, :] = jnp.sum(spread, axis=0, keepdims=True)

    def merge(h):
        logs = [orr[h, c, 2 * heads:ROWS, :] for c in range(n)]
        groups = [[[r * side + b for r in range(side)] for b in range(side)],
                  [[b * side + r for r in range(side)] for b in range(side)]]

        def over(values, op):
            return [[functools.reduce(op, [values[c] for c in group]) for group in part] for part in groups]

        def split(pair, c):
            return jnp.where(low[0:1], pair[0][c % side], pair[1][c // side])

        largest = over(logs, jnp.maximum)
        factors = [jnp.exp(logs[c] - split(largest, c)) for c in range(n)]
        sums = over(factors, jnp.add)
        inverses = [[1.0 / s for s in part] for part in sums]
        factors = [factors[c] * split(inverses, c) for c in range(n)]
        factors = [jnp.broadcast_to(f, (heads, hd)) for f in factors]
        for g in range(2):
            for b, group in enumerate(groups[g]):
                merged = None
                for c in group:
                    factor = jnp.sum(jnp.where(picks[g], factors[c], 0.0), axis=1, keepdims=True)
                    term = orr[h, c, g * heads:(g + 1) * heads, :] * factor
                    merged = term if merged is None else merged + term
                at = (g * side + b) * heads
                cm[h, at:at + heads, :] = merged
        return jnp.concatenate([cm[h, pl.ds(t, batch, stride=heads), :] for t in range(heads)], axis=1).astype(bf16)

    def layer_step(l, carry):
        stream = out_ref[...]
        scaled = (stream * gain[l]).astype(bf16)
        squares = jnp.sum(stream * stream, axis=1, keepdims=True)
        load(WQ, l).wait()
        load(WK, l).wait()
        load(WV, l).wait()

        @pl.when(l + 1 < layers)
        def _():
            for index in range(len(weights)):
                load(index, l + 1).start()

        def put(row, tile):
            qs[pl.ds(row, batch, stride=16), :] = tile

        for i, w in enumerate((wk, wv)):
            kv = jnp.dot(scaled, w[l], preferred_element_type=f32)
            for g in range(2):
                ks[pl.ds(2 * g + i, side, stride=8), :] = kv[g * side:(g + 1) * side]
        put(heads, jnp.broadcast_to(squares, (batch, hd)))
        q = jnp.dot(scaled, wq[l], preferred_element_type=f32)
        for h in range(heads):
            put(h, q[:, h * hd:(h + 1) * hd])
        fresh_sends(lambda c: c.start())
        for k in far_chips:
            for c in q_copies(k):
                c.start()

        odd = lax.rem(l, 2)
        more = l + 1 < layers

        @pl.when(core == 0)
        def _():
            for c in q_copies(n - 1):
                c.start()

            @pl.when(l == 0)
            def _():
                w_out_start(0)

            @pl.when(more)
            def _():
                stage(l + 1)
                w_out_start(l + 1)

            taken(kst.at[l], hs_sem.at[l, 0])
            taken(vst.at[l], hs_sem.at[l, 1])
            for k in range(n):
                for c in q_copies(k):
                    c.wait_send()
            fresh_sends(lambda c: c.wait_send())

            @pl.when(more)
            def _():
                pl.semaphore_wait(go, 1)
                ship_start(l + 1)

            out_ref[...] = out_ref[...] + t_arrivals(odd, 1)

            @pl.when(l == 0)
            def _():
                w_out_copy(0).wait_send()

            @pl.when(more)
            def _():
                w_out_copy(l + 1).wait_send()

        @pl.when(core == 1)
        def _():
            blocks = 2 * side
            taken(kst.at[l, pl.ds(0, blocks - 2)], hs_sem.at[l, 0])
            taken(vst.at[l, pl.ds(0, blocks - 2)], hs_sem.at[l, 1])
            for h in (1, 0):
                taken(krv.at[l, h, pl.ds(0, blocks - 2 * h)], hr_sem.at[l, h, 0])
                taken(vrv.at[l, h, pl.ds(0, blocks - 2 * h)], hr_sem.at[l, h, 1])
                for g in range(2):
                    part = slice(g * side, (g + 1) * side)
                    kb[h, g] = krv[l, h, part].reshape(side * span, hd).astype(bf16)
                    vb[h, g] = vrv[l, h, part].reshape(side * span, hd).astype(bf16)

            for h in (1, 0):
                @pl.when(y == x)
                def _():
                    if h:
                        kr[1, me] = ks[pl.ds(pl.multiple_of(8 * x, 8), 4), :]
                    taken(kr.at[h, pl.ds(0, n - h)], kr_sem.at[h])
                    fresh_sum[h] = functools.reduce(jnp.add, [kr[h, c] for c in range(n)])

                q_arrivals(h)
                attend(h)
                for k in far_chips:
                    o_copy(h, k).start()

            @pl.when(more)
            def _():
                stage(l + 1)

            load(WO, l).wait()
            taken(wo2.at[l], xr_sem.at[l])
            wob[...] = wo2[l].astype(bf16)
            for k in far_chips:
                for c in q_copies(k):
                    c.wait_send()
            fresh_sends(lambda c: c.wait_send())
            for k in far_chips[13:15]:
                taken(orr.at[1, places[k][0], pl.ds(0, ROWS)], or_sem.at[1, k])
            @pl.when(more)
            def _():
                pl.semaphore_signal(go, inc=1, device_id={"tp": cores[0]}, device_id_type=MESH)

            @pl.when(more)
            def _():
                ship_start(l + 1)

            for k in far_chips[0:13]:
                taken(orr.at[1, places[k][0], pl.ds(0, ROWS)], or_sem.at[1, k])
            tps[...] = jnp.dot(merge(1), wo[l], preferred_element_type=f32)
            for k in far_chips:
                taken(orr.at[0, places[k][0], pl.ds(0, ROWS)], or_sem.at[0, k])

            tps[...] = tps[...] + jnp.dot(merge(0), wob[...], preferred_element_type=f32)
            for k in range(tn - 1):
                t_copy(odd, k).start()
            for h in (1, 0):
                for k in far_chips:
                    o_copy(h, k).wait_send()
            out_ref[...] = out_ref[...] + tps[...] + t_arrivals(odd, 0)
            for k in range(tn - 1):
                t_copy(odd, k).wait_send()

        return carry

    lax.fori_loop(0, layers, layer_step, 0)


def shards(sizes, hidden, norm_gains, w_query, w_key, w_value, w_out, key_cache, value_cache, lengths):
    n, tn = sizes
    layers, feat, columns = w_query.shape
    batch = hidden.shape[0]
    _, _, _, span, hd = key_cache.shape
    heads = columns // hd
    side = math.isqrt(n)
    dims = (n, tn, side, layers, batch, feat, feat * n, heads, hd, span)
    f32, bf16 = jnp.float32, jnp.bfloat16
    vmem = pl.BlockSpec(memory_space=pltpu.VMEM)
    far = pl.BlockSpec(memory_space=pl.ANY)

    def like(array):
        return pltpu.VMEM(array.shape, array.dtype)

    dma = pltpu.SemaphoreType.DMA
    return pl.pallas_call(
        functools.partial(kernel, dims),
        out_shape=pltpu.VMEM((batch, feat), f32),
        in_specs=[far] * 9,
        out_specs=vmem,
        scratch_shapes=[
            like(hidden), like(norm_gains), pltpu.SMEM(lengths.shape, lengths.dtype),
            like(w_query), like(w_key), like(w_value), like(w_out), like(key_cache), like(value_cache),
            pltpu.VMEM((layers, batch, feat), f32),
            pltpu.VMEM((2, heads, side * span), f32),
            pltpu.VMEM((2, heads, hd), f32),
            pltpu.VMEM((2, heads, hd), f32),
            pltpu.VMEM((batch * 16, hd), f32),
            pltpu.VMEM((2, n, 2, 16, hd), f32),
            pltpu.VMEM((side * 8, hd), f32),
            pltpu.VMEM((2, n, 4, hd), f32),
            pltpu.VMEM((2, 4, hd), f32),
            pltpu.VMEM((layers, batch, span, hd), f32),
            pltpu.VMEM((layers, batch, span, hd), f32),
            pltpu.VMEM((layers, 2, 2 * side, span, hd), f32),
            pltpu.VMEM((layers, 2, 2 * side, span, hd), f32),
            pltpu.VMEM((2, 2, side * span, hd), bf16),
            pltpu.VMEM((2, 2, side * span, hd), bf16),
            pltpu.VMEM((2, n, 3 * heads, hd), f32),
            pltpu.VMEM((2, batch * heads, hd), f32),
            pltpu.VMEM(w_out.shape, f32),
            pltpu.VMEM(w_out.shape, f32),
            pltpu.VMEM(w_out.shape[1:], bf16),
            pltpu.VMEM((batch, feat), f32),
            pltpu.VMEM((2, tn - 1, batch, feat), f32),
            dma((6, layers)),
            dma((n, 2)), dma((2, n, 2)),
            dma((side,)), dma((2,)),
            dma((2, n)), dma((2, n)),
            dma((tn - 1,)), dma((2, tn - 1)),
            dma((layers, 2)), dma((layers, 2, 2)),
            dma((layers,)), dma((layers,)),
            dma((3,)), pltpu.SemaphoreType.REGULAR, pltpu.SemaphoreType.REGULAR,
        ],
        compiler_params=pltpu.CompilerParams(
            collective_id=0, has_side_effects=True, vmem_limit_bytes=60 * 1024 * 1024),
    )(hidden, norm_gains, lengths, w_query, w_key, w_value, w_out, key_cache, value_cache)


def solution(mesh):
    sizes = (mesh.shape["ctx"], mesh.shape["tp"])
    return jax.shard_map(
        functools.partial(shards, sizes),
        mesh=mesh,
        in_specs=(
            P(None, "ctx"),
            P(None, "ctx"),
            P(None, "ctx", "tp"),
            P(None, "ctx", "tp"),
            P(None, "ctx", "tp"),
            P(None, "tp", "ctx"),
            P(None, None, "tp", "ctx", None),
            P(None, None, "tp", "ctx", None),
            P(),
        ),
        out_specs=P(None, "ctx"),
        check_vma=False,
    )
```

```python
import functools
import math

import jax
import jax.numpy as jnp
from jax import lax
from jax.experimental import pallas as pl
from jax.experimental.pallas import tpu as pltpu
from jax.sharding import PartitionSpec as P

mask_fill = -1e30
norm_eps = 1e-05
rope_base = 500000.0
MESH = pl.DeviceIdType.MESH
QROWS = 9
ROWS = 17


def kernel(dims, hidden_h, gains_h, lengths_h, wq_h, wk_h, wv_h, wo_h, kc_h, vc_h, out_ref,
           hidden_ref, gains_ref, lengths_ref, wq, wk, wv, wo, kc, vc, gain, bias, cosine, sine, qs, qr, ks, kr, fresh_sum, kst, vst, krv, vrv, kb, vb,
           orr, cm, wst, wo2, wob, tps, tpr, w_sem, qs_sem, qr_sem, ks_sem, kr_sem, os_sem, or_sem, ts_sem, tr_sem, hs_sem, hr_sem, xs_sem, xr_sem, small_sem, ready, go):
    n, tn, side, layers, batch, feat, total, heads, hd, span = dims
    f32, bf16 = jnp.float32, jnp.bfloat16
    scale = 1.0 / math.sqrt(hd)
    me = lax.axis_index("ctx")
    mt = lax.axis_index("tp")
    y, x = me // side, lax.rem(me, side)
    z, core = mt // 2, lax.rem(mt, 2)
    zn = tn // 2
    weights = ((kc_h, kc), (vc_h, vc), (wq_h, wq), (wk_h, wk), (wv_h, wv), (wo_h, wo))
    KC, VC, WQ, WK, WV, WO = range(6)

    def load(index, layer):
        source, target = weights[index]
        return pltpu.make_async_copy(source.at[layer], target.at[layer], w_sem.at[index, layer])

    def hops(step, size):
        return min(step, size - step)

    offsets = [(dy, dx) for dy in range(side) for dx in range(side) if (dy, dx) != (0, 0)]
    offsets.sort(key=lambda o: -(hops(o[0], side) + hops(o[1], side)))
    peers = []
    for dy, dx in offsets:
        py, px = lax.rem(y + dy, side), lax.rem(x + dx, side)
        peers.append((py * side + px, py, px))
    toffsets = [(dz, dc) for dz in range(zn) for dc in range(2) if (dz, dc) != (0, 0)]
    toffsets.sort(key=lambda o: -(2 * hops(o[0], zn) + o[1]))
    tpeers = [lax.rem(z + dz, zn) * 2 + lax.rem(core + dc, 2) for dz, dc in toffsets]

    column = [lax.rem(y + r, side) * side + x for r in range(1, side)]
    row = [y * side + lax.rem(x + r, side) for r in range(1, side)]
    barrier = pltpu.get_barrier_semaphore()
    cores = (2 * z, 2 * z + 1)
    for p in row + column:
        for t in cores:
            pl.semaphore_signal(barrier, inc=1, device_id={"ctx": p, "tp": t}, device_id_type=MESH)
    for p in tpeers:
        pl.semaphore_signal(barrier, inc=1, device_id={"tp": p}, device_id_type=MESH)

    smalls = [pltpu.make_async_copy(source, target, small_sem.at[i]) for i, (source, target) in enumerate(
        ((hidden_h, hidden_ref), (gains_h, gains_ref), (lengths_h, lengths_ref)))]
    for index in (KC, VC):
        load(index, 0).start()
    for c in smalls:
        c.start()
    for index in (WQ, WK, WV, WO):
        load(index, 0).start()
    for c in smalls:
        c.wait()

    half = hd // 2
    lane = lax.broadcasted_iota(jnp.int32, (heads, hd), 1)
    low = lane < half
    head = lax.broadcasted_iota(jnp.int32, (heads, hd), 0)
    picks = (lane == head, lane == head + half)
    mine = (x, side + y)
    slot = lax.broadcasted_iota(jnp.int32, (heads, side * span), 1)
    block = slot // span
    positions = (y * side * span + slot, (block * side + x) * span + lax.rem(slot, span))
    exponent = jnp.where(low, lane, lane - half).astype(f32) * (2.0 / hd)
    frequency = jnp.exp(-exponent * math.log(rope_base))
    for g in range(2):
        size = lengths_ref[mine[g]]
        bias[g] = jnp.where(positions[g] < size, 0.0, mask_fill)
        angle = jnp.full((heads, hd), size, jnp.int32).astype(f32) * frequency
        cosine[g] = jnp.cos(angle)
        sine[g] = jnp.where(low, -jnp.sin(angle), jnp.sin(angle))
    for l in range(layers):
        gain[l] = jnp.broadcast_to(gains_ref[l:l + 1, :].astype(f32), (batch, feat))
    out_ref[...] = hidden_ref[...].astype(f32)
    own_mask = jnp.where(jnp.full((heads, 1), y, jnp.int32) == jnp.full((heads, 1), x, jnp.int32), 0.0, mask_fill)

    def ship(l, rounds):
        copies = []
        for r in rounds:
            px, py = lax.rem(x + r, side), lax.rem(y + r, side)
            for i, (source, target) in enumerate(((kst, krv), (vst, vrv))):
                copies.append(pltpu.make_async_remote_copy(
                    src_ref=source.at[l, px], dst_ref=target.at[l, core, x],
                    send_sem=hs_sem.at[l, i], recv_sem=hr_sem.at[l, core, i],
                    device_id={"ctx": y * side + px, "tp": cores[1]}, device_id_type=MESH))
                copies.append(pltpu.make_async_remote_copy(
                    src_ref=source.at[l, side + py], dst_ref=target.at[l, core, side + y],
                    send_sem=hs_sem.at[l, i], recv_sem=hr_sem.at[l, core, i],
                    device_id={"ctx": py * side + x, "tp": cores[1]}, device_id_type=MESH))
        return copies

    def ship_start(l):
        for c in ship(l, (2, 1, 3)):
            c.start()

        @pl.when(core == 0)
        def _():
            for c in ship(l, (0,)):
                c.start()

    def taken(ref, sem):
        pltpu.make_async_copy(ref, ref, sem).wait()

    def stage(l):
        load(KC, l).wait()
        load(VC, l).wait()
        for source, staged, held in ((kc, kst, krv), (vc, vst, vrv)):
            for b in range(batch):
                staged[l, b] = source[l, b, 0].astype(f32)

            @pl.when(core == 1)
            def _():
                held[l, 1, x] = source[l, mine[0], 0].astype(f32)
                held[l, 1, side + y] = source[l, mine[1], 0].astype(f32)

    def fresh_copy(d):
        return pltpu.make_async_remote_copy(
            src_ref=ks.at[pl.ds(8 * d, 4)], dst_ref=kr.at[core, me], send_sem=ks_sem.at[d], recv_sem=kr_sem.at[core],
            device_id={"ctx": d * side + d, "tp": cores[1]}, device_id_type=MESH)

    def fresh_sends(act):
        for d in range(side):
            @pl.when(jnp.logical_or(core == 0, me != d * side + d))
            def _():
                act(fresh_copy(d))

    places = peers + [(me, y, x)]
    far_chips = range(n - 1)

    def q_copies(k):
        p, py, px = places[k]
        return [pltpu.make_async_remote_copy(
            src_ref=qs.at[pl.ds(pl.multiple_of(b * 16, 16), QROWS)], dst_ref=qr.at[core, k, g, pl.ds(0, QROWS)],
            send_sem=qs_sem.at[k, g], recv_sem=qr_sem.at[core, k, g],
            device_id={"ctx": p, "tp": cores[1]}, device_id_type=MESH) for g, b in ((0, px), (1, side + py))]

    def q_arrivals(h):
        for k in range(n - h):
            for g in range(2):
                taken(qr.at[h, k, g, pl.ds(0, QROWS)], qr_sem.at[h, k, g])

    def o_copy(h, k):
        return pltpu.make_async_remote_copy(
            src_ref=orr.at[h, me, pl.ds(0, ROWS)], dst_ref=orr.at[h, me, pl.ds(0, ROWS)], send_sem=os_sem.at[h, k], recv_sem=or_sem.at[h, k],
            device_id={"ctx": places[k][0]}, device_id_type=MESH)

    def w_out_copy(l):
        return pltpu.make_async_remote_copy(
            src_ref=wst.at[l], dst_ref=wo2.at[l], send_sem=xs_sem.at[l], recv_sem=xr_sem.at[l],
            device_id={"tp": cores[1]}, device_id_type=MESH)

    def w_out_start(l):
        load(WO, l).wait()
        wst[l] = wo[l].astype(f32)
        w_out_copy(l).start()

    def t_copy(odd, k):
        return pltpu.make_async_remote_copy(
            src_ref=tps, dst_ref=tpr.at[odd, k], send_sem=ts_sem.at[k], recv_sem=tr_sem.at[odd, k],
            device_id={"tp": tpeers[k]}, device_id_type=MESH)

    def t_arrivals(odd, cross):
        moved = None
        for k, (dz, dc) in enumerate(toffsets):
            if dc == cross:
                taken(tpr.at[odd, k], tr_sem.at[odd, k])
                moved = tpr[odd, k] if moved is None else moved + tpr[odd, k]
        return moved

    fresh_sum[...] = jnp.zeros_like(fresh_sum)
    stage(0)
    pl.semaphore_wait(barrier, 2 * len(row) + 2 * len(column) + len(tpeers))
    for p in column:
        for t in cores:
            pl.semaphore_signal(ready, inc=1, device_id={"ctx": p, "tp": t}, device_id_type=MESH)
    ship_start(0)
    pl.semaphore_wait(ready, 2 * len(column))

    def rotate(u, g):
        return u * cosine[g] + pltpu.roll(u, half, 1) * sine[g]

    def rounded(u):
        return u.astype(bf16).astype(f32)

    def attend(h):
        both = range(2)
        inverse, query = [], []
        for g in both:
            whole, square = qr[h, 0, g, 0:heads], qr[h, 0, g, heads:QROWS]
            for k in range(1, n - h):
                whole = whole + qr[h, k, g, 0:heads]
                square = square + qr[h, k, g, heads:QROWS]
            if h:
                at = pl.multiple_of(mine[g] * 16, 16)
                whole = whole + qs[pl.ds(at, heads), :]
                square = square + qs[pl.ds(pl.multiple_of(at + 8, 8), 1), :]
            inverse.append(lax.rsqrt(square / total + norm_eps))
            query.append(rounded(rotate(whole * inverse[g], g)))
        score = [lax.dot_general(
            query[g].astype(bf16), kb[h, g], (((1,), (1,)), ((), ())), preferred_element_type=f32) for g in both]
        new_key = [rounded(rotate(jnp.broadcast_to(fresh_sum[h, 2 * g:2 * g + 1] * inverse[g], (heads, hd)), g)) for g in both]
        new_value = [rounded(fresh_sum[h, 2 * g + 1:2 * g + 2] * inverse[g]) for g in both]
        own = [jnp.sum(query[g] * new_key[g], axis=1, keepdims=True) * scale + own_mask for g in both]
        masked = [score[g] * scale + bias[g] for g in both]
        top = [jnp.maximum(jnp.max(masked[g], axis=1, keepdims=True), own[g]) for g in both]
        weight = [jnp.exp(masked[g] - top[g]) for g in both]
        numerator = [jnp.dot(weight[g].astype(bf16), vb[h, g], preferred_element_type=f32) for g in both]
        fresh = [jnp.exp(own[g] - top[g]) for g in both]
        denominator = [jnp.sum(weight[g], axis=1, keepdims=True) + fresh[g] for g in both]
        logs = [top[g] + jnp.log(denominator[g]) for g in both]
        share = [1.0 / denominator[g] for g in both]
        parts = [(numerator[g] + rounded(fresh[g]) * new_value[g]) * share[g] for g in both]
        for g in both:
            orr[h, me, g * heads:(g + 1) * heads, :] = parts[g]
        spread = jnp.where(picks[0], logs[0], jnp.where(picks[1], logs[1], 0.0))
        orr[h, me, 2 * heads:ROWS, :] = jnp.sum(spread, axis=0, keepdims=True)

    def merge(h):
        logs = [orr[h, c, 2 * heads:ROWS, :] for c in range(n)]
        groups = [[[r * side + b for r in range(side)] for b in range(side)],
                  [[b * side + r for r in range(side)] for b in range(side)]]

        def over(values, op):
            return [[functools.reduce(op, [values[c] for c in group]) for group in part] for part in groups]

        def split(pair, c):
            return jnp.where(low[0:1], pair[0][c % side], pair[1][c // side])

        largest = over(logs, jnp.maximum)
        factors = [jnp.exp(logs[c] - split(largest, c)) for c in range(n)]
        sums = over(factors, jnp.add)
        inverses = [[1.0 / s for s in part] for part in sums]
        factors = [factors[c] * split(inverses, c) for c in range(n)]
        factors = [jnp.broadcast_to(f, (heads, hd)) for f in factors]
        for g in range(2):
            for b, group in enumerate(groups[g]):
                merged = None
                for c in group:
                    factor = jnp.sum(jnp.where(picks[g], factors[c], 0.0), axis=1, keepdims=True)
                    term = orr[h, c, g * heads:(g + 1) * heads, :] * factor
                    merged = term if merged is None else merged + term
                at = (g * side + b) * heads
                cm[h, at:at + heads, :] = merged
        return jnp.concatenate([cm[h, pl.ds(t, batch, stride=heads), :] for t in range(heads)], axis=1).astype(bf16)

    def layer_step(l, carry):
        stream = out_ref[...]
        scaled = (stream * gain[l]).astype(bf16)
        squares = jnp.sum(stream * stream, axis=1, keepdims=True)
        load(WQ, l).wait()
        load(WK, l).wait()
        load(WV, l).wait()

        @pl.when(l + 1 < layers)
        def _():
            for index in range(len(weights)):
                load(index, l + 1).start()

        def put(row, tile):
            qs[pl.ds(row, batch, stride=16), :] = tile

        for i, w in enumerate((wk, wv)):
            kv = jnp.dot(scaled, w[l], preferred_element_type=f32)
            for g in range(2):
                ks[pl.ds(2 * g + i, side, stride=8), :] = kv[g * side:(g + 1) * side]
        put(heads, jnp.broadcast_to(squares, (batch, hd)))
        q = jnp.dot(scaled, wq[l], preferred_element_type=f32)
        for h in range(heads):
            put(h, q[:, h * hd:(h + 1) * hd])
        fresh_sends(lambda c: c.start())
        for k in far_chips:
            for c in q_copies(k):
                c.start()

        odd = lax.rem(l, 2)
        more = l + 1 < layers

        @pl.when(core == 0)
        def _():
            for c in q_copies(n - 1):
                c.start()

            @pl.when(l == 0)
            def _():
                w_out_start(0)

            @pl.when(more)
            def _():
                stage(l + 1)
                w_out_start(l + 1)

            taken(kst.at[l], hs_sem.at[l, 0])
            taken(vst.at[l], hs_sem.at[l, 1])
            for k in range(n):
                for c in q_copies(k):
                    c.wait_send()
            fresh_sends(lambda c: c.wait_send())

            @pl.when(more)
            def _():
                pl.semaphore_wait(go, 1)
                ship_start(l + 1)

            out_ref[...] = out_ref[...] + t_arrivals(odd, 1)

            @pl.when(l == 0)
            def _():
                w_out_copy(0).wait_send()

            @pl.when(more)
            def _():
                w_out_copy(l + 1).wait_send()

        @pl.when(core == 1)
        def _():
            blocks = 2 * side
            taken(kst.at[l, pl.ds(0, blocks - 2)], hs_sem.at[l, 0])
            taken(vst.at[l, pl.ds(0, blocks - 2)], hs_sem.at[l, 1])
            for h in (1, 0):
                taken(krv.at[l, h, pl.ds(0, blocks - 2 * h)], hr_sem.at[l, h, 0])
                taken(vrv.at[l, h, pl.ds(0, blocks - 2 * h)], hr_sem.at[l, h, 1])
                for g in range(2):
                    part = slice(g * side, (g + 1) * side)
                    kb[h, g] = krv[l, h, part].reshape(side * span, hd).astype(bf16)
                    vb[h, g] = vrv[l, h, part].reshape(side * span, hd).astype(bf16)

            for h in (1, 0):
                @pl.when(y == x)
                def _():
                    if h:
                        kr[1, me] = ks[pl.ds(pl.multiple_of(8 * x, 8), 4), :]
                    taken(kr.at[h, pl.ds(0, n - h)], kr_sem.at[h])
                    fresh_sum[h] = functools.reduce(jnp.add, [kr[h, c] for c in range(n)])

                q_arrivals(h)
                attend(h)
                for k in far_chips:
                    o_copy(h, k).start()

            @pl.when(more)
            def _():
                stage(l + 1)

            load(WO, l).wait()
            taken(wo2.at[l], xr_sem.at[l])
            wob[...] = wo2[l].astype(bf16)
            for k in far_chips:
                for c in q_copies(k):
                    c.wait_send()
            fresh_sends(lambda c: c.wait_send())
            for k in far_chips[14:15]:
                taken(orr.at[1, places[k][0], pl.ds(0, ROWS)], or_sem.at[1, k])
            @pl.when(more)
            def _():
                pl.semaphore_signal(go, inc=1, device_id={"tp": cores[0]}, device_id_type=MESH)

            @pl.when(more)
            def _():
                ship_start(l + 1)

            for k in far_chips[0:14]:
                taken(orr.at[1, places[k][0], pl.ds(0, ROWS)], or_sem.at[1, k])
            tps[...] = jnp.dot(merge(1), wo[l], preferred_element_type=f32)
            for k in far_chips:
                taken(orr.at[0, places[k][0], pl.ds(0, ROWS)], or_sem.at[0, k])

            tps[...] = tps[...] + jnp.dot(merge(0), wob[...], preferred_element_type=f32)
            for k in range(tn - 1):
                t_copy(odd, k).start()
            for h in (1, 0):
                for k in far_chips:
                    o_copy(h, k).wait_send()
            out_ref[...] = out_ref[...] + tps[...] + t_arrivals(odd, 0)
            for k in range(tn - 1):
                t_copy(odd, k).wait_send()

        return carry

    lax.fori_loop(0, layers, layer_step, 0)


def shards(sizes, hidden, norm_gains, w_query, w_key, w_value, w_out, key_cache, value_cache, lengths):
    n, tn = sizes
    layers, feat, columns = w_query.shape
    batch = hidden.shape[0]
    _, _, _, span, hd = key_cache.shape
    heads = columns // hd
    side = math.isqrt(n)
    dims = (n, tn, side, layers, batch, feat, feat * n, heads, hd, span)
    f32, bf16 = jnp.float32, jnp.bfloat16
    vmem = pl.BlockSpec(memory_space=pltpu.VMEM)
    far = pl.BlockSpec(memory_space=pl.ANY)

    def like(array):
        return pltpu.VMEM(array.shape, array.dtype)

    dma = pltpu.SemaphoreType.DMA
    return pl.pallas_call(
        functools.partial(kernel, dims),
        out_shape=pltpu.VMEM((batch, feat), f32),
        in_specs=[far] * 9,
        out_specs=vmem,
        scratch_shapes=[
            like(hidden), like(norm_gains), pltpu.SMEM(lengths.shape, lengths.dtype),
            like(w_query), like(w_key), like(w_value), like(w_out), like(key_cache), like(value_cache),
            pltpu.VMEM((layers, batch, feat), f32),
            pltpu.VMEM((2, heads, side * span), f32),
            pltpu.VMEM((2, heads, hd), f32),
            pltpu.VMEM((2, heads, hd), f32),
            pltpu.VMEM((batch * 16, hd), f32),
            pltpu.VMEM((2, n, 2, 16, hd), f32),
            pltpu.VMEM((side * 8, hd), f32),
            pltpu.VMEM((2, n, 4, hd), f32),
            pltpu.VMEM((2, 4, hd), f32),
            pltpu.VMEM((layers, batch, span, hd), f32),
            pltpu.VMEM((layers, batch, span, hd), f32),
            pltpu.VMEM((layers, 2, 2 * side, span, hd), f32),
            pltpu.VMEM((layers, 2, 2 * side, span, hd), f32),
            pltpu.VMEM((2, 2, side * span, hd), bf16),
            pltpu.VMEM((2, 2, side * span, hd), bf16),
            pltpu.VMEM((2, n, 3 * heads, hd), f32),
            pltpu.VMEM((2, batch * heads, hd), f32),
            pltpu.VMEM(w_out.shape, f32),
            pltpu.VMEM(w_out.shape, f32),
            pltpu.VMEM(w_out.shape[1:], bf16),
            pltpu.VMEM((batch, feat), f32),
            pltpu.VMEM((2, tn - 1, batch, feat), f32),
            dma((6, layers)),
            dma((n, 2)), dma((2, n, 2)),
            dma((side,)), dma((2,)),
            dma((2, n)), dma((2, n)),
            dma((tn - 1,)), dma((2, tn - 1)),
            dma((layers, 2)), dma((layers, 2, 2)),
            dma((layers,)), dma((layers,)),
            dma((3,)), pltpu.SemaphoreType.REGULAR, pltpu.SemaphoreType.REGULAR,
        ],
        compiler_params=pltpu.CompilerParams(
            collective_id=0, has_side_effects=True, vmem_limit_bytes=60 * 1024 * 1024),
    )(hidden, norm_gains, lengths, w_query, w_key, w_value, w_out, key_cache, value_cache)


def solution(mesh):
    sizes = (mesh.shape["ctx"], mesh.shape["tp"])
    return jax.shard_map(
        functools.partial(shards, sizes),
        mesh=mesh,
        in_specs=(
            P(None, "ctx"),
            P(None, "ctx"),
            P(None, "ctx", "tp"),
            P(None, "ctx", "tp"),
            P(None, "ctx", "tp"),
            P(None, "tp", "ctx"),
            P(None, None, "tp", "ctx", None),
            P(None, None, "tp", "ctx", None),
            P(),
        ),
        out_specs=P(None, "ctx"),
        check_vma=False,
    )
```

```python
import functools
import math

import jax
import jax.numpy as jnp
from jax import lax
from jax.experimental import pallas as pl
from jax.experimental.pallas import tpu as pltpu
from jax.sharding import PartitionSpec as P

mask_fill = -1e30
norm_eps = 1e-05
rope_base = 500000.0
MESH = pl.DeviceIdType.MESH
QROWS = 9
ROWS = 17


def kernel(dims, hidden_h, gains_h, lengths_h, wq_h, wk_h, wv_h, wo_h, kc_h, vc_h, out_ref,
           hidden_ref, gains_ref, lengths_ref, wq, wk, wv, wo, kc, vc, gain, bias, cosine, sine, qs, qr, ks, kr, fresh_sum, kst, vst, krv, vrv, kb, vb,
           orr, cm, wst, wo2, wob, tps, tpr, w_sem, qs_sem, qr_sem, ks_sem, kr_sem, os_sem, or_sem, ts_sem, tr_sem, hs_sem, hr_sem, xs_sem, xr_sem, small_sem, ready, go):
    n, tn, side, layers, batch, feat, total, heads, hd, span = dims
    f32, bf16 = jnp.float32, jnp.bfloat16
    scale = 1.0 / math.sqrt(hd)
    me = lax.axis_index("ctx")
    mt = lax.axis_index("tp")
    y, x = me // side, lax.rem(me, side)
    z, core = mt // 2, lax.rem(mt, 2)
    zn = tn // 2
    weights = ((kc_h, kc), (vc_h, vc), (wq_h, wq), (wk_h, wk), (wv_h, wv), (wo_h, wo))
    KC, VC, WQ, WK, WV, WO = range(6)

    def load(index, layer):
        source, target = weights[index]
        return pltpu.make_async_copy(source.at[layer], target.at[layer], w_sem.at[index, layer])

    def hops(step, size):
        return min(step, size - step)

    offsets = [(dy, dx) for dy in range(side) for dx in range(side) if (dy, dx) != (0, 0)]
    offsets.sort(key=lambda o: -(hops(o[0], side) + hops(o[1], side)))
    peers = []
    for dy, dx in offsets:
        py, px = lax.rem(y + dy, side), lax.rem(x + dx, side)
        peers.append((py * side + px, py, px))
    toffsets = [(dz, dc) for dz in range(zn) for dc in range(2) if (dz, dc) != (0, 0)]
    toffsets.sort(key=lambda o: (-o[1], -hops(o[0], zn)))
    tpeers = [lax.rem(z + dz, zn) * 2 + lax.rem(core + dc, 2) for dz, dc in toffsets]

    column = [lax.rem(y + r, side) * side + x for r in range(1, side)]
    row = [y * side + lax.rem(x + r, side) for r in range(1, side)]
    barrier = pltpu.get_barrier_semaphore()
    cores = (2 * z, 2 * z + 1)
    for p in row + column:
        for t in cores:
            pl.semaphore_signal(barrier, inc=1, device_id={"ctx": p, "tp": t}, device_id_type=MESH)
    for p in tpeers:
        pl.semaphore_signal(barrier, inc=1, device_id={"tp": p}, device_id_type=MESH)

    smalls = [pltpu.make_async_copy(source, target, small_sem.at[i]) for i, (source, target) in enumerate(
        ((hidden_h, hidden_ref), (gains_h, gains_ref), (lengths_h, lengths_ref)))]
    for index in (KC, VC):
        load(index, 0).start()
    for c in smalls:
        c.start()
    for index in (WQ, WK, WV, WO):
        load(index, 0).start()
    for c in smalls:
        c.wait()

    half = hd // 2
    lane = lax.broadcasted_iota(jnp.int32, (heads, hd), 1)
    low = lane < half
    head = lax.broadcasted_iota(jnp.int32, (heads, hd), 0)
    picks = (lane == head, lane == head + half)
    mine = (x, side + y)
    slot = lax.broadcasted_iota(jnp.int32, (heads, side * span), 1)
    block = slot // span
    positions = (y * side * span + slot, (block * side + x) * span + lax.rem(slot, span))
    exponent = jnp.where(low, lane, lane - half).astype(f32) * (2.0 / hd)
    frequency = jnp.exp(-exponent * math.log(rope_base))
    for g in range(2):
        size = lengths_ref[mine[g]]
        bias[g] = jnp.where(positions[g] < size, 0.0, mask_fill)
        angle = jnp.full((heads, hd), size, jnp.int32).astype(f32) * frequency
        cosine[g] = jnp.cos(angle)
        sine[g] = jnp.where(low, -jnp.sin(angle), jnp.sin(angle))
    for l in range(layers):
        gain[l] = jnp.broadcast_to(gains_ref[l:l + 1, :].astype(f32), (batch, feat))
    out_ref[...] = hidden_ref[...].astype(f32)
    own_mask = jnp.where(jnp.full((heads, 1), y, jnp.int32) == jnp.full((heads, 1), x, jnp.int32), 0.0, mask_fill)

    def ship(l, rounds):
        copies = []
        for r in rounds:
            px, py = lax.rem(x + r, side), lax.rem(y + r, side)
            for i, (source, target) in enumerate(((kst, krv), (vst, vrv))):
                copies.append(pltpu.make_async_remote_copy(
                    src_ref=source.at[l, px], dst_ref=target.at[l, core, x],
                    send_sem=hs_sem.at[l, i], recv_sem=hr_sem.at[l, core, i],
                    device_id={"ctx": y * side + px, "tp": cores[1]}, device_id_type=MESH))
                copies.append(pltpu.make_async_remote_copy(
                    src_ref=source.at[l, side + py], dst_ref=target.at[l, core, side + y],
                    send_sem=hs_sem.at[l, i], recv_sem=hr_sem.at[l, core, i],
                    device_id={"ctx": py * side + x, "tp": cores[1]}, device_id_type=MESH))
        return copies

    def ship_start(l):
        for c in ship(l, (2, 1, 3)):
            c.start()

        @pl.when(core == 0)
        def _():
            for c in ship(l, (0,)):
                c.start()

    def taken(ref, sem):
        pltpu.make_async_copy(ref, ref, sem).wait()

    def stage(l):
        load(KC, l).wait()
        load(VC, l).wait()
        for source, staged, held in ((kc, kst, krv), (vc, vst, vrv)):
            for b in range(batch):
                staged[l, b] = source[l, b, 0].astype(f32)

            @pl.when(core == 1)
            def _():
                held[l, 1, x] = source[l, mine[0], 0].astype(f32)
                held[l, 1, side + y] = source[l, mine[1], 0].astype(f32)

    def fresh_copy(d):
        return pltpu.make_async_remote_copy(
            src_ref=ks.at[pl.ds(8 * d, 4)], dst_ref=kr.at[core, me], send_sem=ks_sem.at[d], recv_sem=kr_sem.at[core],
            device_id={"ctx": d * side + d, "tp": cores[1]}, device_id_type=MESH)

    def fresh_sends(act):
        for d in range(side):
            @pl.when(jnp.logical_or(core == 0, me != d * side + d))
            def _():
                act(fresh_copy(d))

    places = peers + [(me, y, x)]
    far_chips = range(n - 1)

    def q_copies(k):
        p, py, px = places[k]
        return [pltpu.make_async_remote_copy(
            src_ref=qs.at[pl.ds(pl.multiple_of(b * 16, 16), QROWS)], dst_ref=qr.at[core, k, g, pl.ds(0, QROWS)],
            send_sem=qs_sem.at[k, g], recv_sem=qr_sem.at[core, k, g],
            device_id={"ctx": p, "tp": cores[1]}, device_id_type=MESH) for g, b in ((0, px), (1, side + py))]

    def q_arrivals(h):
        for k in range(n - h):
            for g in range(2):
                taken(qr.at[h, k, g, pl.ds(0, QROWS)], qr_sem.at[h, k, g])

    def o_copy(h, k):
        return pltpu.make_async_remote_copy(
            src_ref=orr.at[h, me, pl.ds(0, ROWS)], dst_ref=orr.at[h, me, pl.ds(0, ROWS)], send_sem=os_sem.at[h, k], recv_sem=or_sem.at[h, k],
            device_id={"ctx": places[k][0]}, device_id_type=MESH)

    def w_out_copy(l):
        return pltpu.make_async_remote_copy(
            src_ref=wst.at[l], dst_ref=wo2.at[l], send_sem=xs_sem.at[l], recv_sem=xr_sem.at[l],
            device_id={"tp": cores[1]}, device_id_type=MESH)

    def w_out_start(l):
        load(WO, l).wait()
        wst[l] = wo[l].astype(f32)
        w_out_copy(l).start()

    def t_copy(odd, k):
        return pltpu.make_async_remote_copy(
            src_ref=tps, dst_ref=tpr.at[odd, k], send_sem=ts_sem.at[k], recv_sem=tr_sem.at[odd, k],
            device_id={"tp": tpeers[k]}, device_id_type=MESH)

    def t_arrivals(odd, cross):
        moved = None
        for k, (dz, dc) in enumerate(toffsets):
            if dc == cross:
                taken(tpr.at[odd, k], tr_sem.at[odd, k])
                moved = tpr[odd, k] if moved is None else moved + tpr[odd, k]
        return moved

    fresh_sum[...] = jnp.zeros_like(fresh_sum)
    stage(0)
    pl.semaphore_wait(barrier, 2 * len(row) + 2 * len(column) + len(tpeers))
    for p in column:
        for t in cores:
            pl.semaphore_signal(ready, inc=1, device_id={"ctx": p, "tp": t}, device_id_type=MESH)
    ship_start(0)
    pl.semaphore_wait(ready, 2 * len(column))

    def rotate(u, g):
        return u * cosine[g] + pltpu.roll(u, half, 1) * sine[g]

    def rounded(u):
        return u.astype(bf16).astype(f32)

    def attend(h):
        both = range(2)
        inverse, query = [], []
        for g in both:
            whole, square = qr[h, 0, g, 0:heads], qr[h, 0, g, heads:QROWS]
            for k in range(1, n - h):
                whole = whole + qr[h, k, g, 0:heads]
                square = square + qr[h, k, g, heads:QROWS]
            if h:
                at = pl.multiple_of(mine[g] * 16, 16)
                whole = whole + qs[pl.ds(at, heads), :]
                square = square + qs[pl.ds(pl.multiple_of(at + 8, 8), 1), :]
            inverse.append(lax.rsqrt(square / total + norm_eps))
            query.append(rounded(rotate(whole * inverse[g], g)))
        score = [lax.dot_general(
            query[g].astype(bf16), kb[h, g], (((1,), (1,)), ((), ())), preferred_element_type=f32) for g in both]
        new_key = [rounded(rotate(jnp.broadcast_to(fresh_sum[h, 2 * g:2 * g + 1] * inverse[g], (heads, hd)), g)) for g in both]
        new_value = [rounded(fresh_sum[h, 2 * g + 1:2 * g + 2] * inverse[g]) for g in both]
        own = [jnp.sum(query[g] * new_key[g], axis=1, keepdims=True) * scale + own_mask for g in both]
        masked = [score[g] * scale + bias[g] for g in both]
        top = [jnp.maximum(jnp.max(masked[g], axis=1, keepdims=True), own[g]) for g in both]
        weight = [jnp.exp(masked[g] - top[g]) for g in both]
        numerator = [jnp.dot(weight[g].astype(bf16), vb[h, g], preferred_element_type=f32) for g in both]
        fresh = [jnp.exp(own[g] - top[g]) for g in both]
        denominator = [jnp.sum(weight[g], axis=1, keepdims=True) + fresh[g] for g in both]
        logs = [top[g] + jnp.log(denominator[g]) for g in both]
        share = [1.0 / denominator[g] for g in both]
        parts = [(numerator[g] + rounded(fresh[g]) * new_value[g]) * share[g] for g in both]
        for g in both:
            orr[h, me, g * heads:(g + 1) * heads, :] = parts[g]
        spread = jnp.where(picks[0], logs[0], jnp.where(picks[1], logs[1], 0.0))
        orr[h, me, 2 * heads:ROWS, :] = jnp.sum(spread, axis=0, keepdims=True)

    def merge(h):
        logs = [orr[h, c, 2 * heads:ROWS, :] for c in range(n)]
        groups = [[[r * side + b for r in range(side)] for b in range(side)],
                  [[b * side + r for r in range(side)] for b in range(side)]]

        def over(values, op):
            return [[functools.reduce(op, [values[c] for c in group]) for group in part] for part in groups]

        def split(pair, c):
            return jnp.where(low[0:1], pair[0][c % side], pair[1][c // side])

        largest = over(logs, jnp.maximum)
        factors = [jnp.exp(logs[c] - split(largest, c)) for c in range(n)]
        sums = over(factors, jnp.add)
        inverses = [[1.0 / s for s in part] for part in sums]
        factors = [factors[c] * split(inverses, c) for c in range(n)]
        factors = [jnp.broadcast_to(f, (heads, hd)) for f in factors]
        for g in range(2):
            for b, group in enumerate(groups[g]):
                merged = None
                for c in group:
                    factor = jnp.sum(jnp.where(picks[g], factors[c], 0.0), axis=1, keepdims=True)
                    term = orr[h, c, g * heads:(g + 1) * heads, :] * factor
                    merged = term if merged is None else merged + term
                at = (g * side + b) * heads
                cm[h, at:at + heads, :] = merged
        return jnp.concatenate([cm[h, pl.ds(t, batch, stride=heads), :] for t in range(heads)], axis=1).astype(bf16)

    def layer_step(l, carry):
        stream = out_ref[...]
        scaled = (stream * gain[l]).astype(bf16)
        squares = jnp.sum(stream * stream, axis=1, keepdims=True)
        load(WQ, l).wait()
        load(WK, l).wait()
        load(WV, l).wait()

        @pl.when(l + 1 < layers)
        def _():
            for index in range(len(weights)):
                load(index, l + 1).start()

        def put(row, tile):
            qs[pl.ds(row, batch, stride=16), :] = tile

        for i, w in enumerate((wk, wv)):
            kv = jnp.dot(scaled, w[l], preferred_element_type=f32)
            for g in range(2):
                ks[pl.ds(2 * g + i, side, stride=8), :] = kv[g * side:(g + 1) * side]
        put(heads, jnp.broadcast_to(squares, (batch, hd)))
        q = jnp.dot(scaled, wq[l], preferred_element_type=f32)
        for h in range(heads):
            put(h, q[:, h * hd:(h + 1) * hd])
        fresh_sends(lambda c: c.start())
        for k in far_chips:
            for c in q_copies(k):
                c.start()

        odd = lax.rem(l, 2)
        more = l + 1 < layers

        @pl.when(core == 0)
        def _():
            for c in q_copies(n - 1):
                c.start()

            @pl.when(l == 0)
            def _():
                w_out_start(0)

            @pl.when(more)
            def _():
                stage(l + 1)
                w_out_start(l + 1)

            taken(kst.at[l], hs_sem.at[l, 0])
            taken(vst.at[l], hs_sem.at[l, 1])
            for k in range(n):
                for c in q_copies(k):
                    c.wait_send()
            fresh_sends(lambda c: c.wait_send())

            @pl.when(more)
            def _():
                pl.semaphore_wait(go, 1)
                ship_start(l + 1)

            out_ref[...] = out_ref[...] + t_arrivals(odd, 1)

            @pl.when(l == 0)
            def _():
                w_out_copy(0).wait_send()

            @pl.when(more)
            def _():
                w_out_copy(l + 1).wait_send()

        @pl.when(core == 1)
        def _():
            blocks = 2 * side
            taken(kst.at[l, pl.ds(0, blocks - 2)], hs_sem.at[l, 0])
            taken(vst.at[l, pl.ds(0, blocks - 2)], hs_sem.at[l, 1])
            for h in (1, 0):
                taken(krv.at[l, h, pl.ds(0, blocks - 2 * h)], hr_sem.at[l, h, 0])
                taken(vrv.at[l, h, pl.ds(0, blocks - 2 * h)], hr_sem.at[l, h, 1])
                for g in range(2):
                    part = slice(g * side, (g + 1) * side)
                    kb[h, g] = krv[l, h, part].reshape(side * span, hd).astype(bf16)
                    vb[h, g] = vrv[l, h, part].reshape(side * span, hd).astype(bf16)

            for h in (1, 0):
                @pl.when(y == x)
                def _():
                    if h:
                        kr[1, me] = ks[pl.ds(pl.multiple_of(8 * x, 8), 4), :]
                    taken(kr.at[h, pl.ds(0, n - h)], kr_sem.at[h])
                    fresh_sum[h] = functools.reduce(jnp.add, [kr[h, c] for c in range(n)])

                q_arrivals(h)
                attend(h)
                for k in far_chips:
                    o_copy(h, k).start()

            @pl.when(more)
            def _():
                stage(l + 1)

            load(WO, l).wait()
            taken(wo2.at[l], xr_sem.at[l])
            wob[...] = wo2[l].astype(bf16)
            for k in far_chips:
                for c in q_copies(k):
                    c.wait_send()
            fresh_sends(lambda c: c.wait_send())
            for k in far_chips[14:15]:
                taken(orr.at[1, places[k][0], pl.ds(0, ROWS)], or_sem.at[1, k])
            @pl.when(more)
            def _():
                pl.semaphore_signal(go, inc=1, device_id={"tp": cores[0]}, device_id_type=MESH)

            @pl.when(more)
            def _():
                ship_start(l + 1)

            for k in far_chips[0:14]:
                taken(orr.at[1, places[k][0], pl.ds(0, ROWS)], or_sem.at[1, k])
            tps[...] = jnp.dot(merge(1), wo[l], preferred_element_type=f32)
            for k in far_chips:
                taken(orr.at[0, places[k][0], pl.ds(0, ROWS)], or_sem.at[0, k])

            tps[...] = tps[...] + jnp.dot(merge(0), wob[...], preferred_element_type=f32)
            for k in range(tn - 1):
                t_copy(odd, k).start()
            for h in (1, 0):
                for k in far_chips:
                    o_copy(h, k).wait_send()
            out_ref[...] = out_ref[...] + tps[...] + t_arrivals(odd, 0)
            for k in range(tn - 1):
                t_copy(odd, k).wait_send()

        return carry

    lax.fori_loop(0, layers, layer_step, 0)


def shards(sizes, hidden, norm_gains, w_query, w_key, w_value, w_out, key_cache, value_cache, lengths):
    n, tn = sizes
    layers, feat, columns = w_query.shape
    batch = hidden.shape[0]
    _, _, _, span, hd = key_cache.shape
    heads = columns // hd
    side = math.isqrt(n)
    dims = (n, tn, side, layers, batch, feat, feat * n, heads, hd, span)
    f32, bf16 = jnp.float32, jnp.bfloat16
    vmem = pl.BlockSpec(memory_space=pltpu.VMEM)
    far = pl.BlockSpec(memory_space=pl.ANY)

    def like(array):
        return pltpu.VMEM(array.shape, array.dtype)

    dma = pltpu.SemaphoreType.DMA
    return pl.pallas_call(
        functools.partial(kernel, dims),
        out_shape=pltpu.VMEM((batch, feat), f32),
        in_specs=[far] * 9,
        out_specs=vmem,
        scratch_shapes=[
            like(hidden), like(norm_gains), pltpu.SMEM(lengths.shape, lengths.dtype),
            like(w_query), like(w_key), like(w_value), like(w_out), like(key_cache), like(value_cache),
            pltpu.VMEM((layers, batch, feat), f32),
            pltpu.VMEM((2, heads, side * span), f32),
            pltpu.VMEM((2, heads, hd), f32),
            pltpu.VMEM((2, heads, hd), f32),
            pltpu.VMEM((batch * 16, hd), f32),
            pltpu.VMEM((2, n, 2, 16, hd), f32),
            pltpu.VMEM((side * 8, hd), f32),
            pltpu.VMEM((2, n, 4, hd), f32),
            pltpu.VMEM((2, 4, hd), f32),
            pltpu.VMEM((layers, batch, span, hd), f32),
            pltpu.VMEM((layers, batch, span, hd), f32),
            pltpu.VMEM((layers, 2, 2 * side, span, hd), f32),
            pltpu.VMEM((layers, 2, 2 * side, span, hd), f32),
            pltpu.VMEM((2, 2, side * span, hd), bf16),
            pltpu.VMEM((2, 2, side * span, hd), bf16),
            pltpu.VMEM((2, n, 3 * heads, hd), f32),
            pltpu.VMEM((2, batch * heads, hd), f32),
            pltpu.VMEM(w_out.shape, f32),
            pltpu.VMEM(w_out.shape, f32),
            pltpu.VMEM(w_out.shape[1:], bf16),
            pltpu.VMEM((batch, feat), f32),
            pltpu.VMEM((2, tn - 1, batch, feat), f32),
            dma((6, layers)),
            dma((n, 2)), dma((2, n, 2)),
            dma((side,)), dma((2,)),
            dma((2, n)), dma((2, n)),
            dma((tn - 1,)), dma((2, tn - 1)),
            dma((layers, 2)), dma((layers, 2, 2)),
            dma((layers,)), dma((layers,)),
            dma((3,)), pltpu.SemaphoreType.REGULAR, pltpu.SemaphoreType.REGULAR,
        ],
        compiler_params=pltpu.CompilerParams(
            collective_id=0, has_side_effects=True, vmem_limit_bytes=60 * 1024 * 1024),
    )(hidden, norm_gains, lengths, w_query, w_key, w_value, w_out, key_cache, value_cache)


def solution(mesh):
    sizes = (mesh.shape["ctx"], mesh.shape["tp"])
    return jax.shard_map(
        functools.partial(shards, sizes),
        mesh=mesh,
        in_specs=(
            P(None, "ctx"),
            P(None, "ctx"),
            P(None, "ctx", "tp"),
            P(None, "ctx", "tp"),
            P(None, "ctx", "tp"),
            P(None, "tp", "ctx"),
            P(None, None, "tp", "ctx", None),
            P(None, None, "tp", "ctx", None),
            P(),
        ),
        out_specs=P(None, "ctx"),
        check_vma=False,
    )
```

```python
import functools
import math

import jax
import jax.numpy as jnp
from jax import lax
from jax.experimental import pallas as pl
from jax.experimental.pallas import tpu as pltpu
from jax.sharding import PartitionSpec as P

mask_fill = -1e30
norm_eps = 1e-05
rope_base = 500000.0
MESH = pl.DeviceIdType.MESH
QROWS = 9
ROWS = 17


def kernel(dims, hidden_h, gains_h, lengths_h, wq_h, wk_h, wv_h, wo_h, kc_h, vc_h, out_ref,
           hidden_ref, gains_ref, lengths_ref, wq, wk, wv, wo, kc, vc, gain, bias, cosine, sine, qs, qr, ks, kr, fresh_sum, kst, vst, krv, vrv, kb, vb,
           orr, cm, wst, wo2, wob, tps, tpr, w_sem, qs_sem, qr_sem, ks_sem, kr_sem, os_sem, or_sem, ts_sem, tr_sem, hs_sem, hr_sem, xs_sem, xr_sem, small_sem, ready, go):
    n, tn, side, layers, batch, feat, total, heads, hd, span = dims
    f32, bf16 = jnp.float32, jnp.bfloat16
    scale = 1.0 / math.sqrt(hd)
    me = lax.axis_index("ctx")
    mt = lax.axis_index("tp")
    y, x = me // side, lax.rem(me, side)
    z, core = mt // 2, lax.rem(mt, 2)
    zn = tn // 2
    weights = ((kc_h, kc), (vc_h, vc), (wq_h, wq), (wk_h, wk), (wv_h, wv), (wo_h, wo))
    KC, VC, WQ, WK, WV, WO = range(6)

    def load(index, layer):
        source, target = weights[index]
        return pltpu.make_async_copy(source.at[layer], target.at[layer], w_sem.at[index, layer])

    def hops(step, size):
        return min(step, size - step)

    offsets = [(dy, dx) for dy in range(side) for dx in range(side) if (dy, dx) != (0, 0)]
    offsets.sort(key=lambda o: -(hops(o[0], side) + hops(o[1], side)))
    peers = []
    for dy, dx in offsets:
        py, px = lax.rem(y + dy, side), lax.rem(x + dx, side)
        peers.append((py * side + px, py, px))
    toffsets = [(dz, dc) for dz in range(zn) for dc in range(2) if (dz, dc) != (0, 0)]
    toffsets.sort(key=lambda o: -(2 * hops(o[0], zn) + o[1]))
    tpeers = [lax.rem(z + dz, zn) * 2 + lax.rem(core + dc, 2) for dz, dc in toffsets]

    column = [lax.rem(y + r, side) * side + x for r in range(1, side)]
    row = [y * side + lax.rem(x + r, side) for r in range(1, side)]
    barrier = pltpu.get_barrier_semaphore()
    cores = (2 * z, 2 * z + 1)
    for p in row + column:
        for t in cores:
            pl.semaphore_signal(barrier, inc=1, device_id={"ctx": p, "tp": t}, device_id_type=MESH)
    for p in tpeers:
        pl.semaphore_signal(barrier, inc=1, device_id={"tp": p}, device_id_type=MESH)

    smalls = [pltpu.make_async_copy(source, target, small_sem.at[i]) for i, (source, target) in enumerate(
        ((hidden_h, hidden_ref), (gains_h, gains_ref), (lengths_h, lengths_ref)))]
    for index in (KC, VC):
        load(index, 0).start()
    for c in smalls:
        c.start()
    for index in (WQ, WK, WV, WO):
        load(index, 0).start()
    for c in smalls:
        c.wait()

    half = hd // 2
    lane = lax.broadcasted_iota(jnp.int32, (heads, hd), 1)
    low = lane < half
    head = lax.broadcasted_iota(jnp.int32, (heads, hd), 0)
    picks = (lane == head, lane == head + half)
    mine = (x, side + y)
    slot = lax.broadcasted_iota(jnp.int32, (heads, side * span), 1)
    block = slot // span
    positions = (y * side * span + slot, (block * side + x) * span + lax.rem(slot, span))
    exponent = jnp.where(low, lane, lane - half).astype(f32) * (2.0 / hd)
    frequency = jnp.exp(-exponent * math.log(rope_base))
    for g in range(2):
        size = lengths_ref[mine[g]]
        bias[g] = jnp.where(positions[g] < size, 0.0, mask_fill)
        angle = jnp.full((heads, hd), size, jnp.int32).astype(f32) * frequency
        cosine[g] = jnp.cos(angle)
        sine[g] = jnp.where(low, -jnp.sin(angle), jnp.sin(angle))
    for l in range(layers):
        gain[l] = jnp.broadcast_to(gains_ref[l:l + 1, :].astype(f32), (batch, feat))
    out_ref[...] = hidden_ref[...].astype(f32)
    own_mask = jnp.where(jnp.full((heads, 1), y, jnp.int32) == jnp.full((heads, 1), x, jnp.int32), 0.0, mask_fill)

    def ship(l, rounds):
        copies = []
        for r in rounds:
            px, py = lax.rem(x + r, side), lax.rem(y + r, side)
            for i, (source, target) in enumerate(((kst, krv), (vst, vrv))):
                copies.append(pltpu.make_async_remote_copy(
                    src_ref=source.at[l, px], dst_ref=target.at[l, core, x],
                    send_sem=hs_sem.at[l, i], recv_sem=hr_sem.at[l, core, i],
                    device_id={"ctx": y * side + px, "tp": cores[1]}, device_id_type=MESH))
                copies.append(pltpu.make_async_remote_copy(
                    src_ref=source.at[l, side + py], dst_ref=target.at[l, core, side + y],
                    send_sem=hs_sem.at[l, i], recv_sem=hr_sem.at[l, core, i],
                    device_id={"ctx": py * side + x, "tp": cores[1]}, device_id_type=MESH))
        return copies

    def ship_start(l):
        for c in ship(l, (2, 1, 3)):
            c.start()

        @pl.when(core == 0)
        def _():
            for c in ship(l, (0,)):
                c.start()

    def taken(ref, sem):
        pltpu.make_async_copy(ref, ref, sem).wait()

    def stage(l):
        load(KC, l).wait()
        load(VC, l).wait()
        for source, staged, held in ((kc, kst, krv), (vc, vst, vrv)):
            for b in range(batch):
                staged[l, b] = source[l, b, 0].astype(f32)

            @pl.when(core == 1)
            def _():
                held[l, 1, x] = source[l, mine[0], 0].astype(f32)
                held[l, 1, side + y] = source[l, mine[1], 0].astype(f32)

    def fresh_copy(d):
        return pltpu.make_async_remote_copy(
            src_ref=ks.at[pl.ds(8 * d, 4)], dst_ref=kr.at[core, me], send_sem=ks_sem.at[d], recv_sem=kr_sem.at[core],
            device_id={"ctx": d * side + d, "tp": cores[1]}, device_id_type=MESH)

    def fresh_sends(act):
        for d in range(side):
            @pl.when(jnp.logical_or(core == 0, me != d * side + d))
            def _():
                act(fresh_copy(d))

    places = peers + [(me, y, x)]
    far_chips = range(n - 1)

    def q_copies(k):
        p, py, px = places[k]
        return [pltpu.make_async_remote_copy(
            src_ref=qs.at[pl.ds(pl.multiple_of(b * 16, 16), QROWS)], dst_ref=qr.at[core, k, g, pl.ds(0, QROWS)],
            send_sem=qs_sem.at[k, g], recv_sem=qr_sem.at[core, k, g],
            device_id={"ctx": p, "tp": cores[1]}, device_id_type=MESH) for g, b in ((0, px), (1, side + py))]

    def q_arrivals(h):
        for k in range(n - h):
            for g in range(2):
                taken(qr.at[h, k, g, pl.ds(0, QROWS)], qr_sem.at[h, k, g])

    def o_copy(h, k):
        return pltpu.make_async_remote_copy(
            src_ref=orr.at[h, me, pl.ds(0, ROWS)], dst_ref=orr.at[h, me, pl.ds(0, ROWS)], send_sem=os_sem.at[h, k], recv_sem=or_sem.at[h, k],
            device_id={"ctx": places[k][0]}, device_id_type=MESH)

    def w_out_copy(l):
        return pltpu.make_async_remote_copy(
            src_ref=wst.at[l], dst_ref=wo2.at[l], send_sem=xs_sem.at[l], recv_sem=xr_sem.at[l],
            device_id={"tp": cores[1]}, device_id_type=MESH)

    def w_out_start(l):
        load(WO, l).wait()
        wst[l] = wo[l].astype(f32)
        w_out_copy(l).start()

    def t_copy(odd, k):
        return pltpu.make_async_remote_copy(
            src_ref=tps, dst_ref=tpr.at[odd, k], send_sem=ts_sem.at[k], recv_sem=tr_sem.at[odd, k],
            device_id={"tp": tpeers[k]}, device_id_type=MESH)

    def t_arrivals(odd, cross):
        moved = None
        for k, (dz, dc) in enumerate(toffsets):
            if dc == cross:
                taken(tpr.at[odd, k], tr_sem.at[odd, k])
                moved = tpr[odd, k] if moved is None else moved + tpr[odd, k]
        return moved

    fresh_sum[...] = jnp.zeros_like(fresh_sum)
    stage(0)
    pl.semaphore_wait(barrier, 2 * len(row) + 2 * len(column) + len(tpeers))
    for p in column:
        for t in cores:
            pl.semaphore_signal(ready, inc=1, device_id={"ctx": p, "tp": t}, device_id_type=MESH)
    ship_start(0)
    pl.semaphore_wait(ready, 2 * len(column))

    def rotate(u, g):
        return u * cosine[g] + pltpu.roll(u, half, 1) * sine[g]

    def rounded(u):
        return u.astype(bf16).astype(f32)

    def attend(h):
        both = range(2)
        inverse, query = [], []
        for g in both:
            whole, square = qr[h, 0, g, 0:heads], qr[h, 0, g, heads:QROWS]
            for k in range(1, n - h):
                whole = whole + qr[h, k, g, 0:heads]
                square = square + qr[h, k, g, heads:QROWS]
            if h:
                at = pl.multiple_of(mine[g] * 16, 16)
                whole = whole + qs[pl.ds(at, heads), :]
                square = square + qs[pl.ds(pl.multiple_of(at + 8, 8), 1), :]
            inverse.append(lax.rsqrt(square / total + norm_eps))
            query.append(rounded(rotate(whole * inverse[g], g)))
        score = [jnp.dot(query[g].astype(bf16), kb[h, g], preferred_element_type=f32) for g in both]
        new_key = [rounded(rotate(jnp.broadcast_to(fresh_sum[h, 2 * g:2 * g + 1] * inverse[g], (heads, hd)), g)) for g in both]
        new_value = [rounded(fresh_sum[h, 2 * g + 1:2 * g + 2] * inverse[g]) for g in both]
        own = [jnp.sum(query[g] * new_key[g], axis=1, keepdims=True) * scale + own_mask for g in both]
        masked = [score[g] * scale + bias[g] for g in both]
        top = [jnp.maximum(jnp.max(masked[g], axis=1, keepdims=True), own[g]) for g in both]
        weight = [jnp.exp(masked[g] - top[g]) for g in both]
        numerator = [jnp.dot(weight[g].astype(bf16), vb[h, g], preferred_element_type=f32) for g in both]
        fresh = [jnp.exp(own[g] - top[g]) for g in both]
        denominator = [jnp.sum(weight[g], axis=1, keepdims=True) + fresh[g] for g in both]
        logs = [top[g] + jnp.log(denominator[g]) for g in both]
        share = [1.0 / denominator[g] for g in both]
        parts = [(numerator[g] + rounded(fresh[g]) * new_value[g]) * share[g] for g in both]
        for g in both:
            orr[h, me, g * heads:(g + 1) * heads, :] = parts[g]
        spread = jnp.where(picks[0], logs[0], jnp.where(picks[1], logs[1], 0.0))
        orr[h, me, 2 * heads:ROWS, :] = jnp.sum(spread, axis=0, keepdims=True)

    def merge(h):
        logs = [orr[h, c, 2 * heads:ROWS, :] for c in range(n)]
        groups = [[[r * side + b for r in range(side)] for b in range(side)],
                  [[b * side + r for r in range(side)] for b in range(side)]]

        def over(values, op):
            return [[functools.reduce(op, [values[c] for c in group]) for group in part] for part in groups]

        def split(pair, c):
            return jnp.where(low[0:1], pair[0][c % side], pair[1][c // side])

        largest = over(logs, jnp.maximum)
        factors = [jnp.exp(logs[c] - split(largest, c)) for c in range(n)]
        sums = over(factors, jnp.add)
        inverses = [[1.0 / s for s in part] for part in sums]
        factors = [factors[c] * split(inverses, c) for c in range(n)]
        factors = [jnp.broadcast_to(f, (heads, hd)) for f in factors]
        for g in range(2):
            for b, group in enumerate(groups[g]):
                merged = None
                for c in group:
                    factor = jnp.sum(jnp.where(picks[g], factors[c], 0.0), axis=1, keepdims=True)
                    term = orr[h, c, g * heads:(g + 1) * heads, :] * factor
                    merged = term if merged is None else merged + term
                at = (g * side + b) * heads
                cm[h, at:at + heads, :] = merged
        return jnp.concatenate([cm[h, pl.ds(t, batch, stride=heads), :] for t in range(heads)], axis=1).astype(bf16)

    def layer_step(l, carry):
        stream = out_ref[...]
        scaled = (stream * gain[l]).astype(bf16)
        squares = jnp.sum(stream * stream, axis=1, keepdims=True)
        load(WQ, l).wait()
        load(WK, l).wait()
        load(WV, l).wait()

        @pl.when(l + 1 < layers)
        def _():
            for index in range(len(weights)):
                load(index, l + 1).start()

        def put(row, tile):
            qs[pl.ds(row, batch, stride=16), :] = tile

        for i, w in enumerate((wk, wv)):
            kv = jnp.dot(scaled, w[l], preferred_element_type=f32)
            for g in range(2):
                ks[pl.ds(2 * g + i, side, stride=8), :] = kv[g * side:(g + 1) * side]
        put(heads, jnp.broadcast_to(squares, (batch, hd)))
        q = jnp.dot(scaled, wq[l], preferred_element_type=f32)
        for h in range(heads):
            put(h, q[:, h * hd:(h + 1) * hd])
        fresh_sends(lambda c: c.start())
        for k in far_chips:
            for c in q_copies(k):
                c.start()

        odd = lax.rem(l, 2)
        more = l + 1 < layers

        @pl.when(core == 0)
        def _():
            for c in q_copies(n - 1):
                c.start()

            @pl.when(l == 0)
            def _():
                w_out_start(0)

            @pl.when(more)
            def _():
                stage(l + 1)
                w_out_start(l + 1)

            taken(kst.at[l], hs_sem.at[l, 0])
            taken(vst.at[l], hs_sem.at[l, 1])
            for k in range(n):
                for c in q_copies(k):
                    c.wait_send()
            fresh_sends(lambda c: c.wait_send())

            @pl.when(more)
            def _():
                pl.semaphore_wait(go, 1)
                ship_start(l + 1)

            out_ref[...] = out_ref[...] + t_arrivals(odd, 1)

            @pl.when(l == 0)
            def _():
                w_out_copy(0).wait_send()

            @pl.when(more)
            def _():
                w_out_copy(l + 1).wait_send()

        @pl.when(core == 1)
        def _():
            blocks = 2 * side
            taken(kst.at[l, pl.ds(0, blocks - 2)], hs_sem.at[l, 0])
            taken(vst.at[l, pl.ds(0, blocks - 2)], hs_sem.at[l, 1])
            for h in (1, 0):
                taken(krv.at[l, h, pl.ds(0, blocks - 2 * h)], hr_sem.at[l, h, 0])
                taken(vrv.at[l, h, pl.ds(0, blocks - 2 * h)], hr_sem.at[l, h, 1])
                for g in range(2):
                    part = slice(g * side, (g + 1) * side)
                    kb[h, g] = krv[l, h, part].reshape(side * span, hd).T.astype(bf16)
                    vb[h, g] = vrv[l, h, part].reshape(side * span, hd).astype(bf16)

            for h in (1, 0):
                @pl.when(y == x)
                def _():
                    if h:
                        kr[1, me] = ks[pl.ds(pl.multiple_of(8 * x, 8), 4), :]
                    taken(kr.at[h, pl.ds(0, n - h)], kr_sem.at[h])
                    fresh_sum[h] = functools.reduce(jnp.add, [kr[h, c] for c in range(n)])

                q_arrivals(h)
                attend(h)
                for k in far_chips:
                    o_copy(h, k).start()

            @pl.when(more)
            def _():
                stage(l + 1)

            load(WO, l).wait()
            taken(wo2.at[l], xr_sem.at[l])
            wob[...] = wo2[l].astype(bf16)
            for k in far_chips:
                for c in q_copies(k):
                    c.wait_send()
            fresh_sends(lambda c: c.wait_send())
            for k in far_chips[14:15]:
                taken(orr.at[1, places[k][0], pl.ds(0, ROWS)], or_sem.at[1, k])
            @pl.when(more)
            def _():
                pl.semaphore_signal(go, inc=1, device_id={"tp": cores[0]}, device_id_type=MESH)

            @pl.when(more)
            def _():
                ship_start(l + 1)

            for k in far_chips[0:14]:
                taken(orr.at[1, places[k][0], pl.ds(0, ROWS)], or_sem.at[1, k])
            tps[...] = jnp.dot(merge(1), wo[l], preferred_element_type=f32)
            for k in far_chips:
                taken(orr.at[0, places[k][0], pl.ds(0, ROWS)], or_sem.at[0, k])

            tps[...] = tps[...] + jnp.dot(merge(0), wob[...], preferred_element_type=f32)
            for k in range(tn - 1):
                t_copy(odd, k).start()
            for h in (1, 0):
                for k in far_chips:
                    o_copy(h, k).wait_send()
            out_ref[...] = out_ref[...] + tps[...] + t_arrivals(odd, 0)
            for k in range(tn - 1):
                t_copy(odd, k).wait_send()

        return carry

    lax.fori_loop(0, layers, layer_step, 0)


def shards(sizes, hidden, norm_gains, w_query, w_key, w_value, w_out, key_cache, value_cache, lengths):
    n, tn = sizes
    layers, feat, columns = w_query.shape
    batch = hidden.shape[0]
    _, _, _, span, hd = key_cache.shape
    heads = columns // hd
    side = math.isqrt(n)
    dims = (n, tn, side, layers, batch, feat, feat * n, heads, hd, span)
    f32, bf16 = jnp.float32, jnp.bfloat16
    vmem = pl.BlockSpec(memory_space=pltpu.VMEM)
    far = pl.BlockSpec(memory_space=pl.ANY)

    def like(array):
        return pltpu.VMEM(array.shape, array.dtype)

    dma = pltpu.SemaphoreType.DMA
    return pl.pallas_call(
        functools.partial(kernel, dims),
        out_shape=pltpu.VMEM((batch, feat), f32),
        in_specs=[far] * 9,
        out_specs=vmem,
        scratch_shapes=[
            like(hidden), like(norm_gains), pltpu.SMEM(lengths.shape, lengths.dtype),
            like(w_query), like(w_key), like(w_value), like(w_out), like(key_cache), like(value_cache),
            pltpu.VMEM((layers, batch, feat), f32),
            pltpu.VMEM((2, heads, side * span), f32),
            pltpu.VMEM((2, heads, hd), f32),
            pltpu.VMEM((2, heads, hd), f32),
            pltpu.VMEM((batch * 16, hd), f32),
            pltpu.VMEM((2, n, 2, 16, hd), f32),
            pltpu.VMEM((side * 8, hd), f32),
            pltpu.VMEM((2, n, 4, hd), f32),
            pltpu.VMEM((2, 4, hd), f32),
            pltpu.VMEM((layers, batch, span, hd), f32),
            pltpu.VMEM((layers, batch, span, hd), f32),
            pltpu.VMEM((layers, 2, 2 * side, span, hd), f32),
            pltpu.VMEM((layers, 2, 2 * side, span, hd), f32),
            pltpu.VMEM((2, 2, hd, side * span), bf16),
            pltpu.VMEM((2, 2, side * span, hd), bf16),
            pltpu.VMEM((2, n, 3 * heads, hd), f32),
            pltpu.VMEM((2, batch * heads, hd), f32),
            pltpu.VMEM(w_out.shape, f32),
            pltpu.VMEM(w_out.shape, f32),
            pltpu.VMEM(w_out.shape[1:], bf16),
            pltpu.VMEM((batch, feat), f32),
            pltpu.VMEM((2, tn - 1, batch, feat), f32),
            dma((6, layers)),
            dma((n, 2)), dma((2, n, 2)),
            dma((side,)), dma((2,)),
            dma((2, n)), dma((2, n)),
            dma((tn - 1,)), dma((2, tn - 1)),
            dma((layers, 2)), dma((layers, 2, 2)),
            dma((layers,)), dma((layers,)),
            dma((3,)), pltpu.SemaphoreType.REGULAR, pltpu.SemaphoreType.REGULAR,
        ],
        compiler_params=pltpu.CompilerParams(
            collective_id=0, has_side_effects=True, vmem_limit_bytes=60 * 1024 * 1024),
    )(hidden, norm_gains, lengths, w_query, w_key, w_value, w_out, key_cache, value_cache)


def solution(mesh):
    sizes = (mesh.shape["ctx"], mesh.shape["tp"])
    return jax.shard_map(
        functools.partial(shards, sizes),
        mesh=mesh,
        in_specs=(
            P(None, "ctx"),
            P(None, "ctx"),
            P(None, "ctx", "tp"),
            P(None, "ctx", "tp"),
            P(None, "ctx", "tp"),
            P(None, "tp", "ctx"),
            P(None, None, "tp", "ctx", None),
            P(None, None, "tp", "ctx", None),
            P(),
        ),
        out_specs=P(None, "ctx"),
        check_vma=False,
    )
```
